8 devices in a mesh: dp: 1 (over z), fsdp: 8 (over y, x, core).
Axes of the slice: x: 2, y: 2, z: 1, core: 2. Of those that a mesh axis runs over, the one named last changes fastest.
Arguments:
- dec_in: bfloat16 [64, 192, 4096], P(('dp', 'fsdp'))
- enc_out: bfloat16 [64, 384, 4096], P(('dp', 'fsdp'))
- dec_mask: int32 [64, 192], P(('dp', 'fsdp'))
- enc_mask: int32 [64, 384], P(('dp', 'fsdp'))
- rel_bias: float32 [32, 64], replicated
- norm_self: bfloat16 [4096], P('fsdp')
- self_q: bfloat16 [4096, 4096], P('fsdp')
- self_k: bfloat16 [4096, 4096], P('fsdp')
- self_v: bfloat16 [4096, 4096], P('fsdp')
- self_o: bfloat16 [4096, 4096], P('fsdp')
- norm_cross: bfloat16 [4096], P('fsdp')
- cross_q: bfloat16 [4096, 4096], P('fsdp')
- cross_k: bfloat16 [4096, 4096], P('fsdp')
- cross_v: bfloat16 [4096, 4096], P('fsdp')
- cross_o: bfloat16 [4096, 4096], P('fsdp')
- norm_ff: bfloat16 [4096], P('fsdp')
- ff_gate: bfloat16 [4096, 10240], P('fsdp')
- ff_lin: bfloat16 [4096, 10240], P('fsdp')
- ff_out: bfloat16 [10240, 4096], P('fsdp')
Outputs:
- output: bfloat16 [64, 192, 4096], P(('dp', 'fsdp'))
All inputs are finite; a program needn't handle non-finite values.
Results may differ from the reference program's by a relative error of at most 0.0177488.
Values are sent between devices in bfloat16 or wider.
A program may use at most 1 GiB of HBM per device.

```python
import math
import jax
import jax.numpy as jnp
from jax import lax

BATCH = 64
TGT_LEN = 192
SRC_LEN = 384
D_MODEL = 4096
HEADS = 64
HEAD_DIM = 64
D_FF = 10240
NUM_BUCKETS = 32
EXACT_BUCKETS = 16
MAX_DISTANCE = 128
INNER_DIM = HEADS * HEAD_DIM
NORM_EPS = 1e-6
MASK_FILL = -1e9


def bucket_ids(length):
    return [offset if offset < EXACT_BUCKETS else min(NUM_BUCKETS - 1, EXACT_BUCKETS + int(math.log(offset / EXACT_BUCKETS) / math.log(MAX_DISTANCE / EXACT_BUCKETS) * (NUM_BUCKETS - EXACT_BUCKETS))) for offset in range(length)]


def prefix_mask(key_in, n_rows, length):
    lengths = jax.random.randint(key_in, (n_rows,), 1, length + 1)
    lengths = lengths.at[0].set(length).at[1].set(1)
    return (jnp.arange(length)[None, :] < lengths[:, None]).astype(jnp.int32)


def normal_bf(key_in, out_shape, factor):
    return (jax.random.normal(key_in, out_shape, jnp.float32) * factor).astype(jnp.bfloat16)


def norm_scale(key_in):
    return (1.0 + 0.3 * jax.random.normal(key_in, (D_MODEL,), jnp.float32)).astype(jnp.bfloat16)


def setup_inputs(seed: int = 0, part: int = 0) -> dict:
    shared = jax.random.split(jax.random.key(seed), 15)
    own = jax.random.split(jax.random.fold_in(jax.random.key(seed + 1), part), 4)
    qk_scale = (D_MODEL * HEAD_DIM) ** -0.5
    in_scale = D_MODEL ** -0.5
    out_scale = 2.0 * INNER_DIM ** -0.5
    return {
        'dec_in': normal_bf(own[0], (BATCH, TGT_LEN, D_MODEL), 1.0),
        'enc_out': normal_bf(own[1], (BATCH, SRC_LEN, D_MODEL), 1.0),
        'dec_mask': prefix_mask(own[2], BATCH, TGT_LEN),
        'enc_mask': prefix_mask(own[3], BATCH, SRC_LEN),
        'rel_bias': jax.random.normal(shared[0], (NUM_BUCKETS, HEADS), jnp.float32),
        'norm_self': norm_scale(shared[1]),
        'self_q': normal_bf(shared[2], (D_MODEL, INNER_DIM), qk_scale),
        'self_k': normal_bf(shared[3], (D_MODEL, INNER_DIM), in_scale),
        'self_v': normal_bf(shared[4], (D_MODEL, INNER_DIM), in_scale),
        'self_o': normal_bf(shared[5], (INNER_DIM, D_MODEL), out_scale),
        'norm_cross': norm_scale(shared[6]),
        'cross_q': normal_bf(shared[7], (D_MODEL, INNER_DIM), 2.0 * qk_scale),
        'cross_k': normal_bf(shared[8], (D_MODEL, INNER_DIM), in_scale),
        'cross_v': normal_bf(shared[9], (D_MODEL, INNER_DIM), in_scale),
        'cross_o': normal_bf(shared[10], (INNER_DIM, D_MODEL), out_scale),
        'norm_ff': norm_scale(shared[11]),
        'ff_gate': normal_bf(shared[12], (D_MODEL, D_FF), in_scale),
        'ff_lin': normal_bf(shared[13], (D_MODEL, D_FF), in_scale),
        'ff_out': normal_bf(shared[14], (D_FF, D_MODEL), D_FF ** -0.5),
    }


def rms_norm(values, scale_vec):
    val_f = values.astype(jnp.float32)
    mean_sq = jnp.mean(val_f * val_f, axis=-1, keepdims=True)
    return (val_f * lax.rsqrt(mean_sq + NORM_EPS) * scale_vec.astype(jnp.float32)).astype(jnp.bfloat16)


def project(hidden_in, weight):
    return jnp.dot(hidden_in, weight, preferred_element_type=jnp.float32).astype(jnp.bfloat16)


def add_residual(residual, update):
    return (residual.astype(jnp.float32) + update.astype(jnp.float32)).astype(jnp.bfloat16)


def attend(q_heads, k_heads, v_heads, add_bias, allowed):
    scores = jnp.einsum('qhd,khd->hqk', q_heads.astype(jnp.float32), k_heads.astype(jnp.float32)) + add_bias
    scores = jnp.where(allowed, scores, MASK_FILL)
    attn_prob = jax.nn.softmax(scores, axis=-1).astype(jnp.bfloat16)
    attn_ctx = jnp.einsum('hqk,khd->qhd', attn_prob.astype(jnp.float32), v_heads.astype(jnp.float32)).astype(jnp.bfloat16)
    return attn_ctx.reshape(attn_ctx.shape[0], INNER_DIM)


def reference(dec_in, enc_out, dec_mask, enc_mask, rel_bias, norm_self, self_q, self_k, self_v, self_o, norm_cross, cross_q, cross_k, cross_v, cross_o, norm_ff, ff_gate, ff_lin, ff_out):
    positions = jnp.arange(TGT_LEN)
    rel_dist = jnp.maximum(positions[:, None] - positions[None, :], 0)
    bucket_table = jnp.array(bucket_ids(TGT_LEN), dtype=jnp.int32)
    bias_heads = jnp.transpose(jnp.take(rel_bias, bucket_table[rel_dist], axis=0), (2, 0, 1))
    causal = positions[None, :] <= positions[:, None]

    def one_row(row_args):
        x_row, e_row, dec_row, enc_row = row_args
        h_self = rms_norm(x_row, norm_self)
        q_self = project(h_self, self_q).reshape(TGT_LEN, HEADS, HEAD_DIM)
        k_self = project(h_self, self_k).reshape(TGT_LEN, HEADS, HEAD_DIM)
        v_self = project(h_self, self_v).reshape(TGT_LEN, HEADS, HEAD_DIM)
        allowed_self = causal[None, :, :] & (dec_row[None, None, :] > 0)
        ctx_self = attend(q_self, k_self, v_self, bias_heads, allowed_self)
        x_one = add_residual(x_row, project(ctx_self, self_o))
        h_cross = rms_norm(x_one, norm_cross)
        q_cross = project(h_cross, cross_q).reshape(TGT_LEN, HEADS, HEAD_DIM)
        k_cross = project(e_row, cross_k).reshape(SRC_LEN, HEADS, HEAD_DIM)
        v_cross = project(e_row, cross_v).reshape(SRC_LEN, HEADS, HEAD_DIM)
        allowed_cross = enc_row[None, None, :] > 0
        ctx_cross = attend(q_cross, k_cross, v_cross, 0.0, allowed_cross)
        x_two = add_residual(x_one, project(ctx_cross, cross_o))
        h_ff = rms_norm(x_two, norm_ff)
        gate_act = project(h_ff, ff_gate).astype(jnp.float32)
        lin_act = project(h_ff, ff_lin).astype(jnp.float32)
        hidden = (jax.nn.gelu(gate_act, approximate=True) * lin_act).astype(jnp.bfloat16)
        return add_residual(x_two, project(hidden, ff_out))

    return lax.map(one_row, (dec_in, enc_out, dec_mask, enc_mask))
```

```python
import math
import jax
import jax.numpy as jnp
import numpy as np
from jax import lax
from jax.experimental import pallas as pl
from jax.experimental.pallas import tpu as pltpu
from jax.sharding import PartitionSpec as P

MESH = pl.DeviceIdType.MESH
F32, BF16 = jnp.float32, jnp.bfloat16
HEAD_DIM = 64
NUM_BUCKETS = 32
EXACT_BUCKETS = 16
MAX_DISTANCE = 128
NORM_EPS = 1e-6
MASK_FILL = -1e9
N_DEV = 8

AHEAD, PASS, DONE, RING = 4, 5, 6, 16
TASKS = {'self_q': 8, 'self_k': 8, 'self_v': 8, 'self_o': 8, 'cross_k': 8, 'cross_v': 8, 'cross_q': 8, 'cross_o': 8, 'ff_gate': 20, 'ff_lin': 20, 'ff_out': 16}
ALL_TASKS = sum(TASKS.values())
TICKS = {'head': 8, 'self_q': 8, 'self_k': 8, 'self_v': 8, 'self_attend': 6, 'self_o': 6, 'cross_k0': 6, 'cross_k1': 5, 'cross_v0': 6, 'cross_v1': 5,
         'cross_q': 6, 'cross_attend': 10, 'cross_o': 6, 'ff_gate': 13, 'ff_lin': 11, 'ff_out': 14}
assert sum(TICKS.values()) == ALL_TASKS + DONE
ROW_BLOCK = 512
GROUP = 512


def bucket_ids(length):
    return [offset if offset < EXACT_BUCKETS else min(NUM_BUCKETS - 1, EXACT_BUCKETS + int(math.log(offset / EXACT_BUCKETS) / math.log(MAX_DISTANCE / EXACT_BUCKETS) * (NUM_BUCKETS - EXACT_BUCKETS))) for offset in range(length)]


def bucket_row(length, lanes):
    ids = bucket_ids(length)
    return np.array([[ids[min((lanes - m) % lanes, length - 1)] for m in range(lanes)]], np.int32)


class Weight:
    def __init__(self, first, count, shard, got):
        self.first, self.count, self.shard, self.got = first, count, shard, got
        self.rows, self.width = shard.shape[0], shard.shape[1] // count


def layer_kernel(batch, names, buckets_ref, rel_ref, dec_mask_ref, enc_mask_ref, norm_ref, dec_ref, enc_ref, *refs):
    n_w = len(names)
    shards, refs = refs[:n_w], refs[n_w:]
    out_ref, q_ref, k_ref, v_ref, c_ref, ck_ref, cv_ref, g_ref, z_ref = refs[:9]
    gots, refs = refs[9:9 + n_w], refs[9 + n_w:]
    x_s, big, bias_s, dist_s, gain_in, gains, send_sem, recv_sem, norm_send, norm_recv, load_sem = refs

    me = lax.axis_index('fsdp')
    weights, first = {}, 0
    for name, shard, got in zip(names, shards, gots):
        weights[name] = Weight(first, TASKS[name], shard, got)
        first += TASKS[name]
    rows, width = dec_ref.shape
    tgt = rows // batch
    src = enc_ref.shape[0] // batch
    row_block = min(ROW_BLOCK, rows)

    def remote(src_ref, dst_ref, kind, ring, bit):
        return pltpu.make_async_remote_copy(src_ref=src_ref, dst_ref=dst_ref, send_sem=send_sem.at[kind, ring], recv_sem=recv_sem.at[kind, ring],
                                            device_id={'fsdp': me ^ bit}, device_id_type=MESH)

    class Task:
        def __init__(self, w, m, ring):
            cols = pl.ds(pl.multiple_of(m * w.width, w.width), w.width)
            own = w.shard.at[:, cols]
            slot = lambda j: w.got.at[j - 1, :, cols]
            low = lambda j: w.got.at[j - 1, pl.ds(0, w.rows // 2), cols]
            high = lambda j: w.got.at[j - 1, pl.ds(w.rows // 2, w.rows // 2), cols]
            self.to_partner = lambda: remote(own, slot(1), 0, ring, 1)
            self.to_x = lambda: remote(own, slot(2), 1, ring, 2)
            self.to_y = lambda: remote(own, slot(4), 2, ring, 4)
            self.relay_y = lambda: remote(low(2), low(6), 3, ring, 4)
            self.relay_x = lambda: remote(high(4), high(6), 4, ring, 2)
            self.swap_x = lambda: remote(slot(2), slot(3), 5, ring, 1)
            self.swap_y = lambda: remote(slot(4), slot(5), 6, ring, 1)
            self.swap_d = lambda: remote(slot(6), slot(7), 7, ring, 1)

    def send(t):
        for copy in (t.to_x, t.to_y, t.to_partner):
            copy().start()

    def arrive(t):
        t.to_partner().wait_recv()
        t.to_x().wait_recv()
        t.relay_y().start()
        t.swap_x().start()
        t.to_y().wait_recv()
        t.relay_x().start()
        t.swap_y().start()

    def pass_on(t):
        t.relay_y().wait_recv()
        t.relay_x().wait_recv()
        t.swap_d().start()

    def finish(t):
        for copy in (t.swap_x, t.swap_y, t.swap_d):
            copy().wait()
        for copy in (t.to_partner, t.to_x, t.to_y, t.relay_y, t.relay_x):
            copy().wait_send()

    def on_task(t, low, high, act):
        for w in weights.values():
            if low < w.first + w.count and w.first < high:
                def run(w=w):
                    act(Task(w, t - w.first, lax.rem(t, RING)))
                if w.first <= low and high <= w.first + w.count:
                    run()
                else:
                    pl.when((t >= w.first) & (t < w.first + w.count))(run)

    def tick(i, low, high):
        on_task(i, low, high, arrive)
        on_task(i + AHEAD, low + AHEAD, high + AHEAD, send)
        on_task(i - PASS, low - PASS, high - PASS, pass_on)
        on_task(i - DONE, low - DONE, high - DONE, finish)

    done = [0]

    def stage_ticks(name):
        low, count = done[0], TICKS[name]
        done[0] = low + count
        return low, count

    def run_ticks(plan, n, steps, one_each=False):
        low, count = plan
        if one_each:
            begin, end = jnp.minimum(low + n, low + count), jnp.minimum(low + n + 1, low + count)
        else:
            begin, end = low + (n * count) // steps, low + ((n + 1) * count) // steps

        @pl.loop(begin, end)
        def _(i):
            tick(i, low, low + count)

    def load(src_ref, dst_ref):
        copy = pltpu.make_async_copy(src_ref, dst_ref, load_sem)
        copy.start()
        copy.wait()

    def norm(which):
        @pl.loop(0, rows // 16)
        def _(r):
            span = pl.ds(pl.multiple_of(r * 16, 16), 16)
            v = x_s[span, :].astype(F32)
            scale = lax.rsqrt(jnp.mean(v * v, axis=-1, keepdims=True) + NORM_EPS)
            big[span, pl.ds(0, width)] = (v * scale * gains[pl.ds(which, 1), :]).astype(BF16)

    def matmul(name, stage, split, store, in_specs=(), ins=(), out_specs=(), outs=()):
        w = weights[name]
        steps, cols = w.count * split, w.width // split
        plan = stage_ticks(stage)

        def body(own, got, *rest):
            n = pl.program_id(0)

            @pl.loop(0, rows // row_block)
            def _(m):
                span = pl.ds(pl.multiple_of(m * row_block, row_block), row_block)
                total = None
                for j in range(N_DEV):
                    part = big[span, pl.ds(pl.multiple_of((me ^ j) * w.rows, 128), w.rows)]
                    term = jnp.dot(part, own[...] if j == 0 else got[j - 1], preferred_element_type=F32)
                    total = term if total is None else total + term
                store(total, span, n, *rest)

            run_ticks(plan, n, steps, stage == 'ff_out')

        pltpu.emit_pipeline(
            body, grid=(steps,),
            in_specs=[pl.BlockSpec((w.rows, cols), lambda n: (0, n)), pl.BlockSpec((N_DEV - 1, w.rows, cols), lambda n: (0, 0, n)), *in_specs],
            out_specs=list(out_specs))(w.shard, w.got, *ins, *outs)

    def project(name, stage, dst_ref, half=0):
        cols = weights[name].width

        def store(total, span, n, dst):
            dst[span, :] = total.astype(BF16)

        matmul(name, stage, 1, store, out_specs=[pl.BlockSpec((rows, cols), lambda n: (half, n))], outs=[dst_ref])

    def residual(name, stage):
        cols = weights[name].width

        def store(total, span, n):
            where = (span, pl.ds(pl.multiple_of(n * cols, cols), cols))
            x_s[where] = (x_s[where].astype(F32) + total.astype(BF16).astype(F32)).astype(BF16)

        matmul(name, stage, 1, store)

    left = lax.broadcasted_iota(jnp.int32, (tgt, 2 * HEAD_DIM), 1) < HEAD_DIM

    def softmax(scores):
        e = jnp.exp(scores - jnp.max(scores, axis=-1, keepdims=True))
        return (e * (1.0 / jnp.sum(e, axis=-1, keepdims=True))).astype(BF16)

    def attend(stage, keys, k_src, v_src, prepare, mask_scores):
        group = min(GROUP, width)
        plan = stage_ticks(stage)
        steps = (width // group) * batch

        def body(q, k, v, c):
            g, b = pl.program_id(0), pl.program_id(1)
            prepare(g, b)
            for pair in range(group // (2 * HEAD_DIM)):
                cols = pl.ds(pair * 2 * HEAD_DIM, 2 * HEAD_DIM)
                q_pair = q[:, cols].astype(F32)
                both = jnp.concatenate([jnp.where(left, q_pair, 0.0), jnp.where(left, 0.0, q_pair)], 0).astype(BF16)
                scores = lax.dot_general(both, k[:, cols], (((1,), (1,)), ((), ())), preferred_element_type=F32)
                prob = jnp.concatenate([softmax(mask_scores(scores[h * tgt:(h + 1) * tgt], 2 * pair + h, b)) for h in range(2)], 0)
                ctx = jnp.dot(prob, v[:, cols], preferred_element_type=F32)
                c[:, cols] = jnp.where(left, ctx[:tgt], ctx[tgt:]).astype(BF16)
            run_ticks(plan, g * batch + b, steps)

        spec = lambda length: pl.BlockSpec((length, group), lambda g, b: (b, g))
        pltpu.emit_pipeline(body, grid=(width // group, batch), in_specs=[spec(tgt), spec(keys), spec(keys)], out_specs=[spec(tgt)])(q_ref, k_src, v_src, c_ref)

    def self_attention():
        heads = min(GROUP, width) // HEAD_DIM
        causal = lax.broadcasted_iota(jnp.int32, (tgt, tgt), 1) <= lax.broadcasted_iota(jnp.int32, (tgt, tgt), 0)

        def prepare(g, b):
            @pl.when(b == 0)
            def _():
                @pl.loop(0, heads)
                def _(h):
                    row = jnp.broadcast_to(dist_s[pl.ds(g * heads + h, 1), :], (tgt, dist_s.shape[1]))
                    bias_s[h] = pltpu.roll(row, 0, 1, stride=1, stride_axis=0)[:, :tgt]

        def mask_scores(scores, h, b):
            allowed = causal & (dec_mask_ref[pl.ds(b, 1), :] > 0)
            return jnp.where(allowed, scores + bias_s[h], MASK_FILL)

        attend('self_attend', tgt, k_ref, v_ref, prepare, mask_scores)

    def cross_attention():
        def mask_scores(scores, h, b):
            return jnp.where(enc_mask_ref[pl.ds(b, 1), :] > 0, scores, MASK_FILL)

        attend('cross_attend', src, ck_ref, cv_ref, lambda g, b: None, mask_scores)

    hidden = big.at[:, pl.ds(0, width)]

    barrier = pltpu.get_barrier_semaphore()
    for j in range(1, N_DEV):
        pl.semaphore_signal(barrier, inc=1, device_id={'fsdp': me ^ j}, device_id_type=MESH)
    pl.semaphore_wait(barrier, N_DEV - 1)

    @pl.loop(0, AHEAD)
    def _(t):
        on_task(t, 0, AHEAD, send)

    def norm_copy(j):
        return pltpu.make_async_remote_copy(src_ref=norm_ref, dst_ref=gain_in.at[me], send_sem=norm_send.at[j], recv_sem=norm_recv.at[j],
                                            device_id={'fsdp': me ^ j}, device_id_type=MESH)

    for j in range(1, N_DEV):
        norm_copy(j).start()
    load(dec_ref, x_s)
    load(norm_ref, gain_in.at[me])
    table = jnp.zeros(dist_s.shape, F32)
    for b in range(NUM_BUCKETS):
        table = table + jnp.where(buckets_ref[...] == b, rel_ref[:, b:b + 1], 0.0)
    dist_s[...] = table
    for j in range(1, N_DEV):
        norm_copy(j).wait()
    per = width // N_DEV
    for d in range(N_DEV):
        gains[:, d * per:(d + 1) * per] = gain_in[d]

    plan = stage_ticks('head')

    @pl.loop(plan[0], plan[0] + plan[1])
    def _(i):
        tick(i, plan[0], plan[0] + plan[1])

    norm(0)
    project('self_q', 'self_q', q_ref)
    project('self_k', 'self_k', k_ref)
    project('self_v', 'self_v', v_ref)
    self_attention()
    load(c_ref, hidden)
    residual('self_o', 'self_o')
    for name, dst in (('cross_k', ck_ref), ('cross_v', cv_ref)):
        for half in range(2):
            load(enc_ref.at[pl.ds(half * rows, rows), :], hidden)
            project(name, f'{name}{half}', dst, half)
    norm(1)
    project('cross_q', 'cross_q', q_ref)
    cross_attention()
    load(c_ref, hidden)
    residual('cross_o', 'cross_o')
    norm(2)

    cols = weights['ff_gate'].width // 2
    block = pl.BlockSpec((rows, cols), lambda n: (0, n))

    def store_gate(total, span, n, g):
        g[span, :] = total.astype(BF16)

    def store_lin(total, span, n, g, z):
        act = jax.nn.gelu(g[span, :].astype(F32), approximate=True)
        z[span, :] = (act * total.astype(BF16).astype(F32)).astype(BF16)

    matmul('ff_gate', 'ff_gate', 2, store_gate, out_specs=[block], outs=[g_ref])
    matmul('ff_lin', 'ff_lin', 2, store_lin, in_specs=[block], ins=[g_ref], out_specs=[block], outs=[z_ref])
    load(z_ref, big)
    cols = weights['ff_out'].width

    def store_out(total, span, n, dst):
        where = (span, pl.ds(pl.multiple_of(n * cols, cols), cols))
        dst[span, :] = (x_s[where].astype(F32) + total.astype(BF16).astype(F32)).astype(BF16)

    matmul('ff_out', 'ff_out', 1, store_out, out_specs=[pl.BlockSpec((rows, cols), lambda n: (0, n))], outs=[out_ref])


def local_layer(dec_in, enc_out, dec_mask, enc_mask, rel_bias, norm_self, self_q, self_k, self_v, self_o, norm_cross, cross_q, cross_k, cross_v, cross_o, norm_ff, ff_gate, ff_lin, ff_out):
    batch, tgt, width = dec_in.shape
    src = enc_out.shape[1]
    rows = batch * tgt
    given = dict(self_q=self_q, self_k=self_k, self_v=self_v, self_o=self_o, cross_k=cross_k, cross_v=cross_v, cross_q=cross_q, cross_o=cross_o, ff_gate=ff_gate, ff_lin=ff_lin, ff_out=ff_out)
    names = list(TASKS)
    shards = [given[n] for n in names]
    lanes = -(-2 * tgt // 128) * 128 if tgt % 128 == 0 else -(-(tgt + 1) // 128) * 128
    norms = jnp.concatenate([jnp.stack([norm_self, norm_cross, norm_ff]).astype(F32), jnp.zeros((5, norm_self.shape[0]), F32)], 0)
    any_spec, vmem_spec = pl.BlockSpec(memory_space=pl.ANY), pl.BlockSpec(memory_space=pltpu.VMEM)
    hbm = lambda *shape: jax.ShapeDtypeStruct(shape, BF16)
    ff = ff_gate.shape[1]
    heads = rel_bias.shape[1]
    outs = [hbm(rows, width)] + [hbm(rows, width)] * 4 + [hbm(batch * src, width)] * 2 + [hbm(rows, ff)] * 2 + [hbm(N_DEV - 1, *s.shape) for s in shards]
    dma = pltpu.SemaphoreType.DMA
    flops = 2 * rows * width * (6 * width + 3 * ff) + 4 * batch * src * width * width
    result = pl.pallas_call(
        lambda *refs: layer_kernel(batch, names, *refs),
        out_shape=outs,
        in_specs=[vmem_spec] * 4 + [any_spec] * (3 + len(shards)),
        out_specs=[any_spec] * len(outs),
        scratch_shapes=[
            pltpu.VMEM((rows, width), BF16),
            pltpu.VMEM((rows, ff), BF16),
            pltpu.VMEM((min(GROUP, width) // HEAD_DIM, tgt, tgt), F32),
            pltpu.VMEM((heads, lanes), F32),
            pltpu.VMEM((N_DEV,) + norms.shape, F32),
            pltpu.VMEM((8, width), F32),
            dma((8, RING)), dma((8, RING)), dma((N_DEV,)), dma((N_DEV,)), dma(()),
        ],
        compiler_params=pltpu.CompilerParams(collective_id=0, has_side_effects=True, vmem_limit_bytes=67_043_328),
        cost_estimate=pl.CostEstimate(flops=flops, bytes_accessed=20 * sum(s.size for s in shards), transcendentals=0),
        name='layer',
    )(jnp.asarray(bucket_row(tgt, lanes)), rel_bias.T, dec_mask, enc_mask, norms, dec_in.reshape(rows, width), enc_out.reshape(batch * src, width), *shards)
    return result[0].reshape(dec_in.shape)


def solution(mesh):
    row_spec = P(('dp', 'fsdp'), None, None)
    mask_spec = P(('dp', 'fsdp'), None)
    weight_spec = P('fsdp', None)
    scale_spec = P('fsdp')
    in_specs = (row_spec, row_spec, mask_spec, mask_spec, P(None, None), scale_spec, weight_spec, weight_spec, weight_spec, weight_spec, scale_spec, weight_spec, weight_spec, weight_spec, weight_spec, scale_spec, weight_spec, weight_spec, weight_spec)
    return jax.shard_map(local_layer, mesh=mesh, in_specs=in_specs, out_specs=row_spec, check_vma=False)
```

```python
import math
import jax
import jax.numpy as jnp
import numpy as np
from jax import lax
from jax.experimental import pallas as pl
from jax.experimental.pallas import tpu as pltpu
from jax.sharding import PartitionSpec as P

MESH = pl.DeviceIdType.MESH
F32, BF16 = jnp.float32, jnp.bfloat16
HEAD_DIM = 64
NUM_BUCKETS = 32
EXACT_BUCKETS = 16
MAX_DISTANCE = 128
NORM_EPS = 1e-6
MASK_FILL = -1e9
N_DEV = 8

AHEAD, PASS, DONE, RING, KINDS = 4, 4, 5, 16, 10
TASKS = {'self_q': 8, 'self_k': 8, 'self_v': 8, 'self_o': 8, 'cross_k': 8, 'cross_v': 8, 'cross_q': 8, 'cross_o': 8, 'ff_gate': 20, 'ff_lin': 20, 'ff_out': 16}
ALL_TASKS = sum(TASKS.values())
TICKS = {'head': DONE + 2, 'self_q': 8, 'self_k': 8, 'self_v': 8, 'self_attend': 6, 'self_o': 6, 'cross_k0': 6, 'cross_k1': 5, 'cross_v0': 6, 'cross_v1': 5,
         'cross_q': 6, 'cross_attend': 10, 'cross_o': 6, 'ff_gate': 12, 'ff_lin': 10}
assert sum(TICKS.values()) == ALL_TASKS - TASKS['ff_out'] + DONE
ROW_BLOCK = 512
GROUP = 512


def bucket_ids(length):
    return [offset if offset < EXACT_BUCKETS else min(NUM_BUCKETS - 1, EXACT_BUCKETS + int(math.log(offset / EXACT_BUCKETS) / math.log(MAX_DISTANCE / EXACT_BUCKETS) * (NUM_BUCKETS - EXACT_BUCKETS))) for offset in range(length)]


def bucket_column(length, lanes):
    ids = bucket_ids(length)
    return np.array([[ids[min((lanes - m) % lanes, length - 1)]] for m in range(lanes)], np.int32)


class Weight:
    def __init__(self, first, count, shard, got):
        self.first, self.count, self.shard, self.got = first, count, shard, got
        self.rows, self.width = shard.shape[0], shard.shape[1] // count


def layer_kernel(batch, names, buckets_ref, rel_ref, dec_mask_ref, enc_mask_ref, norm_ref, dec_ref, enc_ref, *refs):
    n_w = len(names)
    shards, refs = refs[:n_w], refs[n_w:]
    out_ref, q_ref, k_ref, v_ref, c_ref, ck_ref, cv_ref, g_ref, z_ref = refs[:9]
    gots, refs = refs[9:9 + n_w], refs[9 + n_w:]
    x_s, big, bias_s, dist_s, gain_in, gains, send_sem, recv_sem, norm_send, norm_recv, load_sem = refs

    me = lax.axis_index('fsdp')
    weights, first = {}, 0
    for name, shard, got in zip(names, shards, gots):
        weights[name] = Weight(first, TASKS[name], shard, got)
        first += TASKS[name]
    rows, width = dec_ref.shape
    tgt = rows // batch
    src = enc_ref.shape[0] // batch
    row_block = min(ROW_BLOCK, rows)

    def remote(src_ref, dst_ref, kind, ring, bit):
        return pltpu.make_async_remote_copy(src_ref=src_ref, dst_ref=dst_ref, send_sem=send_sem.at[kind, ring], recv_sem=recv_sem.at[kind, ring],
                                            device_id={'fsdp': me ^ bit}, device_id_type=MESH)

    class Task:
        def __init__(self, w, m, ring):
            cols = pl.ds(pl.multiple_of(m * w.width, w.width), w.width)
            own = w.shard.at[:, cols]
            slot = lambda j: w.got.at[j - 1, :, cols]
            bottom, top = pl.ds(0, w.rows // 2), pl.ds(w.rows // 2, w.rows // 2)
            low = lambda j: w.got.at[j - 1, bottom, cols]
            high = lambda j: w.got.at[j - 1, top, cols]
            self.to_partner = lambda: remote(own, slot(1), 0, ring, 1)
            self.first_x = lambda: remote(w.shard.at[bottom, cols], low(2), 1, ring, 2)
            self.first_y = lambda: remote(w.shard.at[top, cols], high(4), 2, ring, 4)
            self.rest_x = lambda: remote(w.shard.at[top, cols], high(2), 3, ring, 2)
            self.rest_y = lambda: remote(w.shard.at[bottom, cols], low(4), 4, ring, 4)
            self.relay_y = lambda: remote(low(2), low(6), 5, ring, 4)
            self.relay_x = lambda: remote(high(4), high(6), 6, ring, 2)
            self.swap_x = lambda: remote(slot(2), slot(3), 7, ring, 1)
            self.swap_y = lambda: remote(slot(4), slot(5), 8, ring, 1)
            self.swap_d = lambda: remote(slot(6), slot(7), 9, ring, 1)

    def send(t):
        for copy in (t.first_x, t.first_y, t.to_partner):
            copy().start()

    def arrive(t):
        t.to_partner().wait_recv()
        t.first_x().wait_recv()
        t.relay_y().start()
        t.rest_y().start()
        t.first_y().wait_recv()
        t.relay_x().start()
        t.rest_x().start()

    def pass_on_diagonal(t):
        t.relay_y().wait_recv()
        t.relay_x().wait_recv()
        t.swap_d().start()

    def pass_on_rest(t):
        t.rest_x().wait_recv()
        t.swap_x().start()
        t.rest_y().wait_recv()
        t.swap_y().start()

    def pass_on(t):
        pass_on_diagonal(t)
        pass_on_rest(t)

    def wait_sends(t):
        for copy in (t.to_partner, t.first_x, t.first_y, t.rest_x, t.rest_y, t.relay_y, t.relay_x, t.swap_x, t.swap_y, t.swap_d):
            copy().wait_send()

    def finish(t):
        for copy in (t.swap_x, t.swap_y, t.swap_d):
            copy().wait_recv()
        wait_sends(t)

    def on_task(t, low, high, act, among=None):
        for w in among or weights.values():
            if low < w.first + w.count and w.first < high:
                def run(w=w):
                    act(Task(w, t - w.first, lax.rem(t, RING)))
                if w.first <= low and high <= w.first + w.count:
                    run()
                else:
                    pl.when((t >= w.first) & (t < w.first + w.count))(run)

    def tick(i, low, high):
        on_task(i, low, high, arrive)
        on_task(i + AHEAD, low + AHEAD, high + AHEAD, send)
        streamed = [w for name, w in weights.items() if name != 'ff_out']
        on_task(i - PASS, low - PASS, high - PASS, pass_on, streamed)
        on_task(i - DONE, low - DONE, high - DONE, finish, streamed)

    done = [0]

    def stage_ticks(name):
        low, count = done[0], TICKS[name]
        done[0] = low + count
        return low, count

    def ticks_before(plan, n, steps, least=min):
        low, count = plan
        spread = steps if count == steps else max(steps - 4, 1)
        return low + least((n * count) // spread, count)

    def run_ticks(plan, n, steps):
        with jax.named_scope('ticks'):
            @pl.loop(ticks_before(plan, n, steps, jnp.minimum), ticks_before(plan, n + 1, steps, jnp.minimum))
            def _(i):
                tick(i, plan[0], plan[0] + plan[1])

    def load(src_ref, dst_ref):
        copy = pltpu.make_async_copy(src_ref, dst_ref, load_sem)
        copy.start()
        copy.wait()

    def norm(which):
        @pl.loop(0, rows // 16)
        def _(r):
            span = pl.ds(pl.multiple_of(r * 16, 16), 16)
            v = x_s[span, :].astype(F32)
            scale = lax.rsqrt(jnp.mean(v * v, axis=-1, keepdims=True) + NORM_EPS)
            big[span, pl.ds(0, width)] = (v * scale * gains[pl.ds(which, 1), :]).astype(BF16)

    def matmul(name, stage, split, store, in_specs=(), ins=(), out_specs=(), outs=()):
        w = weights[name]
        steps, cols = w.count * split, w.width // split
        plan = stage_ticks(stage)
        for n in range(steps):
            assert ticks_before(plan, n, steps) > w.first + min(n + 1, steps - 1) // split + DONE

        def body(own, got, *rest):
            n = pl.program_id(0)

            @pl.loop(0, rows // row_block)
            def _(m):
                span = pl.ds(pl.multiple_of(m * row_block, row_block), row_block)
                total = None
                for j in range(N_DEV):
                    part = big[span, pl.ds(pl.multiple_of((me ^ j) * w.rows, 128), w.rows)]
                    term = jnp.dot(part, own[...] if j == 0 else got[j - 1], preferred_element_type=F32)
                    total = term if total is None else total + term
                store(total, span, n, *rest)

            run_ticks(plan, n, steps)

        with jax.named_scope(stage):
            pltpu.emit_pipeline(
                body, grid=(steps,),
                in_specs=[pl.BlockSpec((w.rows, cols), lambda n: (0, n)), pl.BlockSpec((N_DEV - 1, w.rows, cols), lambda n: (0, 0, n)), *in_specs],
                out_specs=list(out_specs))(w.shard, w.got, *ins, *outs)

    def project(name, stage, dst_ref, half=0):
        cols = weights[name].width

        def store(total, span, n, dst):
            dst[span, :] = total.astype(BF16)

        matmul(name, stage, 1, store, out_specs=[pl.BlockSpec((rows, cols), lambda n: (half, n))], outs=[dst_ref])

    def residual(name, stage):
        cols = weights[name].width

        def store(total, span, n):
            where = (span, pl.ds(pl.multiple_of(n * cols, cols), cols))
            x_s[where] = (x_s[where].astype(F32) + total.astype(BF16).astype(F32)).astype(BF16)

        matmul(name, stage, 1, store)

    left = lax.broadcasted_iota(jnp.int32, (tgt, 2 * HEAD_DIM), 1) < HEAD_DIM

    def softmax(scores):
        e = jnp.exp(scores - jnp.max(scores, axis=-1, keepdims=True))
        return (e * (1.0 / jnp.sum(e, axis=-1, keepdims=True))).astype(BF16)

    def attend(stage, keys, k_src, v_src, prepare, mask_scores):
        group = min(GROUP, width)
        plan = stage_ticks(stage)
        steps = (width // group) * batch

        def body(q, k, v, c):
            g, b = pl.program_id(0), pl.program_id(1)
            prepare(g, b)
            for pair in range(group // (2 * HEAD_DIM)):
                cols = pl.ds(pair * 2 * HEAD_DIM, 2 * HEAD_DIM)
                q_pair = q[:, cols].astype(F32)
                both = jnp.concatenate([jnp.where(left, q_pair, 0.0), jnp.where(left, 0.0, q_pair)], 0).astype(BF16)
                scores = lax.dot_general(both, k[:, cols], (((1,), (1,)), ((), ())), preferred_element_type=F32)
                prob = jnp.concatenate([softmax(mask_scores(scores[h * tgt:(h + 1) * tgt], 2 * pair + h, b)) for h in range(2)], 0)
                ctx = jnp.dot(prob, v[:, cols], preferred_element_type=F32)
                c[:, cols] = jnp.where(left, ctx[:tgt], ctx[tgt:]).astype(BF16)
            run_ticks(plan, g * batch + b, steps)

        spec = lambda length: pl.BlockSpec((length, group), lambda g, b: (b, g))
        with jax.named_scope(stage):
            pltpu.emit_pipeline(body, grid=(width // group, batch), in_specs=[spec(tgt), spec(keys), spec(keys)], out_specs=[spec(tgt)])(q_ref, k_src, v_src, c_ref)

    def self_attention():
        heads = min(GROUP, width) // HEAD_DIM
        causal = lax.broadcasted_iota(jnp.int32, (tgt, tgt), 1) <= lax.broadcasted_iota(jnp.int32, (tgt, tgt), 0)

        def prepare(g, b):
            @pl.when(b == 0)
            def _():
                @pl.loop(0, heads)
                def _(h):
                    row = jnp.broadcast_to(dist_s[pl.ds(g * heads + h, 1), :], (tgt, dist_s.shape[1]))
                    bias_s[h] = pltpu.roll(row, 0, 1, stride=1, stride_axis=0)[:, :tgt]

        def mask_scores(scores, h, b):
            allowed = causal & (dec_mask_ref[pl.ds(b, 1), :] > 0)
            return jnp.where(allowed, scores + bias_s[h], MASK_FILL)

        attend('self_attend', tgt, k_ref, v_ref, prepare, mask_scores)

    def cross_attention():
        def mask_scores(scores, h, b):
            return jnp.where(enc_mask_ref[pl.ds(b, 1), :] > 0, scores, MASK_FILL)

        attend('cross_attend', src, ck_ref, cv_ref, lambda g, b: None, mask_scores)

    hidden = big.at[:, pl.ds(0, width)]

    barrier = pltpu.get_barrier_semaphore()
    for j in range(1, N_DEV):
        pl.semaphore_signal(barrier, inc=1, device_id={'fsdp': me ^ j}, device_id_type=MESH)
    pl.semaphore_wait(barrier, N_DEV - 1)

    @pl.loop(0, AHEAD)
    def _(t):
        on_task(t, 0, AHEAD, send)

    def norm_copy(j):
        return pltpu.make_async_remote_copy(src_ref=norm_ref, dst_ref=gain_in.at[me], send_sem=norm_send.at[j], recv_sem=norm_recv.at[j],
                                            device_id={'fsdp': me ^ j}, device_id_type=MESH)

    for j in range(1, N_DEV):
        norm_copy(j).start()
    load(dec_ref, x_s)
    load(norm_ref, gain_in.at[me])
    table = jnp.zeros((buckets_ref.shape[0], rel_ref.shape[1]), F32)
    for b in range(NUM_BUCKETS):
        table = table + jnp.where(buckets_ref[...] == b, rel_ref[b:b + 1, :], 0.0)
    dist_s[...] = table.T
    for j in range(1, N_DEV):
        norm_copy(j).wait()
    per = width // N_DEV
    for d in range(N_DEV):
        gains[:, d * per:(d + 1) * per] = gain_in[d]

    plan = stage_ticks('head')
    with jax.named_scope('head'):
        @pl.loop(plan[0], plan[0] + plan[1])
        def _(i):
            tick(i, plan[0], plan[0] + plan[1])

    norm(0)
    project('self_q', 'self_q', q_ref)
    project('self_k', 'self_k', k_ref)
    project('self_v', 'self_v', v_ref)
    self_attention()
    load(c_ref, hidden)
    residual('self_o', 'self_o')
    for name, dst in (('cross_k', ck_ref), ('cross_v', cv_ref)):
        for half in range(2):
            load(enc_ref.at[pl.ds(half * rows, rows), :], hidden)
            project(name, f'{name}{half}', dst, half)
    norm(1)
    project('cross_q', 'cross_q', q_ref)
    cross_attention()
    load(c_ref, hidden)
    residual('cross_o', 'cross_o')
    norm(2)

    cols = weights['ff_gate'].width // 2
    block = pl.BlockSpec((rows, cols), lambda n: (0, n))

    def store_gate(total, span, n, g):
        g[span, :] = total.astype(BF16)

    def store_lin(total, span, n, g, z):
        act = jax.nn.gelu(g[span, :].astype(F32), approximate=True)
        z[span, :] = (act * total.astype(BF16).astype(F32)).astype(BF16)

    matmul('ff_gate', 'ff_gate', 2, store_gate, out_specs=[block], outs=[g_ref])
    matmul('ff_lin', 'ff_lin', 2, store_lin, in_specs=[block], ins=[g_ref], out_specs=[block], outs=[z_ref])
    load(z_ref, big)
    w = weights['ff_out']
    last = w.first + w.count

    def ff_out_loop(early, late, total, outs, early_sem, late_sem, out_sem):
        cols = w.width

        def span_of(m):
            return pl.ds(pl.multiple_of(m * row_block, row_block), row_block)

        def product(span, buf, slots):
            terms = [jnp.dot(big[span, pl.ds(pl.multiple_of((me ^ j) * w.rows, 128), w.rows)], buf[p], preferred_element_type=F32) for p, j in enumerate(slots)]
            return sum(terms[1:], terms[0])

        @pl.loop(0, w.count)
        def _(n):
            where = pl.ds(pl.multiple_of(n * cols, cols), cols)
            t = Task(w, n, lax.rem(w.first + n, RING))

            def fetch(j, buf, p, sem):
                return pltpu.make_async_copy(w.shard.at[:, where] if j == 0 else w.got.at[j - 1, :, where], buf.at[p], sem.at[p])

            def out_copy(k):
                return pltpu.make_async_copy(outs.at[lax.rem(k, 2)], out_ref.at[:, pl.ds(pl.multiple_of(k * cols, cols), cols)], out_sem.at[lax.rem(k, 2)])

            first, second = (0, 1, 6, 7), (2, 4, 3, 5)
            for p in (0, 1):
                fetch(first[p], early, p, early_sem).start()
            pass_on_diagonal(t)
            fetch(6, early, 2, early_sem).start()
            t.swap_d().wait_recv()
            fetch(7, early, 3, early_sem).start()
            for p, j in enumerate(first):
                fetch(j, early, p, early_sem).wait()

            @pl.loop(0, rows // row_block)
            def _(m):
                total[span_of(m), :] = product(span_of(m), early, first)

            @pl.when(n >= 2)
            def _():
                out_copy(n - 2).wait()

            pass_on_rest(t)
            for p in (0, 1):
                fetch(second[p], late, p, late_sem).start()
            t.swap_x().wait_recv()
            fetch(3, late, 2, late_sem).start()
            t.swap_y().wait_recv()
            fetch(5, late, 3, late_sem).start()
            for p, j in enumerate(second):
                fetch(j, late, p, late_sem).wait()

            @pl.loop(0, rows // row_block)
            def _(m):
                span = span_of(m)
                update = (total[span, :] + product(span, late, second)).astype(BF16)
                outs[lax.rem(n, 2), span, :] = (x_s[span, where].astype(F32) + update.astype(F32)).astype(BF16)

            out_copy(n).start()
            wait_sends(t)
            begin = w.first + DONE
            on_task(begin + n, begin, last + DONE, arrive, [w])
            on_task(begin + AHEAD + n, begin + AHEAD, last + DONE + AHEAD, send, [w])

            @pl.when(n == w.count - 1)
            def _():
                out_copy(n - 1).wait()
                out_copy(n).wait()

    dma = pltpu.SemaphoreType.DMA
    with jax.named_scope('ff_out'):
        pl.run_scoped(ff_out_loop, pltpu.VMEM((4, w.rows, w.width), BF16), pltpu.VMEM((4, w.rows, w.width), BF16), pltpu.VMEM((rows, w.width), F32),
                      pltpu.VMEM((2, rows, w.width), BF16), dma((4,)), dma((4,)), dma((2,)))


def local_layer(dec_in, enc_out, dec_mask, enc_mask, rel_bias, norm_self, self_q, self_k, self_v, self_o, norm_cross, cross_q, cross_k, cross_v, cross_o, norm_ff, ff_gate, ff_lin, ff_out):
    batch, tgt, width = dec_in.shape
    src = enc_out.shape[1]
    rows = batch * tgt
    given = dict(self_q=self_q, self_k=self_k, self_v=self_v, self_o=self_o, cross_k=cross_k, cross_v=cross_v, cross_q=cross_q, cross_o=cross_o, ff_gate=ff_gate, ff_lin=ff_lin, ff_out=ff_out)
    names = list(TASKS)
    shards = [given[n] for n in names]
    lanes = -(-2 * tgt // 128) * 128 if tgt % 128 == 0 else -(-(tgt + 1) // 128) * 128
    which = lax.broadcasted_iota(jnp.int32, (8, norm_self.shape[0]), 0)
    norms = jnp.where(which == 0, norm_self[None], jnp.where(which == 1, norm_cross[None], norm_ff[None])).astype(F32)
    any_spec, vmem_spec = pl.BlockSpec(memory_space=pl.ANY), pl.BlockSpec(memory_space=pltpu.VMEM)
    hbm = lambda *shape: jax.ShapeDtypeStruct(shape, BF16)
    ff = ff_gate.shape[1]
    heads = rel_bias.shape[1]
    outs = [hbm(rows, width)] + [hbm(rows, width)] * 4 + [hbm(batch * src, width)] * 2 + [hbm(rows, ff)] * 2 + [hbm(N_DEV - 1, *s.shape) for s in shards]
    dma = pltpu.SemaphoreType.DMA
    flops = 2 * rows * width * (6 * width + 3 * ff) + 4 * batch * src * width * width
    result = pl.pallas_call(
        lambda *refs: layer_kernel(batch, names, *refs),
        out_shape=outs,
        in_specs=[vmem_spec] * 4 + [any_spec] * (3 + len(shards)),
        out_specs=[any_spec] * len(outs),
        scratch_shapes=[
            pltpu.VMEM((rows, width), BF16),
            pltpu.VMEM((rows, ff), BF16),
            pltpu.VMEM((min(GROUP, width) // HEAD_DIM, tgt, tgt), F32),
            pltpu.VMEM((heads, lanes), F32),
            pltpu.VMEM((N_DEV,) + norms.shape, F32),
            pltpu.VMEM((8, width), F32),
            dma((KINDS, RING)), dma((KINDS, RING)), dma((N_DEV,)), dma((N_DEV,)), dma(()),
        ],
        compiler_params=pltpu.CompilerParams(collective_id=0, has_side_effects=True, vmem_limit_bytes=67_043_328),
        cost_estimate=pl.CostEstimate(flops=flops, bytes_accessed=20 * sum(s.size for s in shards), transcendentals=0),
        name='layer',
    )(jnp.asarray(bucket_column(tgt, lanes)), rel_bias, dec_mask, enc_mask, norms, dec_in.reshape(rows, width), enc_out.reshape(batch * src, width), *shards)
    return result[0].reshape(dec_in.shape)


def solution(mesh):
    row_spec = P(('dp', 'fsdp'), None, None)
    mask_spec = P(('dp', 'fsdp'), None)
    weight_spec = P('fsdp', None)
    scale_spec = P('fsdp')
    in_specs = (row_spec, row_spec, mask_spec, mask_spec, P(None, None), scale_spec, weight_spec, weight_spec, weight_spec, weight_spec, scale_spec, weight_spec, weight_spec, weight_spec, weight_spec, scale_spec, weight_spec, weight_spec, weight_spec)
    return jax.shard_map(local_layer, mesh=mesh, in_specs=in_specs, out_specs=row_spec, check_vma=False)
```

```python
import math
import jax
import jax.numpy as jnp
import numpy as np
from jax import lax
from jax.experimental import pallas as pl
from jax.experimental.pallas import tpu as pltpu
from jax.sharding import PartitionSpec as P

MESH = pl.DeviceIdType.MESH
F32, BF16 = jnp.float32, jnp.bfloat16
HEAD_DIM = 64
NUM_BUCKETS = 32
EXACT_BUCKETS = 16
MAX_DISTANCE = 128
NORM_EPS = 1e-6
MASK_FILL = -1e9
N_DEV = 8

AHEAD, PASS, DONE, RING, KINDS = 4, 4, 5, 16, 10
TASKS = {'self_q': 8, 'self_k': 8, 'self_v': 8, 'self_o': 8, 'cross_k': 8, 'cross_v': 8, 'cross_q': 8, 'cross_o': 8, 'ff_gate': 20, 'ff_lin': 20, 'ff_out': 16}
ALL_TASKS = sum(TASKS.values())
TICKS = {'head': DONE + 2, 'self_q': 8, 'self_k': 8, 'self_v': 8, 'self_attend': 6, 'self_o': 6, 'cross_k0': 6, 'cross_k1': 5, 'cross_v0': 6, 'cross_v1': 5,
         'cross_q': 6, 'cross_attend': 10, 'cross_o': 6, 'ff_gate': 12, 'ff_lin': 10}
assert sum(TICKS.values()) == ALL_TASKS - TASKS['ff_out'] + DONE
ROW_BLOCK = 512
GROUP = 512


def bucket_ids(length):
    return [offset if offset < EXACT_BUCKETS else min(NUM_BUCKETS - 1, EXACT_BUCKETS + int(math.log(offset / EXACT_BUCKETS) / math.log(MAX_DISTANCE / EXACT_BUCKETS) * (NUM_BUCKETS - EXACT_BUCKETS))) for offset in range(length)]


def bucket_column(length, lanes):
    ids = bucket_ids(length)
    return np.array([[ids[min((lanes - m) % lanes, length - 1)]] for m in range(lanes)], np.int32)


class Weight:
    def __init__(self, first, count, shard, got):
        self.first, self.count, self.shard, self.got = first, count, shard, got
        self.rows, self.width = shard.shape[0], shard.shape[1] // count


def layer_kernel(batch, names, buckets_ref, rel_ref, dec_mask_ref, enc_mask_ref, norm_ref, dec_ref, enc_ref, *refs):
    n_w = len(names)
    shards, refs = refs[:n_w], refs[n_w:]
    out_ref, q_ref, k_ref, v_ref, c_ref, ck_ref, cv_ref, g_ref, z_ref = refs[:9]
    gots, refs = refs[9:9 + n_w], refs[9 + n_w:]
    x_s, big, bias_s, dist_s, gain_in, gains, send_sem, recv_sem, norm_send, norm_recv, load_sem = refs

    me = lax.axis_index('fsdp')
    weights, first = {}, 0
    for name, shard, got in zip(names, shards, gots):
        weights[name] = Weight(first, TASKS[name], shard, got)
        first += TASKS[name]
    rows, width = dec_ref.shape
    tgt = rows // batch
    src = enc_ref.shape[0] // batch
    row_block = min(ROW_BLOCK, rows)

    def remote(src_ref, dst_ref, kind, ring, bit):
        return pltpu.make_async_remote_copy(src_ref=src_ref, dst_ref=dst_ref, send_sem=send_sem.at[kind, ring], recv_sem=recv_sem.at[kind, ring],
                                            device_id={'fsdp': me ^ bit}, device_id_type=MESH)

    class Task:
        def __init__(self, w, m, ring):
            cols = pl.ds(pl.multiple_of(m * w.width, w.width), w.width)
            own = w.shard.at[:, cols]
            slot = lambda j: w.got.at[j - 1, :, cols]
            bottom, top = pl.ds(0, w.rows // 2), pl.ds(w.rows // 2, w.rows // 2)
            low = lambda j: w.got.at[j - 1, bottom, cols]
            high = lambda j: w.got.at[j - 1, top, cols]
            self.to_partner = lambda: remote(own, slot(1), 0, ring, 1)
            self.first_x = lambda: remote(w.shard.at[bottom, cols], low(2), 1, ring, 2)
            self.first_y = lambda: remote(w.shard.at[top, cols], high(4), 2, ring, 4)
            self.rest_x = lambda: remote(w.shard.at[top, cols], high(2), 3, ring, 2)
            self.rest_y = lambda: remote(w.shard.at[bottom, cols], low(4), 4, ring, 4)
            self.relay_y = lambda: remote(low(2), low(6), 5, ring, 4)
            self.relay_x = lambda: remote(high(4), high(6), 6, ring, 2)
            self.swap_x = lambda: remote(slot(2), slot(3), 7, ring, 1)
            self.swap_y = lambda: remote(slot(4), slot(5), 8, ring, 1)
            self.swap_d = lambda: remote(slot(6), slot(7), 9, ring, 1)

    def send(t):
        for copy in (t.first_x, t.first_y, t.to_partner):
            copy().start()

    def arrive(t):
        t.to_partner().wait_recv()
        t.first_x().wait_recv()
        t.relay_y().start()
        t.rest_y().start()
        t.first_y().wait_recv()
        t.relay_x().start()
        t.rest_x().start()

    def pass_on_diagonal(t):
        t.relay_y().wait_recv()
        t.relay_x().wait_recv()
        t.swap_d().start()

    def pass_on_rest(t):
        t.rest_x().wait_recv()
        t.swap_x().start()
        t.rest_y().wait_recv()
        t.swap_y().start()

    def pass_on(t):
        pass_on_diagonal(t)
        pass_on_rest(t)

    def wait_sends(t):
        for copy in (t.to_partner, t.first_x, t.first_y, t.rest_x, t.rest_y, t.relay_y, t.relay_x, t.swap_x, t.swap_y, t.swap_d):
            copy().wait_send()

    def finish(t):
        for copy in (t.swap_x, t.swap_y, t.swap_d):
            copy().wait_recv()
        wait_sends(t)

    def on_task(t, low, high, act, among=None):
        for w in among or weights.values():
            if low < w.first + w.count and w.first < high:
                def run(w=w):
                    act(Task(w, t - w.first, lax.rem(t, RING)))
                if w.first <= low and high <= w.first + w.count:
                    run()
                else:
                    pl.when((t >= w.first) & (t < w.first + w.count))(run)

    def tick(i, low, high):
        on_task(i, low, high, arrive)
        on_task(i + AHEAD, low + AHEAD, high + AHEAD, send)
        streamed = [w for name, w in weights.items() if name != 'ff_out']
        on_task(i - PASS, low - PASS, high - PASS, pass_on, streamed)
        on_task(i - DONE, low - DONE, high - DONE, finish, streamed)

    done = [0]

    def stage_ticks(name):
        low, count = done[0], TICKS[name]
        done[0] = low + count
        return low, count

    def ticks_before(plan, n, steps, least=min):
        low, count = plan
        spread = steps if count == steps else max(steps - 4, 1)
        return low + least((n * count) // spread, count)

    def run_ticks(plan, n, steps):
        with jax.named_scope('ticks'):
            @pl.loop(ticks_before(plan, n, steps, jnp.minimum), ticks_before(plan, n + 1, steps, jnp.minimum))
            def _(i):
                tick(i, plan[0], plan[0] + plan[1])

    def load(src_ref, dst_ref):
        copy = pltpu.make_async_copy(src_ref, dst_ref, load_sem)
        copy.start()
        copy.wait()

    def norm(which):
        @pl.loop(0, rows // 16)
        def _(r):
            span = pl.ds(pl.multiple_of(r * 16, 16), 16)
            v = x_s[span, :].astype(F32)
            scale = lax.rsqrt(jnp.mean(v * v, axis=-1, keepdims=True) + NORM_EPS)
            big[span, pl.ds(0, width)] = (v * scale * gains[pl.ds(which, 1), :]).astype(BF16)

    def matmul(name, stage, split, store, in_specs=(), ins=(), out_specs=(), outs=()):
        w = weights[name]
        steps, cols = w.count * split, w.width // split
        plan = stage_ticks(stage)
        for n in range(steps):
            assert ticks_before(plan, n, steps) > w.first + min(n + 1, steps - 1) // split + DONE

        def body(own, got, *rest):
            n = pl.program_id(0)

            @pl.loop(0, rows // row_block)
            def _(m):
                span = pl.ds(pl.multiple_of(m * row_block, row_block), row_block)
                total = None
                for j in range(N_DEV):
                    part = big[span, pl.ds(pl.multiple_of((me ^ j) * w.rows, 128), w.rows)]
                    term = jnp.dot(part, own[...] if j == 0 else got[j - 1], preferred_element_type=F32)
                    total = term if total is None else total + term
                store(total, span, n, *rest)

            run_ticks(plan, n, steps)

        with jax.named_scope(stage):
            pltpu.emit_pipeline(
                body, grid=(steps,),
                in_specs=[pl.BlockSpec((w.rows, cols), lambda n: (0, n)), pl.BlockSpec((N_DEV - 1, w.rows, cols), lambda n: (0, 0, n)), *in_specs],
                out_specs=list(out_specs))(w.shard, w.got, *ins, *outs)

    def project(name, stage, dst_ref, half=0):
        cols = weights[name].width

        def store(total, span, n, dst):
            dst[span, :] = total.astype(BF16)

        matmul(name, stage, 1, store, out_specs=[pl.BlockSpec((rows, cols), lambda n: (half, n))], outs=[dst_ref])

    def residual(name, stage):
        cols = weights[name].width

        def store(total, span, n):
            where = (span, pl.ds(pl.multiple_of(n * cols, cols), cols))
            x_s[where] = (x_s[where].astype(F32) + total.astype(BF16).astype(F32)).astype(BF16)

        matmul(name, stage, 1, store)

    left = lax.broadcasted_iota(jnp.int32, (tgt, 2 * HEAD_DIM), 1) < HEAD_DIM

    def softmax(scores):
        e = jnp.exp(scores - jnp.max(scores, axis=-1, keepdims=True))
        return (e * (1.0 / jnp.sum(e, axis=-1, keepdims=True))).astype(BF16)

    def attend(stage, keys, k_src, v_src, prepare, mask_scores):
        group = min(GROUP, width)
        plan = stage_ticks(stage)
        steps = (width // group) * batch

        def body(q, k, v, c):
            g, b = pl.program_id(0), pl.program_id(1)
            prepare(g, b)
            for pair in range(group // (2 * HEAD_DIM)):
                cols = pl.ds(pair * 2 * HEAD_DIM, 2 * HEAD_DIM)
                q_pair = q[:, cols].astype(F32)
                both = jnp.concatenate([jnp.where(left, q_pair, 0.0), jnp.where(left, 0.0, q_pair)], 0).astype(BF16)
                scores = lax.dot_general(both, k[:, cols], (((1,), (1,)), ((), ())), preferred_element_type=F32)
                prob = jnp.concatenate([softmax(mask_scores(scores[h * tgt:(h + 1) * tgt], 2 * pair + h, b)) for h in range(2)], 0)
                ctx = jnp.dot(prob, v[:, cols], preferred_element_type=F32)
                c[:, cols] = jnp.where(left, ctx[:tgt], ctx[tgt:]).astype(BF16)
            run_ticks(plan, g * batch + b, steps)

        spec = lambda length: pl.BlockSpec((length, group), lambda g, b: (b, g))
        with jax.named_scope(stage):
            pltpu.emit_pipeline(body, grid=(width // group, batch), in_specs=[spec(tgt), spec(keys), spec(keys)], out_specs=[spec(tgt)])(q_ref, k_src, v_src, c_ref)

    def self_attention():
        heads = min(GROUP, width) // HEAD_DIM
        causal = lax.broadcasted_iota(jnp.int32, (tgt, tgt), 1) <= lax.broadcasted_iota(jnp.int32, (tgt, tgt), 0)

        def prepare(g, b):
            @pl.when(b == 0)
            def _():
                @pl.loop(0, heads)
                def _(h):
                    row = jnp.broadcast_to(dist_s[pl.ds(g * heads + h, 1), :], (tgt, dist_s.shape[1]))
                    bias_s[h] = pltpu.roll(row, 0, 1, stride=1, stride_axis=0)[:, :tgt]

        def mask_scores(scores, h, b):
            allowed = causal & (dec_mask_ref[pl.ds(b, 1), :] > 0)
            return jnp.where(allowed, scores + bias_s[h], MASK_FILL)

        attend('self_attend', tgt, k_ref, v_ref, prepare, mask_scores)

    def cross_attention():
        def mask_scores(scores, h, b):
            return jnp.where(enc_mask_ref[pl.ds(b, 1), :] > 0, scores, MASK_FILL)

        attend('cross_attend', src, ck_ref, cv_ref, lambda g, b: None, mask_scores)

    hidden = big.at[:, pl.ds(0, width)]

    barrier = pltpu.get_barrier_semaphore()
    for j in range(1, N_DEV):
        pl.semaphore_signal(barrier, inc=1, device_id={'fsdp': me ^ j}, device_id_type=MESH)
    pl.semaphore_wait(barrier, N_DEV - 1)

    @pl.loop(0, AHEAD)
    def _(t):
        on_task(t, 0, AHEAD, send)

    def norm_copy(j):
        return pltpu.make_async_remote_copy(src_ref=norm_ref, dst_ref=gain_in.at[me], send_sem=norm_send.at[j], recv_sem=norm_recv.at[j],
                                            device_id={'fsdp': me ^ j}, device_id_type=MESH)

    for j in range(1, N_DEV):
        norm_copy(j).start()
    load_dec = pltpu.make_async_copy(dec_ref, x_s, load_sem)
    load_dec.start()
    load_norm = pltpu.make_async_copy(norm_ref, gain_in.at[me], norm_send.at[0])
    load_norm.start()
    plan = stage_ticks('head')

    def head_ticks(begin, end):
        with jax.named_scope('head'):
            @pl.loop(begin, end)
            def _(i):
                tick(i, plan[0], plan[0] + plan[1])

    head_ticks(0, 2)
    table = jnp.zeros((buckets_ref.shape[0], rel_ref.shape[1]), F32)
    for b in range(NUM_BUCKETS):
        table = table + jnp.where(buckets_ref[...] == b, rel_ref[b:b + 1, :], 0.0)
    dist_s[...] = table.T
    head_ticks(2, 4)
    for j in range(1, N_DEV):
        norm_copy(j).wait()
    load_norm.wait()
    per = width // N_DEV
    for d in range(N_DEV):
        gains[:, d * per:(d + 1) * per] = gain_in[d]
    load_dec.wait()
    norm(0)
    head_ticks(4, plan[1])

    project('self_q', 'self_q', q_ref)
    project('self_k', 'self_k', k_ref)
    project('self_v', 'self_v', v_ref)
    self_attention()
    load(c_ref, hidden)
    residual('self_o', 'self_o')
    for name, dst in (('cross_k', ck_ref), ('cross_v', cv_ref)):
        for half in range(2):
            load(enc_ref.at[pl.ds(half * rows, rows), :], hidden)
            project(name, f'{name}{half}', dst, half)
    norm(1)
    project('cross_q', 'cross_q', q_ref)
    cross_attention()
    load(c_ref, hidden)
    residual('cross_o', 'cross_o')
    norm(2)

    cols = weights['ff_gate'].width // 2
    block = pl.BlockSpec((rows, cols), lambda n: (0, n))

    def store_gate(total, span, n, g):
        g[span, :] = total.astype(BF16)

    def store_lin(total, span, n, g, z):
        act = jax.nn.gelu(g[span, :].astype(F32), approximate=True)
        z[span, :] = (act * total.astype(BF16).astype(F32)).astype(BF16)

    matmul('ff_gate', 'ff_gate', 2, store_gate, out_specs=[block], outs=[g_ref])
    matmul('ff_lin', 'ff_lin', 2, store_lin, in_specs=[block], ins=[g_ref], out_specs=[block], outs=[z_ref])
    load(z_ref, big)
    w = weights['ff_out']
    last = w.first + w.count

    def ff_out_loop(early, late, total, outs, early_sem, late_sem, out_sem):
        cols = w.width

        def span_of(m):
            return pl.ds(pl.multiple_of(m * row_block, row_block), row_block)

        def product(span, buf, first, slots):
            terms = [jnp.dot(big[span, pl.ds(pl.multiple_of((me ^ j) * w.rows, 128), w.rows)], buf[first + p], preferred_element_type=F32) for p, j in enumerate(slots)]
            return sum(terms[1:], terms[0])

        @pl.loop(0, w.count)
        def _(n):
            where = pl.ds(pl.multiple_of(n * cols, cols), cols)
            t = Task(w, n, lax.rem(w.first + n, RING))

            def fetch(j, buf, p, sem):
                return pltpu.make_async_copy(w.shard.at[:, where] if j == 0 else w.got.at[j - 1, :, where], buf.at[p], sem.at[p])

            def out_copy(k):
                return pltpu.make_async_copy(outs.at[lax.rem(k, 2)], out_ref.at[:, pl.ds(pl.multiple_of(k * cols, cols), cols)], out_sem.at[lax.rem(k, 2)])

            def fetch_own(k):
                there = pl.ds(pl.multiple_of(k * cols, cols), cols)
                return [pltpu.make_async_copy(src_ref, early.at[p], early_sem.at[p]) for p, src_ref in enumerate((w.shard.at[:, there], w.got.at[0, :, there]))]

            def add(buf, first, slots):
                @pl.loop(0, rows // row_block)
                def _(m):
                    span = span_of(m)
                    part = product(span, buf, first, slots)
                    total[span, :] = part if slots[0] == 0 else total[span, :] + part

            @pl.when(n == 0)
            def _():
                for copy in fetch_own(n):
                    copy.start()

            with jax.named_scope('wait_diagonal'):
                pass_on_diagonal(t)
            fetch(6, early, 2, early_sem).start()
            for copy in fetch_own(n):
                copy.wait()
            add(early, 0, (0, 1))

            @pl.when(n < w.count - 1)
            def _():
                for copy in fetch_own(n + 1):
                    copy.start()

            t.swap_d().wait_recv()
            fetch(7, early, 3, early_sem).start()
            for p, j in ((2, 6), (3, 7)):
                fetch(j, early, p, early_sem).wait()
            add(early, 2, (6, 7))

            @pl.when(n >= 2)
            def _():
                out_copy(n - 2).wait()

            with jax.named_scope('wait_rest'):
                pass_on_rest(t)
            for p, j in ((0, 2), (1, 4)):
                fetch(j, late, p, late_sem).start()
            for p, j in ((0, 2), (1, 4)):
                fetch(j, late, p, late_sem).wait()
            add(late, 0, (2, 4))
            t.swap_x().wait_recv()
            fetch(3, late, 2, late_sem).start()
            t.swap_y().wait_recv()
            fetch(5, late, 3, late_sem).start()
            for p, j in ((2, 3), (3, 5)):
                fetch(j, late, p, late_sem).wait()

            @pl.loop(0, rows // row_block)
            def _(m):
                span = span_of(m)
                update = (total[span, :] + product(span, late, 2, (3, 5))).astype(BF16)
                outs[lax.rem(n, 2), span, :] = (x_s[span, where].astype(F32) + update.astype(F32)).astype(BF16)

            out_copy(n).start()
            wait_sends(t)
            begin = w.first + DONE
            with jax.named_scope('ticks'):
                on_task(begin + n, begin, last + DONE, arrive, [w])
                on_task(begin + AHEAD + n, begin + AHEAD, last + DONE + AHEAD, send, [w])

            @pl.when(n == w.count - 1)
            def _():
                out_copy(n - 1).wait()
                out_copy(n).wait()

    dma = pltpu.SemaphoreType.DMA
    with jax.named_scope('ff_out'):
        pl.run_scoped(ff_out_loop, pltpu.VMEM((4, w.rows, w.width), BF16), pltpu.VMEM((4, w.rows, w.width), BF16), pltpu.VMEM((rows, w.width), F32),
                      pltpu.VMEM((2, rows, w.width), BF16), dma((4,)), dma((4,)), dma((2,)))


def local_layer(dec_in, enc_out, dec_mask, enc_mask, rel_bias, norm_self, self_q, self_k, self_v, self_o, norm_cross, cross_q, cross_k, cross_v, cross_o, norm_ff, ff_gate, ff_lin, ff_out):
    batch, tgt, width = dec_in.shape
    src = enc_out.shape[1]
    rows = batch * tgt
    given = dict(self_q=self_q, self_k=self_k, self_v=self_v, self_o=self_o, cross_k=cross_k, cross_v=cross_v, cross_q=cross_q, cross_o=cross_o, ff_gate=ff_gate, ff_lin=ff_lin, ff_out=ff_out)
    names = list(TASKS)
    shards = [given[n] for n in names]
    lanes = -(-2 * tgt // 128) * 128 if tgt % 128 == 0 else -(-(tgt + 1) // 128) * 128
    which = lax.broadcasted_iota(jnp.int32, (8, norm_self.shape[0]), 0)
    norms = jnp.where(which == 0, norm_self[None], jnp.where(which == 1, norm_cross[None], norm_ff[None])).astype(F32)
    any_spec, vmem_spec = pl.BlockSpec(memory_space=pl.ANY), pl.BlockSpec(memory_space=pltpu.VMEM)
    hbm = lambda *shape: jax.ShapeDtypeStruct(shape, BF16)
    ff = ff_gate.shape[1]
    heads = rel_bias.shape[1]
    outs = [hbm(rows, width)] + [hbm(rows, width)] * 4 + [hbm(batch * src, width)] * 2 + [hbm(rows, ff)] * 2 + [hbm(N_DEV - 1, *s.shape) for s in shards]
    dma = pltpu.SemaphoreType.DMA
    flops = 2 * rows * width * (6 * width + 3 * ff) + 4 * batch * src * width * width
    result = pl.pallas_call(
        lambda *refs: layer_kernel(batch, names, *refs),
        out_shape=outs,
        in_specs=[vmem_spec] * 4 + [any_spec] * (3 + len(shards)),
        out_specs=[any_spec] * len(outs),
        scratch_shapes=[
            pltpu.VMEM((rows, width), BF16),
            pltpu.VMEM((rows, ff), BF16),
            pltpu.VMEM((min(GROUP, width) // HEAD_DIM, tgt, tgt), F32),
            pltpu.VMEM((heads, lanes), F32),
            pltpu.VMEM((N_DEV,) + norms.shape, F32),
            pltpu.VMEM((8, width), F32),
            dma((KINDS, RING)), dma((KINDS, RING)), dma((N_DEV,)), dma((N_DEV,)), dma(()),
        ],
        compiler_params=pltpu.CompilerParams(collective_id=0, has_side_effects=True, vmem_limit_bytes=67_043_328),
        cost_estimate=pl.CostEstimate(flops=flops, bytes_accessed=20 * sum(s.size for s in shards), transcendentals=0),
        name='layer',
    )(jnp.asarray(bucket_column(tgt, lanes)), rel_bias, dec_mask, enc_mask, norms, dec_in.reshape(rows, width), enc_out.reshape(batch * src, width), *shards)
    return result[0].reshape(dec_in.shape)


def solution(mesh):
    row_spec = P(('dp', 'fsdp'), None, None)
    mask_spec = P(('dp', 'fsdp'), None)
    weight_spec = P('fsdp', None)
    scale_spec = P('fsdp')
    in_specs = (row_spec, row_spec, mask_spec, mask_spec, P(None, None), scale_spec, weight_spec, weight_spec, weight_spec, weight_spec, scale_spec, weight_spec, weight_spec, weight_spec, weight_spec, scale_spec, weight_spec, weight_spec, weight_spec)
    return jax.shard_map(local_layer, mesh=mesh, in_specs=in_specs, out_specs=row_spec, check_vma=False)
```

```python
import math
import jax
import jax.numpy as jnp
from jax import lax
from jax.experimental import pallas as pl
from jax.experimental.pallas import tpu as pltpu
from jax.sharding import PartitionSpec as P

MESH = pl.DeviceIdType.MESH
F32, BF16 = jnp.float32, jnp.bfloat16
HEAD_DIM = 64
NUM_BUCKETS = 32
EXACT_BUCKETS = 16
MAX_DISTANCE = 128
NORM_EPS = 1e-6
MASK_FILL = -1e9
N_DEV = 8

AHEAD, PASS, DONE, RING, KINDS = 4, 4, 5, 16, 10
TASKS = {'self_q': 8, 'self_k': 8, 'self_v': 8, 'self_o': 8, 'cross_k': 8, 'cross_v': 8, 'cross_q': 8, 'cross_o': 8, 'ff_gate': 20, 'ff_lin': 20, 'ff_out': 16}
ALL_TASKS = sum(TASKS.values())
TICKS = {'head': DONE + 2, 'self_q': 8, 'self_k': 8, 'self_v': 8, 'self_attend': 6, 'self_o': 6, 'cross_k0': 6, 'cross_k1': 5, 'cross_v0': 6, 'cross_v1': 5,
         'cross_q': 6, 'cross_attend': 10, 'cross_o': 6, 'ff_gate': 12, 'ff_lin': 10}
assert sum(TICKS.values()) == ALL_TASKS - TASKS['ff_out'] + DONE
ROW_BLOCK = 512
GROUP = 512


def bucket_ids(length):
    return [offset if offset < EXACT_BUCKETS else min(NUM_BUCKETS - 1, EXACT_BUCKETS + int(math.log(offset / EXACT_BUCKETS) / math.log(MAX_DISTANCE / EXACT_BUCKETS) * (NUM_BUCKETS - EXACT_BUCKETS))) for offset in range(length)]


def bucket_starts(length):
    ids = bucket_ids(length)
    return [next(n for n in range(length) if ids[n] >= b) for b in range(1, ids[-1] + 1)]


class Weight:
    def __init__(self, first, count, shard, got):
        self.first, self.count, self.shard, self.got = first, count, shard, got
        self.rows, self.width = shard.shape[0], shard.shape[1] // count


def layer_kernel(batch, names, rel_in, dec_mask_in, enc_mask_in, norm_ref, dec_ref, enc_ref, *refs):
    n_w = len(names)
    shards, refs = refs[:n_w], refs[n_w:]
    out_ref, q_ref, k_ref, v_ref, c_ref, ck_ref, cv_ref, g_ref, z_ref = refs[:9]
    gots, refs = refs[9:9 + n_w], refs[9 + n_w:]
    x_s, big, bias_s, dist_s, gain_in, gains, rel_ref, dec_mask_ref, enc_mask_ref, send_sem, recv_sem, norm_send, norm_recv, load_sem, small_sem = refs

    me = lax.axis_index('fsdp')
    weights, first = {}, 0
    for name, shard, got in zip(names, shards, gots):
        weights[name] = Weight(first, TASKS[name], shard, got)
        first += TASKS[name]
    rows, width = dec_ref.shape
    tgt = rows // batch
    src = enc_ref.shape[0] // batch
    row_block = min(ROW_BLOCK, rows)

    def remote(src_ref, dst_ref, kind, ring, bit):
        return pltpu.make_async_remote_copy(src_ref=src_ref, dst_ref=dst_ref, send_sem=send_sem.at[kind, ring], recv_sem=recv_sem.at[kind, ring],
                                            device_id={'fsdp': me ^ bit}, device_id_type=MESH)

    class Task:
        def __init__(self, w, m, ring):
            cols = pl.ds(pl.multiple_of(m * w.width, w.width), w.width)
            own = w.shard.at[:, cols]
            slot = lambda j: w.got.at[j - 1, :, cols]
            bottom, top = pl.ds(0, w.rows // 2), pl.ds(w.rows // 2, w.rows // 2)
            low = lambda j: w.got.at[j - 1, bottom, cols]
            high = lambda j: w.got.at[j - 1, top, cols]
            self.to_partner = lambda: remote(own, slot(1), 0, ring, 1)
            self.first_x = lambda: remote(w.shard.at[bottom, cols], low(2), 1, ring, 2)
            self.first_y = lambda: remote(w.shard.at[top, cols], high(4), 2, ring, 4)
            self.rest_x = lambda: remote(w.shard.at[top, cols], high(2), 3, ring, 2)
            self.rest_y = lambda: remote(w.shard.at[bottom, cols], low(4), 4, ring, 4)
            self.relay_y = lambda: remote(low(2), low(6), 5, ring, 4)
            self.relay_x = lambda: remote(high(4), high(6), 6, ring, 2)
            self.swap_x = lambda: remote(slot(2), slot(3), 7, ring, 1)
            self.swap_y = lambda: remote(slot(4), slot(5), 8, ring, 1)
            self.swap_d = lambda: remote(slot(6), slot(7), 9, ring, 1)

    def send(t):
        for copy in (t.first_x, t.first_y, t.to_partner):
            copy().start()

    def arrive(t):
        t.to_partner().wait_recv()
        t.first_x().wait_recv()
        t.relay_y().start()
        t.rest_y().start()
        t.first_y().wait_recv()
        t.relay_x().start()
        t.rest_x().start()

    def pass_on_diagonal(t):
        t.relay_y().wait_recv()
        t.relay_x().wait_recv()
        t.swap_d().start()

    def pass_on_rest(t):
        t.rest_x().wait_recv()
        t.swap_x().start()
        t.rest_y().wait_recv()
        t.swap_y().start()

    def pass_on(t):
        pass_on_diagonal(t)
        pass_on_rest(t)

    def wait_sends(t):
        for copy in (t.to_partner, t.first_x, t.first_y, t.rest_x, t.rest_y, t.relay_y, t.relay_x, t.swap_x, t.swap_y, t.swap_d):
            copy().wait_send()

    def finish(t):
        for copy in (t.swap_x, t.swap_y, t.swap_d):
            copy().wait_recv()
        wait_sends(t)

    def on_task(t, low, high, act, among=None):
        for w in among or weights.values():
            if low < w.first + w.count and w.first < high:
                def run(w=w):
                    act(Task(w, t - w.first, lax.rem(t, RING)))
                if w.first <= low and high <= w.first + w.count:
                    run()
                else:
                    pl.when((t >= w.first) & (t < w.first + w.count))(run)

    def tick(i, low, high):
        on_task(i, low, high, arrive)
        on_task(i + AHEAD, low + AHEAD, high + AHEAD, send)
        streamed = [w for name, w in weights.items() if name != 'ff_out']
        on_task(i - PASS, low - PASS, high - PASS, pass_on, streamed)
        on_task(i - DONE, low - DONE, high - DONE, finish, streamed)

    done = [0]

    def stage_ticks(name):
        low, count = done[0], TICKS[name]
        done[0] = low + count
        return low, count

    def ticks_before(plan, n, steps, least=min):
        low, count = plan
        spread = steps if count == steps else max(steps - 4, 1)
        return low + least((n * count) // spread, count)

    def run_ticks(plan, n, steps):
        with jax.named_scope('ticks'):
            @pl.loop(ticks_before(plan, n, steps, jnp.minimum), ticks_before(plan, n + 1, steps, jnp.minimum))
            def _(i):
                tick(i, plan[0], plan[0] + plan[1])

    def load(src_ref, dst_ref):
        copy = pltpu.make_async_copy(src_ref, dst_ref, load_sem)
        copy.start()
        copy.wait()

    def norm(which):
        @pl.loop(0, rows // 16)
        def _(r):
            span = pl.ds(pl.multiple_of(r * 16, 16), 16)
            v = x_s[span, :].astype(F32)
            scale = lax.rsqrt(jnp.mean(v * v, axis=-1, keepdims=True) + NORM_EPS)
            big[span, pl.ds(0, width)] = (v * scale * gains[pl.ds(which, 1), :]).astype(BF16)

    def matmul(name, stage, split, store, in_specs=(), ins=(), out_specs=(), outs=()):
        w = weights[name]
        steps, cols = w.count * split, w.width // split
        plan = stage_ticks(stage)
        for n in range(steps):
            assert ticks_before(plan, n, steps) > w.first + min(n + 1, steps - 1) // split + DONE

        def body(own, got, *rest):
            n = pl.program_id(0)

            @pl.loop(0, rows // row_block)
            def _(m):
                span = pl.ds(pl.multiple_of(m * row_block, row_block), row_block)
                total = None
                for j in range(N_DEV):
                    part = big[span, pl.ds(pl.multiple_of((me ^ j) * w.rows, 128), w.rows)]
                    term = jnp.dot(part, own[...] if j == 0 else got[j - 1], preferred_element_type=F32)
                    total = term if total is None else total + term
                store(total, span, n, *rest)

            run_ticks(plan, n, steps)

        with jax.named_scope(stage):
            pltpu.emit_pipeline(
                body, grid=(steps,),
                in_specs=[pl.BlockSpec((w.rows, cols), lambda n: (0, n)), pl.BlockSpec((N_DEV - 1, w.rows, cols), lambda n: (0, 0, n)), *in_specs],
                out_specs=list(out_specs))(w.shard, w.got, *ins, *outs)

    def project(name, stage, dst_ref, half=0):
        cols = weights[name].width

        def store(total, span, n, dst):
            dst[span, :] = total.astype(BF16)

        matmul(name, stage, 1, store, out_specs=[pl.BlockSpec((rows, cols), lambda n: (half, n))], outs=[dst_ref])

    def residual(name, stage):
        cols = weights[name].width

        def store(total, span, n):
            where = (span, pl.ds(pl.multiple_of(n * cols, cols), cols))
            x_s[where] = (x_s[where].astype(F32) + total.astype(BF16).astype(F32)).astype(BF16)

        matmul(name, stage, 1, store)

    left = lax.broadcasted_iota(jnp.int32, (tgt, 2 * HEAD_DIM), 1) < HEAD_DIM

    def softmax(scores):
        e = jnp.exp(scores - jnp.max(scores, axis=-1, keepdims=True))
        return (e * (1.0 / jnp.sum(e, axis=-1, keepdims=True))).astype(BF16)

    def attend(stage, keys, k_src, v_src, prepare, mask_scores):
        group = min(GROUP, width)
        plan = stage_ticks(stage)
        steps = (width // group) * batch

        def body(q, k, v, c):
            g, b = pl.program_id(0), pl.program_id(1)
            prepare(g, b)
            for pair in range(group // (2 * HEAD_DIM)):
                cols = pl.ds(pair * 2 * HEAD_DIM, 2 * HEAD_DIM)
                q_pair = q[:, cols].astype(F32)
                both = jnp.concatenate([jnp.where(left, q_pair, 0.0), jnp.where(left, 0.0, q_pair)], 0).astype(BF16)
                scores = lax.dot_general(both, k[:, cols], (((1,), (1,)), ((), ())), preferred_element_type=F32)
                prob = jnp.concatenate([softmax(mask_scores(scores[h * tgt:(h + 1) * tgt], 2 * pair + h, b)) for h in range(2)], 0)
                ctx = jnp.dot(prob, v[:, cols], preferred_element_type=F32)
                c[:, cols] = jnp.where(left, ctx[:tgt], ctx[tgt:]).astype(BF16)
            run_ticks(plan, g * batch + b, steps)

        spec = lambda length: pl.BlockSpec((length, group), lambda g, b: (b, g))
        with jax.named_scope(stage):
            pltpu.emit_pipeline(body, grid=(width // group, batch), in_specs=[spec(tgt), spec(keys), spec(keys)], out_specs=[spec(tgt)])(q_ref, k_src, v_src, c_ref)

    def self_attention():
        heads = min(GROUP, width) // HEAD_DIM
        causal = lax.broadcasted_iota(jnp.int32, (tgt, tgt), 1) <= lax.broadcasted_iota(jnp.int32, (tgt, tgt), 0)

        def prepare(g, b):
            @pl.when(b == 0)
            def _():
                @pl.loop(0, heads)
                def _(h):
                    row = jnp.broadcast_to(dist_s[pl.ds(g * heads + h, 1), :], (tgt, dist_s.shape[1]))
                    bias_s[h] = pltpu.roll(row, 0, 1, stride=1, stride_axis=0)[:, :tgt]

        def mask_scores(scores, h, b):
            allowed = causal & (dec_mask_ref[pl.ds(b, 1), :] > 0)
            return jnp.where(allowed, scores + bias_s[h], MASK_FILL)

        attend('self_attend', tgt, k_ref, v_ref, prepare, mask_scores)

    def cross_attention():
        def mask_scores(scores, h, b):
            return jnp.where(enc_mask_ref[pl.ds(b, 1), :] > 0, scores, MASK_FILL)

        attend('cross_attend', src, ck_ref, cv_ref, lambda g, b: None, mask_scores)

    hidden = big.at[:, pl.ds(0, width)]

    barrier = pltpu.get_barrier_semaphore()
    for j in range(1, N_DEV):
        pl.semaphore_signal(barrier, inc=1, device_id={'fsdp': me ^ j}, device_id_type=MESH)
    pl.semaphore_wait(barrier, N_DEV - 1)

    @pl.loop(0, AHEAD)
    def _(t):
        on_task(t, 0, AHEAD, send)

    def norm_copy(j):
        return pltpu.make_async_remote_copy(src_ref=norm_ref, dst_ref=gain_in.at[me], send_sem=norm_send.at[j], recv_sem=norm_recv.at[j],
                                            device_id={'fsdp': me ^ j}, device_id_type=MESH)

    for j in range(1, N_DEV):
        norm_copy(j).start()
    load_dec = pltpu.make_async_copy(dec_ref, x_s, load_sem)
    load_dec.start()
    load_norm = pltpu.make_async_copy(norm_ref, gain_in.at[me], norm_send.at[0])
    load_norm.start()
    small = [pltpu.make_async_copy(*pair, small_sem.at[k]) for k, pair in enumerate(((rel_in, rel_ref), (dec_mask_in, dec_mask_ref), (enc_mask_in, enc_mask_ref)))]
    for copy in small:
        copy.start()
    plan = stage_ticks('head')

    def head_ticks(begin, end):
        with jax.named_scope('head'):
            @pl.loop(begin, end)
            def _(i):
                tick(i, plan[0], plan[0] + plan[1])

    head_ticks(0, 2)
    for copy in small:
        copy.wait()
    lanes = dist_s.shape[1]
    row = lax.broadcasted_iota(jnp.int32, (lanes, rel_ref.shape[1]), 0)
    distance = jnp.where(row == 0, 0, lanes - row)
    table = jnp.broadcast_to(rel_ref[0:1, :], row.shape)
    for b, start in enumerate(bucket_starts(tgt)):
        table = jnp.where(distance >= start, rel_ref[b + 1:b + 2, :], table)
    dist_s[...] = table.T
    head_ticks(2, 4)
    for j in range(1, N_DEV):
        norm_copy(j).wait()
    load_norm.wait()
    per = width // N_DEV
    for d in range(N_DEV):
        gains[:, d * per:(d + 1) * per] = gain_in[d]
    load_dec.wait()
    norm(0)
    head_ticks(4, plan[1])

    project('self_q', 'self_q', q_ref)
    project('self_k', 'self_k', k_ref)
    project('self_v', 'self_v', v_ref)
    self_attention()
    load(c_ref, hidden)
    residual('self_o', 'self_o')
    for name, dst in (('cross_k', ck_ref), ('cross_v', cv_ref)):
        for half in range(2):
            load(enc_ref.at[pl.ds(half * rows, rows), :], hidden)
            project(name, f'{name}{half}', dst, half)
    norm(1)
    project('cross_q', 'cross_q', q_ref)
    cross_attention()
    load(c_ref, hidden)
    residual('cross_o', 'cross_o')
    norm(2)

    cols = weights['ff_gate'].width // 2
    block = pl.BlockSpec((rows, cols), lambda n: (0, n))

    def store_gate(total, span, n, g):
        g[span, :] = total.astype(BF16)

    def store_lin(total, span, n, g, z):
        act = jax.nn.gelu(g[span, :].astype(F32), approximate=True)
        z[span, :] = (act * total.astype(BF16).astype(F32)).astype(BF16)

    matmul('ff_gate', 'ff_gate', 2, store_gate, out_specs=[block], outs=[g_ref])
    matmul('ff_lin', 'ff_lin', 2, store_lin, in_specs=[block], ins=[g_ref], out_specs=[block], outs=[z_ref])
    load(z_ref, big)
    w = weights['ff_out']
    last = w.first + w.count

    def ff_out_loop(early, late, total, outs, early_sem, late_sem, out_sem):
        cols = w.width

        def span_of(m):
            return pl.ds(pl.multiple_of(m * row_block, row_block), row_block)

        def product(span, buf, first, slots):
            terms = [jnp.dot(big[span, pl.ds(pl.multiple_of((me ^ j) * w.rows, 128), w.rows)], buf[first + p], preferred_element_type=F32) for p, j in enumerate(slots)]
            return sum(terms[1:], terms[0])

        @pl.loop(0, w.count)
        def _(n):
            where = pl.ds(pl.multiple_of(n * cols, cols), cols)
            t = Task(w, n, lax.rem(w.first + n, RING))

            def fetch(j, buf, p, sem):
                return pltpu.make_async_copy(w.shard.at[:, where] if j == 0 else w.got.at[j - 1, :, where], buf.at[p], sem.at[p])

            def out_copy(k):
                return pltpu.make_async_copy(outs.at[lax.rem(k, 2)], out_ref.at[:, pl.ds(pl.multiple_of(k * cols, cols), cols)], out_sem.at[lax.rem(k, 2)])

            def fetch_own(k):
                there = pl.ds(pl.multiple_of(k * cols, cols), cols)
                return [pltpu.make_async_copy(src_ref, early.at[p], early_sem.at[p]) for p, src_ref in enumerate((w.shard.at[:, there], w.got.at[0, :, there]))]

            def add(k, buf, first, slots):
                @pl.loop(0, rows // row_block)
                def _(m):
                    at = (lax.rem(k, 2), span_of(m), slice(None))
                    part = product(span_of(m), buf, first, slots)
                    total[at] = part if slots[0] == 0 else total[at] + part

            def first_product(k):
                for copy in fetch_own(k):
                    copy.wait()
                add(k, early, 0, (0, 1))

                @pl.when(k < w.count - 1)
                def _():
                    for copy in fetch_own(k + 1):
                        copy.start()

            @pl.when(n == 0)
            def _():
                for copy in fetch_own(n):
                    copy.start()
                first_product(n)

            with jax.named_scope('wait_diagonal'):
                pass_on_diagonal(t)
            fetch(6, early, 2, early_sem).start()
            t.swap_d().wait_recv()
            fetch(7, early, 3, early_sem).start()
            for p, j in ((2, 6), (3, 7)):
                fetch(j, early, p, early_sem).wait()
            add(n, early, 2, (6, 7))
            with jax.named_scope('wait_rest'):
                pass_on_rest(t)
            for p, j in ((0, 2), (1, 4)):
                fetch(j, late, p, late_sem).start()

            @pl.when(n < w.count - 1)
            def _():
                first_product(n + 1)

            for p, j in ((0, 2), (1, 4)):
                fetch(j, late, p, late_sem).wait()
            pl.when(n == w.count - 1)(lambda: add(n, late, 0, (2, 4)))
            t.swap_x().wait_recv()
            fetch(3, late, 2, late_sem).start()
            t.swap_y().wait_recv()
            fetch(5, late, 3, late_sem).start()
            pl.when(n < w.count - 1)(lambda: add(n, late, 0, (2, 4)))

            @pl.when(n >= 2)
            def _():
                out_copy(n - 2).wait()

            for p, j in ((2, 3), (3, 5)):
                fetch(j, late, p, late_sem).wait()

            @pl.loop(0, rows // row_block)
            def _(m):
                span = span_of(m)
                update = (total[lax.rem(n, 2), span, :] + product(span, late, 2, (3, 5))).astype(BF16)
                outs[lax.rem(n, 2), span, :] = (x_s[span, where].astype(F32) + update.astype(F32)).astype(BF16)

            out_copy(n).start()
            wait_sends(t)
            begin = w.first + DONE
            with jax.named_scope('ticks'):
                on_task(begin + n, begin, last + DONE, arrive, [w])
                on_task(begin + AHEAD + n, begin + AHEAD, last + DONE + AHEAD, send, [w])

            @pl.when(n == w.count - 1)
            def _():
                out_copy(n - 1).wait()
                out_copy(n).wait()

    dma = pltpu.SemaphoreType.DMA
    with jax.named_scope('ff_out'):
        pl.run_scoped(ff_out_loop, pltpu.VMEM((4, w.rows, w.width), BF16), pltpu.VMEM((4, w.rows, w.width), BF16), pltpu.VMEM((2, rows, w.width), F32),
                      pltpu.VMEM((2, rows, w.width), BF16), dma((4,)), dma((4,)), dma((2,)))


def local_layer(dec_in, enc_out, dec_mask, enc_mask, rel_bias, norm_self, self_q, self_k, self_v, self_o, norm_cross, cross_q, cross_k, cross_v, cross_o, norm_ff, ff_gate, ff_lin, ff_out):
    batch, tgt, width = dec_in.shape
    src = enc_out.shape[1]
    rows = batch * tgt
    given = dict(self_q=self_q, self_k=self_k, self_v=self_v, self_o=self_o, cross_k=cross_k, cross_v=cross_v, cross_q=cross_q, cross_o=cross_o, ff_gate=ff_gate, ff_lin=ff_lin, ff_out=ff_out)
    names = list(TASKS)
    shards = [given[n] for n in names]
    lanes = -(-2 * tgt // 128) * 128 if tgt % 128 == 0 else -(-(tgt + 1) // 128) * 128
    which = lax.broadcasted_iota(jnp.int32, (8, norm_self.shape[0]), 0)
    norms = jnp.where(which == 0, norm_self[None], jnp.where(which == 1, norm_cross[None], norm_ff[None])).astype(F32)
    any_spec = pl.BlockSpec(memory_space=pl.ANY)
    hbm = lambda *shape: jax.ShapeDtypeStruct(shape, BF16)
    ff = ff_gate.shape[1]
    heads = rel_bias.shape[1]
    outs = [hbm(rows, width)] + [hbm(rows, width)] * 4 + [hbm(batch * src, width)] * 2 + [hbm(rows, ff)] * 2 + [hbm(N_DEV - 1, *s.shape) for s in shards]
    dma = pltpu.SemaphoreType.DMA
    flops = 2 * rows * width * (6 * width + 3 * ff) + 4 * batch * src * width * width
    result = pl.pallas_call(
        lambda *refs: layer_kernel(batch, names, *refs),
        out_shape=outs,
        in_specs=[any_spec] * (6 + len(shards)),
        out_specs=[any_spec] * len(outs),
        scratch_shapes=[
            pltpu.VMEM((rows, width), BF16),
            pltpu.VMEM((rows, ff), BF16),
            pltpu.VMEM((min(GROUP, width) // HEAD_DIM, tgt, tgt), F32),
            pltpu.VMEM((heads, lanes), F32),
            pltpu.VMEM((N_DEV,) + norms.shape, F32),
            pltpu.VMEM((8, width), F32),
            pltpu.VMEM(rel_bias.shape, F32), pltpu.VMEM(dec_mask.shape, jnp.int32), pltpu.VMEM(enc_mask.shape, jnp.int32),
            dma((KINDS, RING)), dma((KINDS, RING)), dma((N_DEV,)), dma((N_DEV,)), dma(()), dma((3,)),
        ],
        compiler_params=pltpu.CompilerParams(collective_id=0, has_side_effects=True, vmem_limit_bytes=67_043_328),
        cost_estimate=pl.CostEstimate(flops=flops, bytes_accessed=20 * sum(s.size for s in shards), transcendentals=0),
        name='layer',
    )(rel_bias, dec_mask, enc_mask, norms, dec_in.reshape(rows, width), enc_out.reshape(batch * src, width), *shards)
    return result[0].reshape(dec_in.shape)


def solution(mesh):
    row_spec = P(('dp', 'fsdp'), None, None)
    mask_spec = P(('dp', 'fsdp'), None)
    weight_spec = P('fsdp', None)
    scale_spec = P('fsdp')
    in_specs = (row_spec, row_spec, mask_spec, mask_spec, P(None, None), scale_spec, weight_spec, weight_spec, weight_spec, weight_spec, scale_spec, weight_spec, weight_spec, weight_spec, weight_spec, scale_spec, weight_spec, weight_spec, weight_spec)
    return jax.shard_map(local_layer, mesh=mesh, in_specs=in_specs, out_specs=row_spec, check_vma=False)
```

```python
import math
import jax
import jax.numpy as jnp
from jax import lax
from jax.experimental import pallas as pl
from jax.experimental.pallas import tpu as pltpu
from jax.sharding import PartitionSpec as P

MESH = pl.DeviceIdType.MESH
F32, BF16 = jnp.float32, jnp.bfloat16
HEAD_DIM = 64
NUM_BUCKETS = 32
EXACT_BUCKETS = 16
MAX_DISTANCE = 128
NORM_EPS = 1e-6
MASK_FILL = -1e9
N_DEV = 8

AHEAD, PASS, DONE, RING = 4, 4, 5, 14
PARTNER, FIRST, REST, RELAY, SWAP, SWAP_D, KINDS = range(7)
TASKS = {'self_q': 8, 'self_k': 8, 'self_v': 8, 'self_o': 8, 'cross_k': 8, 'cross_v': 8, 'cross_q': 8, 'cross_o': 8, 'ff_gate': 20, 'ff_lin': 20, 'ff_out': 16}
ALL_TASKS = sum(TASKS.values())
TICKS = {'head': DONE + 2, 'self_q': 8, 'self_k': 8, 'self_v': 8, 'self_attend': 6, 'self_o': 6, 'cross_k0': 6, 'cross_k1': 5, 'cross_v0': 6, 'cross_v1': 5,
         'cross_q': 6, 'cross_attend': 10, 'cross_o': 6, 'ff_gate': 12, 'ff_lin': 10}
assert sum(TICKS.values()) == ALL_TASKS - TASKS['ff_out'] + DONE
ROW_BLOCK = 512
GROUP = 512


def bucket_ids(length):
    return [offset if offset < EXACT_BUCKETS else min(NUM_BUCKETS - 1, EXACT_BUCKETS + int(math.log(offset / EXACT_BUCKETS) / math.log(MAX_DISTANCE / EXACT_BUCKETS) * (NUM_BUCKETS - EXACT_BUCKETS))) for offset in range(length)]


def bucket_starts(length):
    ids = bucket_ids(length)
    return [next(n for n in range(length) if ids[n] >= b) for b in range(1, ids[-1] + 1)]


class Weight:
    def __init__(self, first, count, shard, got):
        self.first, self.count, self.shard, self.got = first, count, shard, got
        self.rows, self.width = shard.shape[0], shard.shape[1] // count


def layer_kernel(batch, names, rel_in, dec_mask_in, enc_mask_in, norm_ref, dec_ref, enc_ref, *refs):
    n_w = len(names)
    shards, refs = refs[:n_w], refs[n_w:]
    out_ref, q_ref, k_ref, v_ref, c_ref, ck_ref, cv_ref, g_ref, z_ref = refs[:9]
    gots, refs = refs[9:9 + n_w], refs[9 + n_w:]
    x_s, big, bias_s, dist_s, gain_in, gains, rel_ref, dec_mask_ref, enc_mask_ref, send_sem, recv_sem, norm_send, norm_recv, load_sem, small_sem = refs

    me = lax.axis_index('fsdp')
    weights, first = {}, 0
    for name, shard, got in zip(names, shards, gots):
        weights[name] = Weight(first, TASKS[name], shard, got)
        first += TASKS[name]
    rows, width = dec_ref.shape
    tgt = rows // batch
    src = enc_ref.shape[0] // batch
    row_block = min(ROW_BLOCK, rows)

    def remote(src_ref, dst_ref, kind, ring, bit):
        return pltpu.make_async_remote_copy(src_ref=src_ref, dst_ref=dst_ref, send_sem=send_sem.at[ring], recv_sem=recv_sem.at[kind, ring],
                                            device_id={'fsdp': me ^ bit}, device_id_type=MESH)

    class Task:
        def __init__(self, w, m, ring):
            cols = pl.ds(pl.multiple_of(m * w.width, w.width), w.width)
            own = w.shard.at[:, cols]
            slot = lambda j: w.got.at[j - 1, :, cols]
            bottom, top = pl.ds(0, w.rows // 2), pl.ds(w.rows // 2, w.rows // 2)
            low = lambda j: w.got.at[j - 1, bottom, cols]
            high = lambda j: w.got.at[j - 1, top, cols]
            self.to_partner = lambda: remote(own, slot(1), PARTNER, ring, 1)
            self.first_x = lambda: remote(w.shard.at[bottom, cols], low(2), FIRST, ring, 2)
            self.first_y = lambda: remote(w.shard.at[top, cols], high(4), FIRST, ring, 4)
            self.rest_x = lambda: remote(w.shard.at[top, cols], high(2), REST, ring, 2)
            self.rest_y = lambda: remote(w.shard.at[bottom, cols], low(4), REST, ring, 4)
            self.relay_y = lambda: remote(low(2), low(6), RELAY, ring, 4)
            self.relay_x = lambda: remote(high(4), high(6), RELAY, ring, 2)
            self.swap_x = lambda: remote(slot(2), slot(3), SWAP, ring, 1)
            self.swap_y = lambda: remote(slot(4), slot(5), SWAP, ring, 1)
            self.swap_d = lambda: remote(slot(6), slot(7), SWAP_D, ring, 1)
            shape = lambda slots: w.got.at[pl.ds(0, slots), :, cols]
            self.got_all = lambda kind, slots: remote(shape(slots), shape(slots), kind, ring, 1).wait_recv()
            self.sent_all = lambda: remote(shape(7), shape(7), PARTNER, ring, 1).wait_send()

    def send(t):
        for copy in (t.first_x, t.first_y, t.to_partner):
            copy().start()

    def arrive(t):
        t.to_partner().wait_recv()
        t.got_all(FIRST, 1)
        for copy in (t.relay_y, t.relay_x, t.rest_y, t.rest_x):
            copy().start()

    def pass_on_diagonal(t):
        t.got_all(RELAY, 1)
        t.swap_d().start()

    def pass_on_rest(t):
        t.got_all(REST, 1)
        t.swap_x().start()
        t.swap_y().start()

    def pass_on(t):
        pass_on_diagonal(t)
        pass_on_rest(t)

    def finish(t):
        t.swap_d().wait_recv()
        t.got_all(SWAP, 2)
        t.sent_all()

    def on_task(t, low, high, act, among=None, stop=ALL_TASKS):
        for w in among or weights.values():
            last = min(w.first + w.count, stop)
            if low < last and w.first < high:
                def run(w=w):
                    act(Task(w, t - w.first, lax.rem(t, RING)))
                if w.first <= low and high <= last:
                    run()
                else:
                    pl.when((t >= w.first) & (t < last))(run)

    streamed = [w for name, w in weights.items() if name != 'ff_out']
    out_look = weights['ff_out'].first + PASS

    def tick(i, low, high):
        on_task(i, low, high, arrive, stop=out_look)
        on_task(i + AHEAD, low + AHEAD, high + AHEAD, send, stop=out_look + AHEAD)
        on_task(i - PASS, low - PASS, high - PASS, pass_on, streamed)
        on_task(i - DONE, low - DONE, high - DONE, finish, streamed)

    done = [0]

    def stage_ticks(name):
        low, count = done[0], TICKS[name]
        done[0] = low + count
        return low, count

    def ticks_before(plan, n, steps, least=min):
        low, count = plan
        spread = steps if count == steps else max(steps - 4, 1)
        return low + least((n * count) // spread, count)

    def run_ticks(plan, n, steps):
        with jax.named_scope('ticks'):
            @pl.loop(ticks_before(plan, n, steps, jnp.minimum), ticks_before(plan, n + 1, steps, jnp.minimum))
            def _(i):
                tick(i, plan[0], plan[0] + plan[1])

    def load(src_ref, dst_ref):
        copy = pltpu.make_async_copy(src_ref, dst_ref, load_sem)
        copy.start()
        copy.wait()

    def norm(which):
        @pl.loop(0, rows // 16)
        def _(r):
            span = pl.ds(pl.multiple_of(r * 16, 16), 16)
            v = x_s[span, :].astype(F32)
            scale = lax.rsqrt(jnp.mean(v * v, axis=-1, keepdims=True) + NORM_EPS)
            big[span, pl.ds(0, width)] = (v * scale * gains[pl.ds(which, 1), :]).astype(BF16)

    def matmul(name, stage, split, store, in_specs=(), ins=(), out_specs=(), outs=()):
        w = weights[name]
        steps, cols = w.count * split, w.width // split
        plan = stage_ticks(stage)
        for n in range(steps):
            assert ticks_before(plan, n, steps) > w.first + min(n + 1, steps - 1) // split + DONE

        def body(own, got, *rest):
            n = pl.program_id(0)

            @pl.loop(0, rows // row_block)
            def _(m):
                span = pl.ds(pl.multiple_of(m * row_block, row_block), row_block)
                total = None
                for j in range(N_DEV):
                    part = big[span, pl.ds(pl.multiple_of((me ^ j) * w.rows, 128), w.rows)]
                    term = jnp.dot(part, own[...] if j == 0 else got[j - 1], preferred_element_type=F32)
                    total = term if total is None else total + term
                store(total, span, n, *rest)

            run_ticks(plan, n, steps)

        with jax.named_scope(stage):
            pltpu.emit_pipeline(
                body, grid=(steps,),
                in_specs=[pl.BlockSpec((w.rows, cols), lambda n: (0, n)), pl.BlockSpec((N_DEV - 1, w.rows, cols), lambda n: (0, 0, n)), *in_specs],
                out_specs=list(out_specs))(w.shard, w.got, *ins, *outs)

    def project(name, stage, dst_ref, half=0):
        cols = weights[name].width

        def store(total, span, n, dst):
            dst[span, :] = total.astype(BF16)

        matmul(name, stage, 1, store, out_specs=[pl.BlockSpec((rows, cols), lambda n: (half, n))], outs=[dst_ref])

    def residual(name, stage):
        cols = weights[name].width

        def store(total, span, n):
            where = (span, pl.ds(pl.multiple_of(n * cols, cols), cols))
            x_s[where] = (x_s[where].astype(F32) + total.astype(BF16).astype(F32)).astype(BF16)

        matmul(name, stage, 1, store)

    left = lax.broadcasted_iota(jnp.int32, (tgt, 2 * HEAD_DIM), 1) < HEAD_DIM

    def softmax(scores):
        e = jnp.exp(scores - jnp.max(scores, axis=-1, keepdims=True))
        return (e * (1.0 / jnp.sum(e, axis=-1, keepdims=True))).astype(BF16)

    def attend(stage, keys, k_src, v_src, prepare, mask_scores):
        group = min(GROUP, width)
        plan = stage_ticks(stage)
        steps = (width // group) * batch

        def body(q, k, v, c):
            g, b = pl.program_id(0), pl.program_id(1)
            prepare(g, b)
            for pair in range(group // (2 * HEAD_DIM)):
                cols = pl.ds(pair * 2 * HEAD_DIM, 2 * HEAD_DIM)
                q_pair = q[:, cols].astype(F32)
                both = jnp.concatenate([jnp.where(left, q_pair, 0.0), jnp.where(left, 0.0, q_pair)], 0).astype(BF16)
                scores = lax.dot_general(both, k[:, cols], (((1,), (1,)), ((), ())), preferred_element_type=F32)
                prob = jnp.concatenate([softmax(mask_scores(scores[h * tgt:(h + 1) * tgt], 2 * pair + h, b)) for h in range(2)], 0)
                ctx = jnp.dot(prob, v[:, cols], preferred_element_type=F32)
                c[:, cols] = jnp.where(left, ctx[:tgt], ctx[tgt:]).astype(BF16)
            run_ticks(plan, g * batch + b, steps)

        spec = lambda length: pl.BlockSpec((length, group), lambda g, b: (b, g))
        with jax.named_scope(stage):
            pltpu.emit_pipeline(body, grid=(width // group, batch), in_specs=[spec(tgt), spec(keys), spec(keys)], out_specs=[spec(tgt)])(q_ref, k_src, v_src, c_ref)

    def self_attention():
        heads = min(GROUP, width) // HEAD_DIM
        causal = lax.broadcasted_iota(jnp.int32, (tgt, tgt), 1) <= lax.broadcasted_iota(jnp.int32, (tgt, tgt), 0)

        def prepare(g, b):
            @pl.when(b == 0)
            def _():
                @pl.loop(0, heads)
                def _(h):
                    row = jnp.broadcast_to(dist_s[pl.ds(g * heads + h, 1), :], (tgt, dist_s.shape[1]))
                    bias_s[h] = pltpu.roll(row, 0, 1, stride=1, stride_axis=0)[:, :tgt]

        def mask_scores(scores, h, b):
            allowed = causal & (dec_mask_ref[pl.ds(b, 1), :] > 0)
            return jnp.where(allowed, scores + bias_s[h], MASK_FILL)

        attend('self_attend', tgt, k_ref, v_ref, prepare, mask_scores)

    def cross_attention():
        def mask_scores(scores, h, b):
            return jnp.where(enc_mask_ref[pl.ds(b, 1), :] > 0, scores, MASK_FILL)

        attend('cross_attend', src, ck_ref, cv_ref, lambda g, b: None, mask_scores)

    hidden = big.at[:, pl.ds(0, width)]

    barrier = pltpu.get_barrier_semaphore()
    for j in range(1, N_DEV):
        pl.semaphore_signal(barrier, inc=1, device_id={'fsdp': me ^ j}, device_id_type=MESH)
    pl.semaphore_wait(barrier, N_DEV - 1)

    @pl.loop(0, AHEAD)
    def _(t):
        on_task(t, 0, AHEAD, send)

    def norm_copy(j):
        return pltpu.make_async_remote_copy(src_ref=norm_ref, dst_ref=gain_in.at[me], send_sem=norm_send.at[j], recv_sem=norm_recv.at[j],
                                            device_id={'fsdp': me ^ j}, device_id_type=MESH)

    for j in range(1, N_DEV):
        norm_copy(j).start()
    load_dec = pltpu.make_async_copy(dec_ref, x_s, load_sem)
    load_dec.start()
    load_norm = pltpu.make_async_copy(norm_ref, gain_in.at[me], norm_send.at[0])
    load_norm.start()
    small = [pltpu.make_async_copy(*pair, small_sem.at[k]) for k, pair in enumerate(((rel_in, rel_ref), (dec_mask_in, dec_mask_ref), (enc_mask_in, enc_mask_ref)))]
    for copy in small:
        copy.start()
    plan = stage_ticks('head')

    def head_ticks(begin, end):
        with jax.named_scope('head'):
            @pl.loop(begin, end)
            def _(i):
                tick(i, plan[0], plan[0] + plan[1])

    head_ticks(0, 2)
    for copy in small:
        copy.wait()
    lanes = dist_s.shape[1]
    row = lax.broadcasted_iota(jnp.int32, (lanes, rel_ref.shape[1]), 0)
    distance = jnp.where(row == 0, 0, lanes - row)
    table = jnp.broadcast_to(rel_ref[0:1, :], row.shape)
    for b, start in enumerate(bucket_starts(tgt)):
        table = jnp.where(distance >= start, rel_ref[b + 1:b + 2, :], table)
    dist_s[...] = table.T
    head_ticks(2, 4)
    for j in range(1, N_DEV):
        norm_copy(j).wait()
    load_norm.wait()
    per = width // N_DEV
    for d in range(N_DEV):
        gains[:, d * per:(d + 1) * per] = gain_in[d]
    load_dec.wait()
    norm(0)
    head_ticks(4, plan[1])

    project('self_q', 'self_q', q_ref)
    project('self_k', 'self_k', k_ref)
    project('self_v', 'self_v', v_ref)
    self_attention()
    load(c_ref, hidden)
    residual('self_o', 'self_o')
    for name, dst in (('cross_k', ck_ref), ('cross_v', cv_ref)):
        for half in range(2):
            load(enc_ref.at[pl.ds(half * rows, rows), :], hidden)
            project(name, f'{name}{half}', dst, half)
    norm(1)
    project('cross_q', 'cross_q', q_ref)
    cross_attention()
    load(c_ref, hidden)
    residual('cross_o', 'cross_o')
    norm(2)

    cols = weights['ff_gate'].width // 2
    block = pl.BlockSpec((rows, cols), lambda n: (0, n))

    def store_gate(total, span, n, g):
        g[span, :] = total.astype(BF16)

    def store_lin(total, span, n, g, z):
        act = jax.nn.gelu(g[span, :].astype(F32), approximate=True)
        z[span, :] = (act * total.astype(BF16).astype(F32)).astype(BF16)

    matmul('ff_gate', 'ff_gate', 2, store_gate, out_specs=[block], outs=[g_ref])
    matmul('ff_lin', 'ff_lin', 2, store_lin, in_specs=[block], ins=[g_ref], out_specs=[block], outs=[z_ref])
    load(z_ref, big)
    w = weights['ff_out']

    def ff_out_loop(early, late, total, outs, early_sem, late_sem, out_sem):
        cols = w.width

        def span_of(m):
            return pl.ds(pl.multiple_of(m * row_block, row_block), row_block)

        def product(span, buf, first, slots):
            terms = [jnp.dot(big[span, pl.ds(pl.multiple_of((me ^ j) * w.rows, 128), w.rows)], buf[first + p], preferred_element_type=F32) for p, j in enumerate(slots)]
            return sum(terms[1:], terms[0])

        @pl.loop(0, w.count)
        def _(n):
            where = pl.ds(pl.multiple_of(n * cols, cols), cols)
            t = Task(w, n, lax.rem(w.first + n, RING))

            def fetch(j, buf, p, sem):
                return pltpu.make_async_copy(w.shard.at[:, where] if j == 0 else w.got.at[j - 1, :, where], buf.at[p], sem.at[p])

            def out_copy(k):
                return pltpu.make_async_copy(outs.at[lax.rem(k, 2)], out_ref.at[:, pl.ds(pl.multiple_of(k * cols, cols), cols)], out_sem.at[lax.rem(k, 2)])

            def fetch_own(k):
                there = pl.ds(pl.multiple_of(k * cols, cols), cols)
                return [pltpu.make_async_copy(src_ref, early.at[p], early_sem.at[p]) for p, src_ref in enumerate((w.shard.at[:, there], w.got.at[0, :, there]))]

            def add(k, buf, first, slots):
                @pl.loop(0, rows // row_block)
                def _(m):
                    at = (lax.rem(k, 2), span_of(m), slice(None))
                    part = product(span_of(m), buf, first, slots)
                    total[at] = part if slots[0] == 0 else total[at] + part

            def first_product(k):
                for copy in fetch_own(k):
                    copy.wait()
                add(k, early, 0, (0, 1))

                @pl.when(k < w.count - 1)
                def _():
                    for copy in fetch_own(k + 1):
                        copy.start()

            @pl.when(n == 0)
            def _():
                for copy in fetch_own(n):
                    copy.start()
                first_product(n)

            with jax.named_scope('wait_diagonal'):
                pass_on_diagonal(t)
            fetch(6, early, 2, early_sem).start()
            t.swap_d().wait_recv()
            fetch(7, early, 3, early_sem).start()
            for p, j in ((2, 6), (3, 7)):
                fetch(j, early, p, early_sem).wait()
            add(n, early, 2, (6, 7))
            with jax.named_scope('wait_rest'):
                pass_on_rest(t)
            for p, j in ((0, 2), (1, 4)):
                fetch(j, late, p, late_sem).start()

            @pl.when(n < w.count - 1)
            def _():
                first_product(n + 1)

            for p, j in ((0, 2), (1, 4)):
                fetch(j, late, p, late_sem).wait()
            pl.when(n == w.count - 1)(lambda: add(n, late, 0, (2, 4)))
            t.got_all(SWAP, 2)
            for p, j in ((2, 3), (3, 5)):
                fetch(j, late, p, late_sem).start()
            pl.when(n < w.count - 1)(lambda: add(n, late, 0, (2, 4)))

            @pl.when(n >= 2)
            def _():
                out_copy(n - 2).wait()

            for p, j in ((2, 3), (3, 5)):
                fetch(j, late, p, late_sem).wait()

            @pl.loop(0, rows // row_block)
            def _(m):
                span = span_of(m)
                update = (total[lax.rem(n, 2), span, :] + product(span, late, 2, (3, 5))).astype(BF16)
                outs[lax.rem(n, 2), span, :] = (x_s[span, where].astype(F32) + update.astype(F32)).astype(BF16)

            out_copy(n).start()
            t.sent_all()
            with jax.named_scope('ticks'):
                on_task(out_look + n, out_look, out_look + w.count, arrive, [w])
                on_task(out_look + AHEAD + n, out_look + AHEAD, out_look + AHEAD + w.count, send, [w])

            @pl.when(n == w.count - 1)
            def _():
                out_copy(n - 1).wait()
                out_copy(n).wait()

    dma = pltpu.SemaphoreType.DMA
    with jax.named_scope('ff_out'):
        pl.run_scoped(ff_out_loop, pltpu.VMEM((4, w.rows, w.width), BF16), pltpu.VMEM((4, w.rows, w.width), BF16), pltpu.VMEM((2, rows, w.width), F32),
                      pltpu.VMEM((2, rows, w.width), BF16), dma((4,)), dma((4,)), dma((2,)))


def local_layer(dec_in, enc_out, dec_mask, enc_mask, rel_bias, norm_self, self_q, self_k, self_v, self_o, norm_cross, cross_q, cross_k, cross_v, cross_o, norm_ff, ff_gate, ff_lin, ff_out):
    batch, tgt, width = dec_in.shape
    src = enc_out.shape[1]
    rows = batch * tgt
    given = dict(self_q=self_q, self_k=self_k, self_v=self_v, self_o=self_o, cross_k=cross_k, cross_v=cross_v, cross_q=cross_q, cross_o=cross_o, ff_gate=ff_gate, ff_lin=ff_lin, ff_out=ff_out)
    names = list(TASKS)
    shards = [given[n] for n in names]
    lanes = -(-2 * tgt // 128) * 128 if tgt % 128 == 0 else -(-(tgt + 1) // 128) * 128
    which = lax.broadcasted_iota(jnp.int32, (8, norm_self.shape[0]), 0)
    norms = jnp.where(which == 0, norm_self[None], jnp.where(which == 1, norm_cross[None], norm_ff[None])).astype(F32)
    any_spec = pl.BlockSpec(memory_space=pl.ANY)
    hbm = lambda *shape: jax.ShapeDtypeStruct(shape, BF16)
    ff = ff_gate.shape[1]
    heads = rel_bias.shape[1]
    outs = [hbm(rows, width)] + [hbm(rows, width)] * 4 + [hbm(batch * src, width)] * 2 + [hbm(rows, ff)] * 2 + [hbm(N_DEV - 1, *s.shape) for s in shards]
    dma = pltpu.SemaphoreType.DMA
    flops = 2 * rows * width * (6 * width + 3 * ff) + 4 * batch * src * width * width
    result = pl.pallas_call(
        lambda *refs: layer_kernel(batch, names, *refs),
        out_shape=outs,
        in_specs=[any_spec] * (6 + len(shards)),
        out_specs=[any_spec] * len(outs),
        scratch_shapes=[
            pltpu.VMEM((rows, width), BF16),
            pltpu.VMEM((rows, ff), BF16),
            pltpu.VMEM((min(GROUP, width) // HEAD_DIM, tgt, tgt), F32),
            pltpu.VMEM((heads, lanes), F32),
            pltpu.VMEM((N_DEV,) + norms.shape, F32),
            pltpu.VMEM((8, width), F32),
            pltpu.VMEM(rel_bias.shape, F32), pltpu.VMEM(dec_mask.shape, jnp.int32), pltpu.VMEM(enc_mask.shape, jnp.int32),
            dma((RING,)), dma((KINDS, RING)), dma((N_DEV,)), dma((N_DEV,)), dma(()), dma((3,)),
        ],
        compiler_params=pltpu.CompilerParams(collective_id=0, has_side_effects=True, vmem_limit_bytes=67_043_328),
        cost_estimate=pl.CostEstimate(flops=flops, bytes_accessed=20 * sum(s.size for s in shards), transcendentals=0),
        name='layer',
    )(rel_bias, dec_mask, enc_mask, norms, dec_in.reshape(rows, width), enc_out.reshape(batch * src, width), *shards)
    return result[0].reshape(dec_in.shape)


def solution(mesh):
    row_spec = P(('dp', 'fsdp'), None, None)
    mask_spec = P(('dp', 'fsdp'), None)
    weight_spec = P('fsdp', None)
    scale_spec = P('fsdp')
    in_specs = (row_spec, row_spec, mask_spec, mask_spec, P(None, None), scale_spec, weight_spec, weight_spec, weight_spec, weight_spec, scale_spec, weight_spec, weight_spec, weight_spec, weight_spec, scale_spec, weight_spec, weight_spec, weight_spec)
    return jax.shard_map(local_layer, mesh=mesh, in_specs=in_specs, out_specs=row_spec, check_vma=False)
```

```python
import math
import jax
import jax.numpy as jnp
from jax import lax
from jax.experimental import pallas as pl
from jax.experimental.pallas import tpu as pltpu
from jax.sharding import PartitionSpec as P

MESH = pl.DeviceIdType.MESH
F32, BF16 = jnp.float32, jnp.bfloat16
HEAD_DIM = 64
NUM_BUCKETS = 32
EXACT_BUCKETS = 16
MAX_DISTANCE = 128
NORM_EPS = 1e-6
MASK_FILL = -1e9
N_DEV = 8

AHEAD, PASS, DONE, RING = 4, 4, 5, 14
PARTNER, FIRST, REST, RELAY, SWAP_FIRST, SWAP, SWAP_D, KINDS = range(8)
TASKS = {'self_q': 8, 'self_k': 8, 'self_v': 8, 'self_o': 8, 'cross_k': 8, 'cross_v': 8, 'cross_q': 8, 'cross_o': 8, 'ff_gate': 20, 'ff_lin': 20, 'ff_out': 16}
ALL_TASKS = sum(TASKS.values())
TICKS = {'head': DONE + 2, 'self_q': 8, 'self_k': 8, 'self_v': 8, 'self_attend': 6, 'self_o': 6, 'cross_k0': 6, 'cross_k1': 5, 'cross_v0': 6, 'cross_v1': 5,
         'cross_q': 6, 'cross_attend': 10, 'cross_o': 6, 'ff_gate': 12, 'ff_lin': 10}
assert sum(TICKS.values()) == ALL_TASKS - TASKS['ff_out'] + DONE
ROW_BLOCK = 512
GROUP = 512


def bucket_ids(length):
    return [offset if offset < EXACT_BUCKETS else min(NUM_BUCKETS - 1, EXACT_BUCKETS + int(math.log(offset / EXACT_BUCKETS) / math.log(MAX_DISTANCE / EXACT_BUCKETS) * (NUM_BUCKETS - EXACT_BUCKETS))) for offset in range(length)]


def bucket_starts(length):
    ids = bucket_ids(length)
    return [next(n for n in range(length) if ids[n] >= b) for b in range(1, ids[-1] + 1)]


class Weight:
    def __init__(self, first, count, shard, got):
        self.first, self.count, self.shard, self.got = first, count, shard, got
        self.rows, self.width = shard.shape[0], shard.shape[1] // count


def layer_kernel(batch, names, rel_in, dec_mask_in, enc_mask_in, norm_ref, dec_ref, enc_ref, *refs):
    n_w = len(names)
    shards, refs = refs[:n_w], refs[n_w:]
    out_ref, q_ref, k_ref, v_ref, c_ref, ck_ref, cv_ref, g_ref, z_ref = refs[:9]
    gots, refs = refs[9:9 + n_w], refs[9 + n_w:]
    x_s, big, bias_s, dist_s, gain_in, gains, rel_ref, dec_mask_ref, enc_mask_ref, send_sem, recv_sem, norm_send, norm_recv, load_sem, small_sem = refs

    me = lax.axis_index('fsdp')
    weights, first = {}, 0
    for name, shard, got in zip(names, shards, gots):
        weights[name] = Weight(first, TASKS[name], shard, got)
        first += TASKS[name]
    rows, width = dec_ref.shape
    tgt = rows // batch
    src = enc_ref.shape[0] // batch
    row_block = min(ROW_BLOCK, rows)

    def remote(src_ref, dst_ref, kind, ring, bit):
        return pltpu.make_async_remote_copy(src_ref=src_ref, dst_ref=dst_ref, send_sem=send_sem.at[ring], recv_sem=recv_sem.at[kind, ring],
                                            device_id={'fsdp': me ^ bit}, device_id_type=MESH)

    class Task:
        def __init__(self, w, m, ring):
            cols = pl.ds(pl.multiple_of(m * w.width, w.width), w.width)
            own = w.shard.at[:, cols]
            slot = lambda j: w.got.at[j - 1, :, cols]
            bottom, top = pl.ds(0, w.rows // 2), pl.ds(w.rows // 2, w.rows // 2)
            low = lambda j: w.got.at[j - 1, bottom, cols]
            high = lambda j: w.got.at[j - 1, top, cols]
            self.to_partner = lambda: remote(own, slot(1), PARTNER, ring, 1)
            self.first_x = lambda: remote(w.shard.at[bottom, cols], low(2), FIRST, ring, 2)
            self.first_y = lambda: remote(w.shard.at[top, cols], high(4), FIRST, ring, 4)
            self.rest_x = lambda: remote(w.shard.at[top, cols], high(2), REST, ring, 2)
            self.rest_y = lambda: remote(w.shard.at[bottom, cols], low(4), REST, ring, 4)
            self.relay_y = lambda: remote(low(2), low(6), RELAY, ring, 4)
            self.relay_x = lambda: remote(high(4), high(6), RELAY, ring, 2)
            self.swap_x = lambda: remote(slot(2), slot(3), SWAP, ring, 1)
            self.swap_y = lambda: remote(slot(4), slot(5), SWAP, ring, 1)
            self.swap_d = lambda: remote(slot(6), slot(7), SWAP_D, ring, 1)
            self.swap_first_x = lambda: remote(low(2), low(3), SWAP_FIRST, ring, 1)
            self.swap_first_y = lambda: remote(high(4), high(5), SWAP_FIRST, ring, 1)
            self.swap_rest_x = lambda: remote(high(2), high(3), SWAP, ring, 1)
            self.swap_rest_y = lambda: remote(low(4), low(5), SWAP, ring, 1)
            self.halves = w is weights['ff_out']
            shape = lambda slots: w.got.at[pl.ds(0, slots), :, cols]
            self.got_all = lambda kind, slots: remote(shape(slots), shape(slots), kind, ring, 1).wait_recv()
            self.sent_all = lambda: remote(shape(7), shape(7), PARTNER, ring, 1).wait_send()

    def send(t):
        for copy in (t.first_x, t.first_y, t.to_partner):
            copy().start()

    def arrive(t):
        t.to_partner().wait_recv()
        t.got_all(FIRST, 1)
        for copy in (t.relay_y, t.relay_x, t.rest_y, t.rest_x, *((t.swap_first_x, t.swap_first_y) if t.halves else ())):
            copy().start()

    def pass_on_diagonal(t):
        t.got_all(RELAY, 1)
        t.swap_d().start()

    def pass_on_rest(t):
        t.got_all(REST, 1)
        for copy in (t.swap_rest_x, t.swap_rest_y) if t.halves else (t.swap_x, t.swap_y):
            copy().start()

    def pass_on(t):
        pass_on_diagonal(t)
        pass_on_rest(t)

    def finish(t):
        t.swap_d().wait_recv()
        t.got_all(SWAP, 2)
        t.sent_all()

    def on_task(t, low, high, act, among=None, stop=ALL_TASKS):
        for w in among or weights.values():
            last = min(w.first + w.count, stop)
            if low < last and w.first < high:
                def run(w=w):
                    act(Task(w, t - w.first, lax.rem(t, RING)))
                if w.first <= low and high <= last:
                    run()
                else:
                    pl.when((t >= w.first) & (t < last))(run)

    streamed = [w for name, w in weights.items() if name != 'ff_out']
    out_look = weights['ff_out'].first + PASS

    def tick(i, low, high):
        on_task(i, low, high, arrive, stop=out_look)
        on_task(i + AHEAD, low + AHEAD, high + AHEAD, send, stop=out_look + AHEAD)
        on_task(i - PASS, low - PASS, high - PASS, pass_on, streamed)
        on_task(i - DONE, low - DONE, high - DONE, finish, streamed)

    done = [0]

    def stage_ticks(name):
        low, count = done[0], TICKS[name]
        done[0] = low + count
        return low, count

    def ticks_before(plan, n, steps, least=min):
        low, count = plan
        spread = steps if count == steps else max(steps - 4, 1)
        return low + least((n * count) // spread, count)

    def run_ticks(plan, n, steps):
        with jax.named_scope('ticks'):
            @pl.loop(ticks_before(plan, n, steps, jnp.minimum), ticks_before(plan, n + 1, steps, jnp.minimum))
            def _(i):
                tick(i, plan[0], plan[0] + plan[1])

    def load(src_ref, dst_ref):
        copy = pltpu.make_async_copy(src_ref, dst_ref, load_sem)
        copy.start()
        copy.wait()

    def norm(which):
        @pl.loop(0, rows // 16)
        def _(r):
            span = pl.ds(pl.multiple_of(r * 16, 16), 16)
            v = x_s[span, :].astype(F32)
            scale = lax.rsqrt(jnp.mean(v * v, axis=-1, keepdims=True) + NORM_EPS)
            big[span, pl.ds(0, width)] = (v * scale * gains[pl.ds(which, 1), :]).astype(BF16)

    def matmul(name, stage, split, store, in_specs=(), ins=(), out_specs=(), outs=()):
        w = weights[name]
        steps, cols = w.count * split, w.width // split
        plan = stage_ticks(stage)
        for n in range(steps):
            assert ticks_before(plan, n, steps) > w.first + min(n + 1, steps - 1) // split + DONE

        def body(own, got, *rest):
            n = pl.program_id(0)

            @pl.loop(0, rows // row_block)
            def _(m):
                span = pl.ds(pl.multiple_of(m * row_block, row_block), row_block)
                total = None
                for j in range(N_DEV):
                    part = big[span, pl.ds(pl.multiple_of((me ^ j) * w.rows, 128), w.rows)]
                    term = jnp.dot(part, own[...] if j == 0 else got[j - 1], preferred_element_type=F32)
                    total = term if total is None else total + term
                store(total, span, n, *rest)

            run_ticks(plan, n, steps)

        with jax.named_scope(stage):
            pltpu.emit_pipeline(
                body, grid=(steps,),
                in_specs=[pl.BlockSpec((w.rows, cols), lambda n: (0, n)), pl.BlockSpec((N_DEV - 1, w.rows, cols), lambda n: (0, 0, n)), *in_specs],
                out_specs=list(out_specs))(w.shard, w.got, *ins, *outs)

    def project(name, stage, dst_ref, half=0):
        cols = weights[name].width

        def store(total, span, n, dst):
            dst[span, :] = total.astype(BF16)

        matmul(name, stage, 1, store, out_specs=[pl.BlockSpec((rows, cols), lambda n: (half, n))], outs=[dst_ref])

    def residual(name, stage):
        cols = weights[name].width

        def store(total, span, n):
            where = (span, pl.ds(pl.multiple_of(n * cols, cols), cols))
            x_s[where] = (x_s[where].astype(F32) + total.astype(BF16).astype(F32)).astype(BF16)

        matmul(name, stage, 1, store)

    left = lax.broadcasted_iota(jnp.int32, (tgt, 2 * HEAD_DIM), 1) < HEAD_DIM

    def softmax(scores):
        e = jnp.exp(scores - jnp.max(scores, axis=-1, keepdims=True))
        return (e * (1.0 / jnp.sum(e, axis=-1, keepdims=True))).astype(BF16)

    def attend(stage, keys, k_src, v_src, prepare, mask_scores):
        group = min(GROUP, width)
        plan = stage_ticks(stage)
        steps = (width // group) * batch

        def body(q, k, v, c):
            g, b = pl.program_id(0), pl.program_id(1)
            prepare(g, b)
            for pair in range(group // (2 * HEAD_DIM)):
                cols = pl.ds(pair * 2 * HEAD_DIM, 2 * HEAD_DIM)
                q_pair = q[:, cols].astype(F32)
                both = jnp.concatenate([jnp.where(left, q_pair, 0.0), jnp.where(left, 0.0, q_pair)], 0).astype(BF16)
                scores = lax.dot_general(both, k[:, cols], (((1,), (1,)), ((), ())), preferred_element_type=F32)
                prob = jnp.concatenate([softmax(mask_scores(scores[h * tgt:(h + 1) * tgt], 2 * pair + h, b)) for h in range(2)], 0)
                ctx = jnp.dot(prob, v[:, cols], preferred_element_type=F32)
                c[:, cols] = jnp.where(left, ctx[:tgt], ctx[tgt:]).astype(BF16)
            run_ticks(plan, g * batch + b, steps)

        spec = lambda length: pl.BlockSpec((length, group), lambda g, b: (b, g))
        with jax.named_scope(stage):
            pltpu.emit_pipeline(body, grid=(width // group, batch), in_specs=[spec(tgt), spec(keys), spec(keys)], out_specs=[spec(tgt)])(q_ref, k_src, v_src, c_ref)

    def self_attention():
        heads = min(GROUP, width) // HEAD_DIM
        causal = lax.broadcasted_iota(jnp.int32, (tgt, tgt), 1) <= lax.broadcasted_iota(jnp.int32, (tgt, tgt), 0)

        def prepare(g, b):
            @pl.when(b == 0)
            def _():
                @pl.loop(0, heads)
                def _(h):
                    row = jnp.broadcast_to(dist_s[pl.ds(g * heads + h, 1), :], (tgt, dist_s.shape[1]))
                    bias_s[h] = pltpu.roll(row, 0, 1, stride=1, stride_axis=0)[:, :tgt]

        def mask_scores(scores, h, b):
            allowed = causal & (dec_mask_ref[pl.ds(b, 1), :] > 0)
            return jnp.where(allowed, scores + bias_s[h], MASK_FILL)

        attend('self_attend', tgt, k_ref, v_ref, prepare, mask_scores)

    def cross_attention():
        def mask_scores(scores, h, b):
            return jnp.where(enc_mask_ref[pl.ds(b, 1), :] > 0, scores, MASK_FILL)

        attend('cross_attend', src, ck_ref, cv_ref, lambda g, b: None, mask_scores)

    hidden = big.at[:, pl.ds(0, width)]

    barrier = pltpu.get_barrier_semaphore()
    for j in range(1, N_DEV):
        pl.semaphore_signal(barrier, inc=1, device_id={'fsdp': me ^ j}, device_id_type=MESH)
    pl.semaphore_wait(barrier, N_DEV - 1)

    @pl.loop(0, AHEAD)
    def _(t):
        on_task(t, 0, AHEAD, send)

    def norm_copy(j):
        return pltpu.make_async_remote_copy(src_ref=norm_ref, dst_ref=gain_in.at[me], send_sem=norm_send.at[j], recv_sem=norm_recv.at[j],
                                            device_id={'fsdp': me ^ j}, device_id_type=MESH)

    for j in range(1, N_DEV):
        norm_copy(j).start()
    load_dec = pltpu.make_async_copy(dec_ref, x_s, load_sem)
    load_dec.start()
    load_norm = pltpu.make_async_copy(norm_ref, gain_in.at[me], norm_send.at[0])
    load_norm.start()
    small = [pltpu.make_async_copy(*pair, small_sem.at[k]) for k, pair in enumerate(((rel_in, rel_ref), (dec_mask_in, dec_mask_ref), (enc_mask_in, enc_mask_ref)))]
    for copy in small:
        copy.start()
    plan = stage_ticks('head')

    def head_ticks(begin, end):
        with jax.named_scope('head'):
            @pl.loop(begin, end)
            def _(i):
                tick(i, plan[0], plan[0] + plan[1])

    head_ticks(0, 2)
    for copy in small:
        copy.wait()
    lanes = dist_s.shape[1]
    row = lax.broadcasted_iota(jnp.int32, (lanes, rel_ref.shape[1]), 0)
    distance = jnp.where(row == 0, 0, lanes - row)
    table = jnp.broadcast_to(rel_ref[0:1, :], row.shape)
    for b, start in enumerate(bucket_starts(tgt)):
        table = jnp.where(distance >= start, rel_ref[b + 1:b + 2, :], table)
    dist_s[...] = table.T
    head_ticks(2, 4)
    for j in range(1, N_DEV):
        norm_copy(j).wait()
    load_norm.wait()
    per = width // N_DEV
    for d in range(N_DEV):
        gains[:, d * per:(d + 1) * per] = gain_in[d]
    load_dec.wait()
    norm(0)
    head_ticks(4, plan[1])

    project('self_q', 'self_q', q_ref)
    project('self_k', 'self_k', k_ref)
    project('self_v', 'self_v', v_ref)
    self_attention()
    load(c_ref, hidden)
    residual('self_o', 'self_o')
    for name, dst in (('cross_k', ck_ref), ('cross_v', cv_ref)):
        for half in range(2):
            load(enc_ref.at[pl.ds(half * rows, rows), :], hidden)
            project(name, f'{name}{half}', dst, half)
    norm(1)
    project('cross_q', 'cross_q', q_ref)
    cross_attention()
    load(c_ref, hidden)
    residual('cross_o', 'cross_o')
    norm(2)

    cols = weights['ff_gate'].width // 2
    block = pl.BlockSpec((rows, cols), lambda n: (0, n))

    def store_gate(total, span, n, g):
        g[span, :] = total.astype(BF16)

    def store_lin(total, span, n, g, z):
        act = jax.nn.gelu(g[span, :].astype(F32), approximate=True)
        z[span, :] = (act * total.astype(BF16).astype(F32)).astype(BF16)

    matmul('ff_gate', 'ff_gate', 2, store_gate, out_specs=[block], outs=[g_ref])
    matmul('ff_lin', 'ff_lin', 2, store_lin, in_specs=[block], ins=[g_ref], out_specs=[block], outs=[z_ref])
    load(z_ref, big)
    w = weights['ff_out']

    def ff_out_loop(early, late, total, outs, early_sem, late_sem, out_sem):
        cols, half = w.width, w.rows // 2
        direct = (2, 4, 3, 5)
        begins = lambda j, first: 0 if (j in (2, 3)) == first else half

        def span_of(m):
            return pl.ds(pl.multiple_of(m * row_block, row_block), row_block)

        def cols_of(n):
            return pl.ds(pl.multiple_of(n * cols, cols), cols)

        def product(span, parts):
            terms = [jnp.dot(big[span, pl.ds(pl.multiple_of((me ^ j) * w.rows + at, 128), size)], read(), preferred_element_type=F32) for j, at, size, read in parts]
            return sum(terms[1:], terms[0])

        def add(n, parts, new=False):
            @pl.loop(0, rows // row_block)
            def _(m):
                at = (lax.rem(n, 2), span_of(m), slice(None))
                part = product(span_of(m), parts)
                total[at] = part if new else total[at] + part

        def whole(p, j):
            return (j, 0, w.rows, lambda: early[p])

        def halves(n, first, which):
            return [(j, begins(j, first), half, lambda p=p, j=j: late[lax.rem(n, 2), p, pl.ds(begins(j, first), half), :]) for p, j in enumerate(direct) if j in which]

        def fetch(n, p, j):
            return pltpu.make_async_copy(w.shard.at[:, cols_of(n)] if j == 0 else w.got.at[j - 1, :, cols_of(n)], early.at[p], early_sem.at[p])

        def fetch_half(n, j, first):
            p, span = direct.index(j), pl.ds(begins(j, first), half)
            return pltpu.make_async_copy(w.got.at[j - 1, span, cols_of(n)], late.at[lax.rem(n, 2), p, span], late_sem.at[lax.rem(n, 2), 2 * p + int(first)])

        def out_copy(n):
            return pltpu.make_async_copy(outs.at[lax.rem(n, 2)], out_ref.at[:, cols_of(n)], out_sem.at[lax.rem(n, 2)])

        def task(n):
            return Task(w, n, lax.rem(w.first + n, RING))

        def fetch_early(n):
            for p in (0, 1):
                fetch(n, p, p).start()
            task(n).got_all(SWAP_FIRST, 1)
            for j in direct:
                fetch_half(n, j, True).start()

        def add_own(n):
            for p in (0, 1):
                fetch(n, p, p).wait()
            add(n, [whole(0, 0), whole(1, 1)], new=True)

        def add_first(n):
            for j in direct:
                fetch_half(n, j, True).wait()
            add(n, halves(n, True, direct))

        fetch_early(0)
        add_own(0)
        add_first(0)

        @pl.loop(0, w.count)
        def _(n):
            t = task(n)
            more = n < w.count - 1

            @pl.when(more)
            def _():
                fetch_early(n + 1)

            with jax.named_scope('wait_diagonal'):
                pass_on_diagonal(t)
            fetch(n, 2, 6).start()
            t.swap_d().wait_recv()
            fetch(n, 3, 7).start()
            for p, j in ((2, 6), (3, 7)):
                fetch(n, p, j).wait()
            add(n, [whole(2, 6), whole(3, 7)])
            with jax.named_scope('wait_rest'):
                pass_on_rest(t)
            for j in (2, 4):
                fetch_half(n, j, False).start()
            pl.when(more)(lambda: add_own(n + 1))
            for j in (2, 4):
                fetch_half(n, j, False).wait()
            add(n, halves(n, False, (2, 4)))
            t.got_all(SWAP, 1)
            for j in (3, 5):
                fetch_half(n, j, False).start()
            pl.when(more)(lambda: add_first(n + 1))

            @pl.when(n >= 2)
            def _():
                out_copy(n - 2).wait()

            for j in (3, 5):
                fetch_half(n, j, False).wait()

            @pl.loop(0, rows // row_block)
            def _(m):
                span = span_of(m)
                update = (total[lax.rem(n, 2), span, :] + product(span, halves(n, False, (3, 5)))).astype(BF16)
                outs[lax.rem(n, 2), span, :] = (x_s[span, cols_of(n)].astype(F32) + update.astype(F32)).astype(BF16)

            out_copy(n).start()
            t.sent_all()
            with jax.named_scope('ticks'):
                on_task(out_look + n, out_look, out_look + w.count, arrive, [w])
                on_task(out_look + AHEAD + n, out_look + AHEAD, out_look + AHEAD + w.count, send, [w])

            @pl.when(n == w.count - 1)
            def _():
                out_copy(n - 1).wait()
                out_copy(n).wait()

    dma = pltpu.SemaphoreType.DMA
    with jax.named_scope('ff_out'):
        pl.run_scoped(ff_out_loop, pltpu.VMEM((4, w.rows, w.width), BF16), pltpu.VMEM((2, 4, w.rows, w.width), BF16), pltpu.VMEM((2, rows, w.width), F32),
                      pltpu.VMEM((2, rows, w.width), BF16), dma((4,)), dma((2, 8)), dma((2,)))


def hand_on_kernel(src_ref, dst_ref, held, read_sem, write_sem):
    parts = read_sem.shape[0]
    size = src_ref.shape[0] // parts
    read = lambda k: pltpu.make_async_copy(src_ref.at[pl.ds(k * size, size)], held.at[pl.ds(k * size, size)], read_sem.at[k])
    write = lambda k: pltpu.make_async_copy(held.at[pl.ds(k * size, size)], dst_ref.at[pl.ds(k * size, size)], write_sem.at[k])
    for k in range(parts):
        read(k).start()
    for k in range(parts):
        read(k).wait()
        write(k).start()
    for k in range(parts):
        write(k).wait()


def hand_on(x):
    parts = 12
    any_spec, dma = pl.BlockSpec(memory_space=pl.ANY), pltpu.SemaphoreType.DMA
    return pl.pallas_call(hand_on_kernel, out_shape=jax.ShapeDtypeStruct(x.shape, x.dtype), in_specs=[any_spec], out_specs=any_spec,
                          scratch_shapes=[pltpu.VMEM(x.shape, x.dtype), dma((parts,)), dma((parts,))], name='hand_on')(x)


def local_layer(dec_in, enc_out, dec_mask, enc_mask, rel_bias, norm_self, self_q, self_k, self_v, self_o, norm_cross, cross_q, cross_k, cross_v, cross_o, norm_ff, ff_gate, ff_lin, ff_out):
    batch, tgt, width = dec_in.shape
    src = enc_out.shape[1]
    rows = batch * tgt
    given = dict(self_q=self_q, self_k=self_k, self_v=self_v, self_o=self_o, cross_k=cross_k, cross_v=cross_v, cross_q=cross_q, cross_o=cross_o, ff_gate=ff_gate, ff_lin=ff_lin, ff_out=ff_out)
    names = list(TASKS)
    shards = [given[n] for n in names]
    lanes = -(-2 * tgt // 128) * 128 if tgt % 128 == 0 else -(-(tgt + 1) // 128) * 128
    which = lax.broadcasted_iota(jnp.int32, (8, norm_self.shape[0]), 0)
    norms = jnp.where(which == 0, norm_self[None], jnp.where(which == 1, norm_cross[None], norm_ff[None])).astype(F32)
    any_spec = pl.BlockSpec(memory_space=pl.ANY)
    hbm = lambda *shape: jax.ShapeDtypeStruct(shape, BF16)
    ff = ff_gate.shape[1]
    heads = rel_bias.shape[1]
    outs = [hbm(rows, width)] + [hbm(rows, width)] * 4 + [hbm(batch * src, width)] * 2 + [hbm(rows, ff)] * 2 + [hbm(N_DEV - 1, *s.shape) for s in shards]
    dma = pltpu.SemaphoreType.DMA
    flops = 2 * rows * width * (6 * width + 3 * ff) + 4 * batch * src * width * width
    result = pl.pallas_call(
        lambda *refs: layer_kernel(batch, names, *refs),
        out_shape=outs,
        in_specs=[any_spec] * (6 + len(shards)),
        out_specs=[any_spec] * len(outs),
        scratch_shapes=[
            pltpu.VMEM((rows, width), BF16),
            pltpu.VMEM((rows, ff), BF16),
            pltpu.VMEM((min(GROUP, width) // HEAD_DIM, tgt, tgt), F32),
            pltpu.VMEM((heads, lanes), F32),
            pltpu.VMEM((N_DEV,) + norms.shape, F32),
            pltpu.VMEM((8, width), F32),
            pltpu.VMEM(rel_bias.shape, F32), pltpu.VMEM(dec_mask.shape, jnp.int32), pltpu.VMEM(enc_mask.shape, jnp.int32),
            dma((RING,)), dma((KINDS, RING)), dma((N_DEV,)), dma((N_DEV,)), dma(()), dma((3,)),
        ],
        compiler_params=pltpu.CompilerParams(collective_id=0, has_side_effects=True, vmem_limit_bytes=67_043_328),
        cost_estimate=pl.CostEstimate(flops=flops, bytes_accessed=20 * sum(s.size for s in shards), transcendentals=0),
        name='layer',
    )(rel_bias, dec_mask, enc_mask, norms, dec_in.reshape(rows, width), enc_out.reshape(batch * src, width), *shards)
    return hand_on(result[0]).reshape(dec_in.shape)


def solution(mesh):
    row_spec = P(('dp', 'fsdp'), None, None)
    mask_spec = P(('dp', 'fsdp'), None)
    weight_spec = P('fsdp', None)
    scale_spec = P('fsdp')
    in_specs = (row_spec, row_spec, mask_spec, mask_spec, P(None, None), scale_spec, weight_spec, weight_spec, weight_spec, weight_spec, scale_spec, weight_spec, weight_spec, weight_spec, weight_spec, scale_spec, weight_spec, weight_spec, weight_spec)
    return jax.shard_map(local_layer, mesh=mesh, in_specs=in_specs, out_specs=row_spec, check_vma=False)
```

```python
import math
import jax
import jax.numpy as jnp
from jax import lax
from jax.experimental import pallas as pl
from jax.experimental.pallas import tpu as pltpu
from jax.sharding import PartitionSpec as P

MESH = pl.DeviceIdType.MESH
F32, BF16 = jnp.float32, jnp.bfloat16
HEAD_DIM = 64
NUM_BUCKETS = 32
EXACT_BUCKETS = 16
MAX_DISTANCE = 128
NORM_EPS = 1e-6
MASK_FILL = -1e9
N_DEV = 8

AHEAD, PASS, DONE, RING = 4, 4, 5, 14
PARTNER, FIRST, REST, RELAY, SWAP_FIRST, SWAP, SWAP_D, KINDS = range(8)
TASKS = {'self_q': 8, 'self_k': 8, 'self_v': 8, 'self_o': 8, 'cross_k': 8, 'cross_v': 8, 'cross_q': 8, 'cross_o': 8, 'ff_gate': 20, 'ff_lin': 20, 'ff_out': 16}
ALL_TASKS = sum(TASKS.values())
TICKS = {'head': DONE + 2, 'self_q': 8, 'self_k': 8, 'self_v': 8, 'self_attend': 6, 'self_o': 6, 'cross_k0': 6, 'cross_k1': 5, 'cross_v0': 6, 'cross_v1': 5,
         'cross_q': 6, 'cross_attend': 10, 'cross_o': 6, 'ff_gate': 12, 'ff_lin': 10}
assert sum(TICKS.values()) == ALL_TASKS - TASKS['ff_out'] + DONE
ROW_BLOCK = 512
GROUP = 512


def bucket_ids(length):
    return [offset if offset < EXACT_BUCKETS else min(NUM_BUCKETS - 1, EXACT_BUCKETS + int(math.log(offset / EXACT_BUCKETS) / math.log(MAX_DISTANCE / EXACT_BUCKETS) * (NUM_BUCKETS - EXACT_BUCKETS))) for offset in range(length)]


def bucket_starts(length):
    ids = bucket_ids(length)
    return [next(n for n in range(length) if ids[n] >= b) for b in range(1, ids[-1] + 1)]


class Weight:
    def __init__(self, first, count, shard, got):
        self.first, self.count, self.shard, self.got = first, count, shard, got
        self.rows, self.width = shard.shape[0], shard.shape[1] // count


def layer_kernel(batch, names, rel_in, dec_mask_in, enc_mask_in, norm_ref, dec_ref, enc_ref, *refs):
    n_w = len(names)
    shards, refs = refs[:n_w], refs[n_w:]
    out_ref, q_ref, k_ref, v_ref, c_ref, ck_ref, cv_ref, g_ref, z_ref = refs[:9]
    gots, refs = refs[9:9 + n_w], refs[9 + n_w:]
    x_s, big, bias_s, dist_s, gain_in, gains, rel_ref, dec_mask_ref, enc_mask_ref, send_sem, recv_sem, norm_send, norm_recv, load_sem, small_sem = refs

    me = lax.axis_index('fsdp')
    weights, first = {}, 0
    for name, shard, got in zip(names, shards, gots):
        weights[name] = Weight(first, TASKS[name], shard, got)
        first += TASKS[name]
    rows, width = dec_ref.shape
    tgt = rows // batch
    src = enc_ref.shape[0] // batch
    row_block = min(ROW_BLOCK, rows)

    def remote(src_ref, dst_ref, kind, ring, bit):
        return pltpu.make_async_remote_copy(src_ref=src_ref, dst_ref=dst_ref, send_sem=send_sem.at[ring], recv_sem=recv_sem.at[kind, ring],
                                            device_id={'fsdp': me ^ bit}, device_id_type=MESH)

    class Task:
        def __init__(self, w, m, ring):
            cols = pl.ds(pl.multiple_of(m * w.width, w.width), w.width)
            own = w.shard.at[:, cols]
            slot = lambda j: w.got.at[j - 1, :, cols]
            bottom, top = pl.ds(0, w.rows // 2), pl.ds(w.rows // 2, w.rows // 2)
            low = lambda j: w.got.at[j - 1, bottom, cols]
            high = lambda j: w.got.at[j - 1, top, cols]
            self.to_partner = lambda: remote(own, slot(1), PARTNER, ring, 1)
            self.first_x = lambda: remote(w.shard.at[bottom, cols], low(2), FIRST, ring, 2)
            self.first_y = lambda: remote(w.shard.at[top, cols], high(4), FIRST, ring, 4)
            self.rest_x = lambda: remote(w.shard.at[top, cols], high(2), REST, ring, 2)
            self.rest_y = lambda: remote(w.shard.at[bottom, cols], low(4), REST, ring, 4)
            self.relay_y = lambda: remote(low(2), low(6), RELAY, ring, 4)
            self.relay_x = lambda: remote(high(4), high(6), RELAY, ring, 2)
            self.swap_x = lambda: remote(slot(2), slot(3), SWAP, ring, 1)
            self.swap_y = lambda: remote(slot(4), slot(5), SWAP, ring, 1)
            self.swap_d = lambda: remote(slot(6), slot(7), SWAP_D, ring, 1)
            self.swap_first_x = lambda: remote(low(2), low(3), SWAP_FIRST, ring, 1)
            self.swap_first_y = lambda: remote(high(4), high(5), SWAP_FIRST, ring, 1)
            self.swap_rest_x = lambda: remote(high(2), high(3), SWAP, ring, 1)
            self.swap_rest_y = lambda: remote(low(4), low(5), SWAP, ring, 1)
            self.halves = w is weights['ff_out']
            shape = lambda slots: w.got.at[pl.ds(0, slots), :, cols]
            self.got_all = lambda kind, slots: remote(shape(slots), shape(slots), kind, ring, 1).wait_recv()
            self.sent_all = lambda: remote(shape(7), shape(7), PARTNER, ring, 1).wait_send()

    def send(t):
        for copy in (t.first_x, t.first_y, t.to_partner):
            copy().start()

    def arrive(t):
        t.to_partner().wait_recv()
        t.got_all(FIRST, 1)
        for copy in (t.relay_y, t.relay_x, t.rest_y, t.rest_x, *((t.swap_first_x, t.swap_first_y) if t.halves else ())):
            copy().start()

    def pass_on_diagonal(t):
        t.got_all(RELAY, 1)
        t.swap_d().start()

    def pass_on_rest(t):
        t.got_all(REST, 1)
        for copy in (t.swap_rest_x, t.swap_rest_y) if t.halves else (t.swap_x, t.swap_y):
            copy().start()

    def pass_on(t):
        pass_on_diagonal(t)
        pass_on_rest(t)

    def finish(t):
        t.swap_d().wait_recv()
        t.got_all(SWAP, 2)
        t.sent_all()

    def on_task(t, low, high, act, among=None, stop=ALL_TASKS):
        for w in among or weights.values():
            last = min(w.first + w.count, stop)
            if low < last and w.first < high:
                def run(w=w):
                    act(Task(w, t - w.first, lax.rem(t, RING)))
                if w.first <= low and high <= last:
                    run()
                else:
                    pl.when((t >= w.first) & (t < last))(run)

    streamed = [w for name, w in weights.items() if name != 'ff_out']
    out_look = weights['ff_out'].first + PASS

    def tick(i, low, high):
        on_task(i, low, high, arrive, stop=out_look)
        on_task(i + AHEAD, low + AHEAD, high + AHEAD, send, stop=out_look + AHEAD)
        on_task(i - PASS, low - PASS, high - PASS, pass_on, streamed)
        on_task(i - DONE, low - DONE, high - DONE, finish, streamed)

    done = [0]

    def stage_ticks(name):
        low, count = done[0], TICKS[name]
        done[0] = low + count
        return low, count

    def ticks_before(plan, n, steps, least=min):
        low, count = plan
        spread = steps if count == steps else max(steps - 4, 1)
        return low + least((n * count) // spread, count)

    def run_ticks(plan, n, steps):
        with jax.named_scope('ticks'):
            @pl.loop(ticks_before(plan, n, steps, jnp.minimum), ticks_before(plan, n + 1, steps, jnp.minimum))
            def _(i):
                tick(i, plan[0], plan[0] + plan[1])

    def load(src_ref, dst_ref):
        copy = pltpu.make_async_copy(src_ref, dst_ref, load_sem)
        copy.start()
        copy.wait()

    def norm(which):
        @pl.loop(0, rows // 16)
        def _(r):
            span = pl.ds(pl.multiple_of(r * 16, 16), 16)
            v = x_s[span, :].astype(F32)
            scale = lax.rsqrt(jnp.mean(v * v, axis=-1, keepdims=True) + NORM_EPS)
            big[span, pl.ds(0, width)] = (v * scale * gains[pl.ds(which, 1), :]).astype(BF16)

    def matmul(name, stage, split, store, in_specs=(), ins=(), out_specs=(), outs=()):
        w = weights[name]
        steps, cols = w.count * split, w.width // split
        plan = stage_ticks(stage)
        for n in range(steps):
            assert ticks_before(plan, n, steps) > w.first + min(n + 1, steps - 1) // split + DONE

        def body(own, got, *rest):
            n = pl.program_id(0)

            @pl.loop(0, rows // row_block)
            def _(m):
                span = pl.ds(pl.multiple_of(m * row_block, row_block), row_block)
                total = None
                for j in range(N_DEV):
                    part = big[span, pl.ds(pl.multiple_of((me ^ j) * w.rows, 128), w.rows)]
                    term = jnp.dot(part, own[...] if j == 0 else got[j - 1], preferred_element_type=F32)
                    total = term if total is None else total + term
                store(total, span, n, *rest)

            run_ticks(plan, n, steps)

        with jax.named_scope(stage):
            pltpu.emit_pipeline(
                body, grid=(steps,),
                in_specs=[pl.BlockSpec((w.rows, cols), lambda n: (0, n)), pl.BlockSpec((N_DEV - 1, w.rows, cols), lambda n: (0, 0, n)), *in_specs],
                out_specs=list(out_specs))(w.shard, w.got, *ins, *outs)

    def project(name, stage, dst_ref, half=0):
        cols = weights[name].width

        def store(total, span, n, dst):
            dst[span, :] = total.astype(BF16)

        matmul(name, stage, 1, store, out_specs=[pl.BlockSpec((rows, cols), lambda n: (half, n))], outs=[dst_ref])

    def residual(name, stage):
        cols = weights[name].width

        def store(total, span, n):
            where = (span, pl.ds(pl.multiple_of(n * cols, cols), cols))
            x_s[where] = (x_s[where].astype(F32) + total.astype(BF16).astype(F32)).astype(BF16)

        matmul(name, stage, 1, store)

    left = lax.broadcasted_iota(jnp.int32, (tgt, 2 * HEAD_DIM), 1) < HEAD_DIM

    def softmax(scores):
        e = jnp.exp(scores - jnp.max(scores, axis=-1, keepdims=True))
        return (e * (1.0 / jnp.sum(e, axis=-1, keepdims=True))).astype(BF16)

    def attend(stage, keys, k_src, v_src, prepare, mask_scores):
        group = min(GROUP, width)
        plan = stage_ticks(stage)
        steps = (width // group) * batch

        def body(q, k, v, c):
            g, b = pl.program_id(0), pl.program_id(1)
            prepare(g, b)
            for pair in range(group // (2 * HEAD_DIM)):
                cols = pl.ds(pair * 2 * HEAD_DIM, 2 * HEAD_DIM)
                q_pair = q[:, cols].astype(F32)
                both = jnp.concatenate([jnp.where(left, q_pair, 0.0), jnp.where(left, 0.0, q_pair)], 0).astype(BF16)
                scores = lax.dot_general(both, k[:, cols], (((1,), (1,)), ((), ())), preferred_element_type=F32)
                prob = jnp.concatenate([softmax(mask_scores(scores[h * tgt:(h + 1) * tgt], 2 * pair + h, b)) for h in range(2)], 0)
                ctx = jnp.dot(prob, v[:, cols], preferred_element_type=F32)
                c[:, cols] = jnp.where(left, ctx[:tgt], ctx[tgt:]).astype(BF16)
            run_ticks(plan, g * batch + b, steps)

        spec = lambda length: pl.BlockSpec((length, group), lambda g, b: (b, g))
        with jax.named_scope(stage):
            pltpu.emit_pipeline(body, grid=(width // group, batch), in_specs=[spec(tgt), spec(keys), spec(keys)], out_specs=[spec(tgt)])(q_ref, k_src, v_src, c_ref)

    def self_attention():
        heads = min(GROUP, width) // HEAD_DIM
        causal = lax.broadcasted_iota(jnp.int32, (tgt, tgt), 1) <= lax.broadcasted_iota(jnp.int32, (tgt, tgt), 0)

        def prepare(g, b):
            @pl.when(b == 0)
            def _():
                @pl.loop(0, heads)
                def _(h):
                    row = jnp.broadcast_to(dist_s[pl.ds(g * heads + h, 1), :], (tgt, dist_s.shape[1]))
                    bias_s[h] = pltpu.roll(row, 0, 1, stride=1, stride_axis=0)[:, :tgt]

        def mask_scores(scores, h, b):
            allowed = causal & (dec_mask_ref[pl.ds(b, 1), :] > 0)
            return jnp.where(allowed, scores + bias_s[h], MASK_FILL)

        attend('self_attend', tgt, k_ref, v_ref, prepare, mask_scores)

    def cross_attention():
        def mask_scores(scores, h, b):
            return jnp.where(enc_mask_ref[pl.ds(b, 1), :] > 0, scores, MASK_FILL)

        attend('cross_attend', src, ck_ref, cv_ref, lambda g, b: None, mask_scores)

    hidden = big.at[:, pl.ds(0, width)]

    barrier = pltpu.get_barrier_semaphore()
    for j in range(1, N_DEV):
        pl.semaphore_signal(barrier, inc=1, device_id={'fsdp': me ^ j}, device_id_type=MESH)
    pl.semaphore_wait(barrier, N_DEV - 1)

    @pl.loop(0, AHEAD)
    def _(t):
        on_task(t, 0, AHEAD, send)

    def norm_copy(j):
        return pltpu.make_async_remote_copy(src_ref=norm_ref, dst_ref=gain_in.at[me], send_sem=norm_send.at[j], recv_sem=norm_recv.at[j],
                                            device_id={'fsdp': me ^ j}, device_id_type=MESH)

    for j in range(1, N_DEV):
        norm_copy(j).start()
    load_dec = pltpu.make_async_copy(dec_ref, x_s, load_sem)
    load_dec.start()
    load_norm = pltpu.make_async_copy(norm_ref, gain_in.at[me], norm_send.at[0])
    load_norm.start()
    small = [pltpu.make_async_copy(*pair, small_sem.at[k]) for k, pair in enumerate(((rel_in, rel_ref), (dec_mask_in, dec_mask_ref), (enc_mask_in, enc_mask_ref)))]
    for copy in small:
        copy.start()
    plan = stage_ticks('head')

    def head_ticks(begin, end):
        with jax.named_scope('head'):
            @pl.loop(begin, end)
            def _(i):
                tick(i, plan[0], plan[0] + plan[1])

    head_ticks(0, 2)
    for copy in small:
        copy.wait()
    lanes = dist_s.shape[1]
    row = lax.broadcasted_iota(jnp.int32, (lanes, rel_ref.shape[1]), 0)
    distance = jnp.where(row == 0, 0, lanes - row)
    table = jnp.broadcast_to(rel_ref[0:1, :], row.shape)
    for b, start in enumerate(bucket_starts(tgt)):
        table = jnp.where(distance >= start, rel_ref[b + 1:b + 2, :], table)
    dist_s[...] = table.T
    head_ticks(2, 4)
    for j in range(1, N_DEV):
        norm_copy(j).wait()
    load_norm.wait()
    per = width // N_DEV
    for d in range(N_DEV):
        gains[:, d * per:(d + 1) * per] = gain_in[d]
    load_dec.wait()
    norm(0)
    head_ticks(4, plan[1])

    project('self_q', 'self_q', q_ref)
    project('self_k', 'self_k', k_ref)
    project('self_v', 'self_v', v_ref)
    self_attention()
    load(c_ref, hidden)
    residual('self_o', 'self_o')
    for name, dst in (('cross_k', ck_ref), ('cross_v', cv_ref)):
        for half in range(2):
            load(enc_ref.at[pl.ds(half * rows, rows), :], hidden)
            project(name, f'{name}{half}', dst, half)
    norm(1)
    project('cross_q', 'cross_q', q_ref)
    cross_attention()
    load(c_ref, hidden)
    residual('cross_o', 'cross_o')
    norm(2)

    cols = weights['ff_gate'].width // 2
    block = pl.BlockSpec((rows, cols), lambda n: (0, n))

    def store_gate(total, span, n, g):
        g[span, :] = total.astype(BF16)

    def store_lin(total, span, n, g, z):
        act = jax.nn.gelu(g[span, :].astype(F32), approximate=True)
        z[span, :] = (act * total.astype(BF16).astype(F32)).astype(BF16)

    matmul('ff_gate', 'ff_gate', 2, store_gate, out_specs=[block], outs=[g_ref])
    matmul('ff_lin', 'ff_lin', 2, store_lin, in_specs=[block], ins=[g_ref], out_specs=[block], outs=[z_ref])
    load(z_ref, big)
    w = weights['ff_out']

    def ff_out_loop(early, late, total, outs, early_sem, late_sem, out_sem):
        cols, half = w.width, w.rows // 2
        direct = (2, 4, 3, 5)
        begins = lambda j, first: 0 if (j in (2, 3)) == first else half

        def span_of(m):
            return pl.ds(pl.multiple_of(m * row_block, row_block), row_block)

        def cols_of(n):
            return pl.ds(pl.multiple_of(n * cols, cols), cols)

        def product(span, parts):
            terms = [jnp.dot(big[span, pl.ds(pl.multiple_of((me ^ j) * w.rows + at, 128), size)], read(), preferred_element_type=F32) for j, at, size, read in parts]
            return sum(terms[1:], terms[0])

        def add(n, parts, new=False):
            @pl.loop(0, rows // row_block)
            def _(m):
                at = (lax.rem(n, 2), span_of(m), slice(None))
                part = product(span_of(m), parts)
                total[at] = part if new else total[at] + part

        def whole(p, j):
            return (j, 0, w.rows, lambda: early[p])

        def halves(n, first, which):
            return [(j, begins(j, first), half, lambda p=p, j=j: late[lax.rem(n, 2), p, pl.ds(begins(j, first), half), :]) for p, j in enumerate(direct) if j in which]

        def fetch(n, p, j):
            return pltpu.make_async_copy(w.shard.at[:, cols_of(n)] if j == 0 else w.got.at[j - 1, :, cols_of(n)], early.at[p], early_sem.at[p])

        def fetch_half(n, j, first):
            p, span = direct.index(j), pl.ds(begins(j, first), half)
            return pltpu.make_async_copy(w.got.at[j - 1, span, cols_of(n)], late.at[lax.rem(n, 2), p, span], late_sem.at[lax.rem(n, 2), 2 * p + int(first)])

        def out_copy(n):
            return pltpu.make_async_copy(outs.at[lax.rem(n, 2)], out_ref.at[:, cols_of(n)], out_sem.at[lax.rem(n, 2)])

        def task(n):
            return Task(w, n, lax.rem(w.first + n, RING))

        def fetch_early(n):
            for p in (0, 1):
                fetch(n, p, p).start()
            task(n).got_all(SWAP_FIRST, 1)
            for j in direct:
                fetch_half(n, j, True).start()

        def add_own(n):
            for p in (0, 1):
                fetch(n, p, p).wait()
            add(n, [whole(0, 0), whole(1, 1)], new=True)

        def add_first(n):
            for j in direct:
                fetch_half(n, j, True).wait()
            add(n, halves(n, True, direct))

        fetch_early(0)
        add_own(0)

        @pl.loop(0, w.count)
        def _(n):
            t = task(n)
            more = n < w.count - 1

            @pl.when(more)
            def _():
                fetch_early(n + 1)

            with jax.named_scope('wait_diagonal'):
                pass_on_diagonal(t)
            fetch(n, 2, 6).start()
            add_first(n)
            t.swap_d().wait_recv()
            fetch(n, 3, 7).start()
            for p, j in ((2, 6), (3, 7)):
                fetch(n, p, j).wait()
                add(n, [whole(p, j)])
            with jax.named_scope('wait_rest'):
                pass_on_rest(t)
            for j in (2, 4):
                fetch_half(n, j, False).start()
            pl.when(more)(lambda: add_own(n + 1))
            for j in (2, 4):
                fetch_half(n, j, False).wait()
            add(n, halves(n, False, (2, 4)))
            t.got_all(SWAP, 1)
            for j in (3, 5):
                fetch_half(n, j, False).start()

            @pl.when(n >= 2)
            def _():
                out_copy(n - 2).wait()

            for j in (3, 5):
                fetch_half(n, j, False).wait()

            @pl.loop(0, rows // row_block)
            def _(m):
                span = span_of(m)
                update = (total[lax.rem(n, 2), span, :] + product(span, halves(n, False, (3, 5)))).astype(BF16)
                outs[lax.rem(n, 2), span, :] = (x_s[span, cols_of(n)].astype(F32) + update.astype(F32)).astype(BF16)

            out_copy(n).start()
            t.sent_all()
            with jax.named_scope('ticks'):
                on_task(out_look + n, out_look, out_look + w.count, arrive, [w])
                on_task(out_look + AHEAD + n, out_look + AHEAD, out_look + AHEAD + w.count, send, [w])

            @pl.when(n == w.count - 1)
            def _():
                out_copy(n - 1).wait()
                out_copy(n).wait()

    dma = pltpu.SemaphoreType.DMA
    with jax.named_scope('ff_out'):
        pl.run_scoped(ff_out_loop, pltpu.VMEM((4, w.rows, w.width), BF16), pltpu.VMEM((2, 4, w.rows, w.width), BF16), pltpu.VMEM((2, rows, w.width), F32),
                      pltpu.VMEM((2, rows, w.width), BF16), dma((4,)), dma((2, 8)), dma((2,)))


def hand_on_kernel(src_ref, dst_ref, held, read_sem, write_sem):
    parts = read_sem.shape[0]
    size = src_ref.shape[0] // parts
    read = lambda k: pltpu.make_async_copy(src_ref.at[pl.ds(k * size, size)], held.at[pl.ds(k * size, size)], read_sem.at[k])
    write = lambda k: pltpu.make_async_copy(held.at[pl.ds(k * size, size)], dst_ref.at[pl.ds(k * size, size)], write_sem.at[k])
    for k in range(parts):
        read(k).start()
    for k in range(parts):
        read(k).wait()
        write(k).start()
    for k in range(parts):
        write(k).wait()


def hand_on(x):
    parts = 12
    any_spec, dma = pl.BlockSpec(memory_space=pl.ANY), pltpu.SemaphoreType.DMA
    return pl.pallas_call(hand_on_kernel, out_shape=jax.ShapeDtypeStruct(x.shape, x.dtype), in_specs=[any_spec], out_specs=any_spec,
                          scratch_shapes=[pltpu.VMEM(x.shape, x.dtype), dma((parts,)), dma((parts,))], name='hand_on')(x)


def local_layer(dec_in, enc_out, dec_mask, enc_mask, rel_bias, norm_self, self_q, self_k, self_v, self_o, norm_cross, cross_q, cross_k, cross_v, cross_o, norm_ff, ff_gate, ff_lin, ff_out):
    batch, tgt, width = dec_in.shape
    src = enc_out.shape[1]
    rows = batch * tgt
    given = dict(self_q=self_q, self_k=self_k, self_v=self_v, self_o=self_o, cross_k=cross_k, cross_v=cross_v, cross_q=cross_q, cross_o=cross_o, ff_gate=ff_gate, ff_lin=ff_lin, ff_out=ff_out)
    names = list(TASKS)
    shards = [given[n] for n in names]
    lanes = -(-2 * tgt // 128) * 128 if tgt % 128 == 0 else -(-(tgt + 1) // 128) * 128
    which = lax.broadcasted_iota(jnp.int32, (8, norm_self.shape[0]), 0)
    norms = jnp.where(which == 0, norm_self[None], jnp.where(which == 1, norm_cross[None], norm_ff[None])).astype(F32)
    any_spec = pl.BlockSpec(memory_space=pl.ANY)
    hbm = lambda *shape: jax.ShapeDtypeStruct(shape, BF16)
    ff = ff_gate.shape[1]
    heads = rel_bias.shape[1]
    outs = [hbm(rows, width)] + [hbm(rows, width)] * 4 + [hbm(batch * src, width)] * 2 + [hbm(rows, ff)] * 2 + [hbm(N_DEV - 1, *s.shape) for s in shards]
    dma = pltpu.SemaphoreType.DMA
    flops = 2 * rows * width * (6 * width + 3 * ff) + 4 * batch * src * width * width
    result = pl.pallas_call(
        lambda *refs: layer_kernel(batch, names, *refs),
        out_shape=outs,
        in_specs=[any_spec] * (6 + len(shards)),
        out_specs=[any_spec] * len(outs),
        scratch_shapes=[
            pltpu.VMEM((rows, width), BF16),
            pltpu.VMEM((rows, ff), BF16),
            pltpu.VMEM((min(GROUP, width) // HEAD_DIM, tgt, tgt), F32),
            pltpu.VMEM((heads, lanes), F32),
            pltpu.VMEM((N_DEV,) + norms.shape, F32),
            pltpu.VMEM((8, width), F32),
            pltpu.VMEM(rel_bias.shape, F32), pltpu.VMEM(dec_mask.shape, jnp.int32), pltpu.VMEM(enc_mask.shape, jnp.int32),
            dma((RING,)), dma((KINDS, RING)), dma((N_DEV,)), dma((N_DEV,)), dma(()), dma((3,)),
        ],
        compiler_params=pltpu.CompilerParams(collective_id=0, has_side_effects=True, vmem_limit_bytes=67_043_328),
        cost_estimate=pl.CostEstimate(flops=flops, bytes_accessed=20 * sum(s.size for s in shards), transcendentals=0),
        name='layer',
    )(rel_bias, dec_mask, enc_mask, norms, dec_in.reshape(rows, width), enc_out.reshape(batch * src, width), *shards)
    return hand_on(result[0]).reshape(dec_in.shape)


def solution(mesh):
    row_spec = P(('dp', 'fsdp'), None, None)
    mask_spec = P(('dp', 'fsdp'), None)
    weight_spec = P('fsdp', None)
    scale_spec = P('fsdp')
    in_specs = (row_spec, row_spec, mask_spec, mask_spec, P(None, None), scale_spec, weight_spec, weight_spec, weight_spec, weight_spec, scale_spec, weight_spec, weight_spec, weight_spec, weight_spec, scale_spec, weight_spec, weight_spec, weight_spec)
    return jax.shard_map(local_layer, mesh=mesh, in_specs=in_specs, out_specs=row_spec, check_vma=False)
```

```python
import math
import jax
import jax.numpy as jnp
from jax import lax
from jax.experimental import pallas as pl
from jax.experimental.pallas import tpu as pltpu
from jax.sharding import PartitionSpec as P

MESH = pl.DeviceIdType.MESH
F32, BF16 = jnp.float32, jnp.bfloat16
HEAD_DIM = 64
NUM_BUCKETS = 32
EXACT_BUCKETS = 16
MAX_DISTANCE = 128
NORM_EPS = 1e-6
MASK_FILL = -1e9
N_DEV = 8

AHEAD, PASS, DONE, RING = 4, 4, 5, 14
PARTNER, FIRST, REST, RELAY, SWAP_FIRST, SWAP, SWAP_D, KINDS = range(8)
TASKS = {'self_q': 8, 'self_k': 8, 'self_v': 8, 'self_o': 8, 'cross_k': 8, 'cross_v': 8, 'cross_q': 8, 'cross_o': 8, 'ff_gate': 20, 'ff_lin': 20, 'ff_out': 16}
ALL_TASKS = sum(TASKS.values())
TICKS = {'head': DONE + 2, 'self_q': 8, 'self_k': 8, 'self_v': 8, 'self_attend': 6, 'self_o': 6, 'cross_k0': 6, 'cross_k1': 5, 'cross_v0': 6, 'cross_v1': 5,
         'cross_q': 6, 'cross_attend': 10, 'cross_o': 6, 'ff_gate': 12, 'ff_lin': 10}
assert sum(TICKS.values()) == ALL_TASKS - TASKS['ff_out'] + DONE
ROW_BLOCK = 512
GROUP = 512


def bucket_ids(length):
    return [offset if offset < EXACT_BUCKETS else min(NUM_BUCKETS - 1, EXACT_BUCKETS + int(math.log(offset / EXACT_BUCKETS) / math.log(MAX_DISTANCE / EXACT_BUCKETS) * (NUM_BUCKETS - EXACT_BUCKETS))) for offset in range(length)]


def bucket_starts(length):
    ids = bucket_ids(length)
    return [next(n for n in range(length) if ids[n] >= b) for b in range(1, ids[-1] + 1)]


class Weight:
    def __init__(self, first, count, shard, got):
        self.first, self.count, self.shard, self.got = first, count, shard, got
        self.rows, self.width = shard.shape[0], shard.shape[1] // count


def layer_kernel(batch, names, rel_in, dec_mask_in, enc_mask_in, norm_ref, dec_ref, enc_ref, *refs):
    n_w = len(names)
    shards, refs = refs[:n_w], refs[n_w:]
    out_ref, q_ref, k_ref, v_ref, c_ref, ck_ref, cv_ref, g_ref, z_ref = refs[:9]
    gots, refs = refs[9:9 + n_w], refs[9 + n_w:]
    x_s, big, bias_s, dist_s, gain_in, gains, rel_ref, dec_mask_ref, enc_mask_ref, send_sem, recv_sem, norm_send, norm_recv, load_sem, small_sem = refs

    me = lax.axis_index('fsdp')
    weights, first = {}, 0
    for name, shard, got in zip(names, shards, gots):
        weights[name] = Weight(first, TASKS[name], shard, got)
        first += TASKS[name]
    rows, width = dec_ref.shape
    tgt = rows // batch
    src = enc_ref.shape[0] // batch
    row_block = min(ROW_BLOCK, rows)

    def remote(src_ref, dst_ref, kind, ring, bit):
        return pltpu.make_async_remote_copy(src_ref=src_ref, dst_ref=dst_ref, send_sem=send_sem.at[ring], recv_sem=recv_sem.at[kind, ring],
                                            device_id={'fsdp': me ^ bit}, device_id_type=MESH)

    class Task:
        def __init__(self, w, m, ring):
            cols = pl.ds(pl.multiple_of(m * w.width, w.width), w.width)
            own = w.shard.at[:, cols]
            slot = lambda j: w.got.at[j - 1, :, cols]
            bottom, top = pl.ds(0, w.rows // 2), pl.ds(w.rows // 2, w.rows // 2)
            low = lambda j: w.got.at[j - 1, bottom, cols]
            high = lambda j: w.got.at[j - 1, top, cols]
            self.to_partner = lambda: remote(own, slot(1), PARTNER, ring, 1)
            self.first_x = lambda: remote(w.shard.at[bottom, cols], low(2), FIRST, ring, 2)
            self.first_y = lambda: remote(w.shard.at[top, cols], high(4), FIRST, ring, 4)
            self.rest_x = lambda: remote(w.shard.at[top, cols], high(2), REST, ring, 2)
            self.rest_y = lambda: remote(w.shard.at[bottom, cols], low(4), REST, ring, 4)
            self.relay_y = lambda: remote(low(2), low(6), RELAY, ring, 4)
            self.relay_x = lambda: remote(high(4), high(6), RELAY, ring, 2)
            self.swap_x = lambda: remote(slot(2), slot(3), SWAP, ring, 1)
            self.swap_y = lambda: remote(slot(4), slot(5), SWAP, ring, 1)
            self.swap_d = lambda: remote(slot(6), slot(7), SWAP_D, ring, 1)
            self.swap_first_x = lambda: remote(low(2), low(3), SWAP_FIRST, ring, 1)
            self.swap_first_y = lambda: remote(high(4), high(5), SWAP_FIRST, ring, 1)
            self.swap_rest_x = lambda: remote(high(2), high(3), SWAP, ring, 1)
            self.swap_rest_y = lambda: remote(low(4), low(5), SWAP, ring, 1)
            self.halves = w is weights['ff_out']
            shape = lambda slots: w.got.at[pl.ds(0, slots), :, cols]
            self.got_all = lambda kind, slots: remote(shape(slots), shape(slots), kind, ring, 1).wait_recv()
            self.sent_all = lambda: remote(shape(7), shape(7), PARTNER, ring, 1).wait_send()

    def send(t):
        for copy in (t.first_x, t.first_y, t.to_partner):
            copy().start()

    def arrive(t):
        t.to_partner().wait_recv()
        t.got_all(FIRST, 1)
        for copy in (t.relay_y, t.relay_x, t.rest_y, t.rest_x, *((t.swap_first_x, t.swap_first_y) if t.halves else ())):
            copy().start()

    def pass_on_diagonal(t):
        t.got_all(RELAY, 1)
        t.swap_d().start()

    def pass_on_rest(t):
        t.got_all(REST, 1)
        for copy in (t.swap_rest_x, t.swap_rest_y) if t.halves else (t.swap_x, t.swap_y):
            copy().start()

    def pass_on(t):
        pass_on_diagonal(t)
        pass_on_rest(t)

    def finish(t):
        t.swap_d().wait_recv()
        t.got_all(SWAP, 2)
        t.sent_all()

    def on_task(t, low, high, act, among=None, stop=ALL_TASKS):
        for w in among or weights.values():
            last = min(w.first + w.count, stop)
            if low < last and w.first < high:
                def run(w=w):
                    act(Task(w, t - w.first, lax.rem(t, RING)))
                if w.first <= low and high <= last:
                    run()
                else:
                    pl.when((t >= w.first) & (t < last))(run)

    streamed = [w for name, w in weights.items() if name != 'ff_out']
    out_look = weights['ff_out'].first + PASS

    def tick(i, low, high):
        on_task(i, low, high, arrive, stop=out_look)
        on_task(i + AHEAD, low + AHEAD, high + AHEAD, send, stop=out_look + AHEAD)
        on_task(i - PASS, low - PASS, high - PASS, pass_on, streamed)
        on_task(i - DONE, low - DONE, high - DONE, finish, streamed)

    done = [0]

    def stage_ticks(name):
        low, count = done[0], TICKS[name]
        done[0] = low + count
        return low, count

    def ticks_before(plan, n, steps, least=min):
        low, count = plan
        spread = steps if count == steps else max(steps - 4, 1)
        return low + least((n * count) // spread, count)

    def run_ticks(plan, n, steps):
        with jax.named_scope('ticks'):
            @pl.loop(ticks_before(plan, n, steps, jnp.minimum), ticks_before(plan, n + 1, steps, jnp.minimum))
            def _(i):
                tick(i, plan[0], plan[0] + plan[1])

    def load(src_ref, dst_ref):
        copy = pltpu.make_async_copy(src_ref, dst_ref, load_sem)
        copy.start()
        copy.wait()

    def norm(which):
        @pl.loop(0, rows // 16)
        def _(r):
            span = pl.ds(pl.multiple_of(r * 16, 16), 16)
            v = x_s[span, :].astype(F32)
            scale = lax.rsqrt(jnp.mean(v * v, axis=-1, keepdims=True) + NORM_EPS)
            big[span, pl.ds(0, width)] = (v * scale * gains[pl.ds(which, 1), :]).astype(BF16)

    def matmul(name, stage, split, store, in_specs=(), ins=(), out_specs=(), outs=()):
        w = weights[name]
        steps, cols = w.count * split, w.width // split
        plan = stage_ticks(stage)
        for n in range(steps):
            assert ticks_before(plan, n, steps) > w.first + min(n + 1, steps - 1) // split + DONE

        def body(own, got, *rest):
            n = pl.program_id(0)

            @pl.loop(0, rows // row_block)
            def _(m):
                span = pl.ds(pl.multiple_of(m * row_block, row_block), row_block)
                total = None
                for j in range(N_DEV):
                    part = big[span, pl.ds(pl.multiple_of((me ^ j) * w.rows, 128), w.rows)]
                    term = jnp.dot(part, own[...] if j == 0 else got[j - 1], preferred_element_type=F32)
                    total = term if total is None else total + term
                store(total, span, n, *rest)

            run_ticks(plan, n, steps)

        with jax.named_scope(stage):
            pltpu.emit_pipeline(
                body, grid=(steps,),
                in_specs=[pl.BlockSpec((w.rows, cols), lambda n: (0, n)), pl.BlockSpec((N_DEV - 1, w.rows, cols), lambda n: (0, 0, n)), *in_specs],
                out_specs=list(out_specs))(w.shard, w.got, *ins, *outs)

    def project(name, stage, dst_ref, half=0):
        cols = weights[name].width

        def store(total, span, n, dst):
            dst[span, :] = total.astype(BF16)

        matmul(name, stage, 1, store, out_specs=[pl.BlockSpec((rows, cols), lambda n: (half, n))], outs=[dst_ref])

    def residual(name, stage):
        cols = weights[name].width

        def store(total, span, n):
            where = (span, pl.ds(pl.multiple_of(n * cols, cols), cols))
            x_s[where] = (x_s[where].astype(F32) + total.astype(BF16).astype(F32)).astype(BF16)

        matmul(name, stage, 1, store)

    left = lax.broadcasted_iota(jnp.int32, (tgt, 2 * HEAD_DIM), 1) < HEAD_DIM

    def softmax(scores):
        e = jnp.exp(scores - jnp.max(scores, axis=-1, keepdims=True))
        return (e * (1.0 / jnp.sum(e, axis=-1, keepdims=True))).astype(BF16)

    def attend(stage, keys, k_src, v_src, prepare, mask_scores):
        group = min(GROUP, width)
        plan = stage_ticks(stage)
        steps = (width // group) * batch

        def body(q, k, v, c):
            g, b = pl.program_id(0), pl.program_id(1)
            prepare(g, b)
            for pair in range(group // (2 * HEAD_DIM)):
                cols = pl.ds(pair * 2 * HEAD_DIM, 2 * HEAD_DIM)
                q_pair = q[:, cols].astype(F32)
                both = jnp.concatenate([jnp.where(left, q_pair, 0.0), jnp.where(left, 0.0, q_pair)], 0).astype(BF16)
                scores = lax.dot_general(both, k[:, cols], (((1,), (1,)), ((), ())), preferred_element_type=F32)
                prob = jnp.concatenate([softmax(mask_scores(scores[h * tgt:(h + 1) * tgt], 2 * pair + h, b)) for h in range(2)], 0)
                ctx = jnp.dot(prob, v[:, cols], preferred_element_type=F32)
                c[:, cols] = jnp.where(left, ctx[:tgt], ctx[tgt:]).astype(BF16)
            run_ticks(plan, g * batch + b, steps)

        spec = lambda length: pl.BlockSpec((length, group), lambda g, b: (b, g))
        with jax.named_scope(stage):
            pltpu.emit_pipeline(body, grid=(width // group, batch), in_specs=[spec(tgt), spec(keys), spec(keys)], out_specs=[spec(tgt)])(q_ref, k_src, v_src, c_ref)

    def self_attention():
        heads = min(GROUP, width) // HEAD_DIM
        causal = lax.broadcasted_iota(jnp.int32, (tgt, tgt), 1) <= lax.broadcasted_iota(jnp.int32, (tgt, tgt), 0)

        def prepare(g, b):
            @pl.when(b == 0)
            def _():
                @pl.loop(0, heads)
                def _(h):
                    row = jnp.broadcast_to(dist_s[pl.ds(g * heads + h, 1), :], (tgt, dist_s.shape[1]))
                    bias_s[h] = pltpu.roll(row, 0, 1, stride=1, stride_axis=0)[:, :tgt]

        def mask_scores(scores, h, b):
            allowed = causal & (dec_mask_ref[pl.ds(b, 1), :] > 0)
            return jnp.where(allowed, scores + bias_s[h], MASK_FILL)

        attend('self_attend', tgt, k_ref, v_ref, prepare, mask_scores)

    def cross_attention():
        def mask_scores(scores, h, b):
            return jnp.where(enc_mask_ref[pl.ds(b, 1), :] > 0, scores, MASK_FILL)

        attend('cross_attend', src, ck_ref, cv_ref, lambda g, b: None, mask_scores)

    hidden = big.at[:, pl.ds(0, width)]

    barrier = pltpu.get_barrier_semaphore()
    for j in range(1, N_DEV):
        pl.semaphore_signal(barrier, inc=1, device_id={'fsdp': me ^ j}, device_id_type=MESH)
    pl.semaphore_wait(barrier, N_DEV - 1)

    @pl.loop(0, AHEAD)
    def _(t):
        on_task(t, 0, AHEAD, send)

    def norm_copy(j):
        return pltpu.make_async_remote_copy(src_ref=norm_ref, dst_ref=gain_in.at[me], send_sem=norm_send.at[j], recv_sem=norm_recv.at[j],
                                            device_id={'fsdp': me ^ j}, device_id_type=MESH)

    for j in range(1, N_DEV):
        norm_copy(j).start()
    load_dec = pltpu.make_async_copy(dec_ref, x_s, load_sem)
    load_dec.start()
    load_norm = pltpu.make_async_copy(norm_ref, gain_in.at[me], norm_send.at[0])
    load_norm.start()
    small = [pltpu.make_async_copy(*pair, small_sem.at[k]) for k, pair in enumerate(((rel_in, rel_ref), (dec_mask_in, dec_mask_ref), (enc_mask_in, enc_mask_ref)))]
    for copy in small:
        copy.start()
    plan = stage_ticks('head')

    def head_ticks(begin, end):
        with jax.named_scope('head'):
            @pl.loop(begin, end)
            def _(i):
                tick(i, plan[0], plan[0] + plan[1])

    head_ticks(0, 2)
    for copy in small:
        copy.wait()
    lanes = dist_s.shape[1]
    row = lax.broadcasted_iota(jnp.int32, (lanes, rel_ref.shape[1]), 0)
    distance = jnp.where(row == 0, 0, lanes - row)
    table = jnp.broadcast_to(rel_ref[0:1, :], row.shape)
    for b, start in enumerate(bucket_starts(tgt)):
        table = jnp.where(distance >= start, rel_ref[b + 1:b + 2, :], table)
    dist_s[...] = table.T
    head_ticks(2, 4)
    for j in range(1, N_DEV):
        norm_copy(j).wait()
    load_norm.wait()
    per = width // N_DEV
    for d in range(N_DEV):
        gains[:, d * per:(d + 1) * per] = gain_in[d]
    load_dec.wait()
    norm(0)
    head_ticks(4, plan[1])

    project('self_q', 'self_q', q_ref)
    project('self_k', 'self_k', k_ref)
    project('self_v', 'self_v', v_ref)
    self_attention()
    load(c_ref, hidden)
    residual('self_o', 'self_o')
    for name, dst in (('cross_k', ck_ref), ('cross_v', cv_ref)):
        for half in range(2):
            load(enc_ref.at[pl.ds(half * rows, rows), :], hidden)
            project(name, f'{name}{half}', dst, half)
    norm(1)
    project('cross_q', 'cross_q', q_ref)
    cross_attention()
    load(c_ref, hidden)
    residual('cross_o', 'cross_o')
    norm(2)

    cols = weights['ff_gate'].width // 2
    block = pl.BlockSpec((rows, cols), lambda n: (0, n))

    def store_gate(total, span, n, g):
        g[span, :] = total.astype(BF16)

    def store_lin(total, span, n, g, z):
        act = jax.nn.gelu(g[span, :].astype(F32), approximate=True)
        z[span, :] = (act * total.astype(BF16).astype(F32)).astype(BF16)

    matmul('ff_gate', 'ff_gate', 2, store_gate, out_specs=[block], outs=[g_ref])
    matmul('ff_lin', 'ff_lin', 2, store_lin, in_specs=[block], ins=[g_ref], out_specs=[block], outs=[z_ref])
    load(z_ref, big)
    w = weights['ff_out']

    def ff_out_loop(early, late, total, outs, early_sem, late_sem, out_sem):
        cols, half = w.width, w.rows // 2
        direct = (2, 4, 3, 5)
        begins = lambda j, first: 0 if (j in (2, 3)) == first else half

        def span_of(m):
            return pl.ds(pl.multiple_of(m * row_block, row_block), row_block)

        def cols_of(n):
            return pl.ds(pl.multiple_of(n * cols, cols), cols)

        def product(span, parts):
            terms = [jnp.dot(big[span, pl.ds(pl.multiple_of((me ^ j) * w.rows + at, 128), size)], read(), preferred_element_type=F32) for j, at, size, read in parts]
            return sum(terms[1:], terms[0])

        def add(n, parts, new=False):
            @pl.loop(0, rows // row_block)
            def _(m):
                at = (lax.rem(n, 2), span_of(m), slice(None))
                part = product(span_of(m), parts)
                total[at] = part if new else total[at] + part

        def whole(p, j):
            return (j, 0, w.rows, lambda: early[p])

        def halves(n, first, which):
            return [(j, begins(j, first), half, lambda p=p, j=j: late[lax.rem(n, 2), p, pl.ds(begins(j, first), half), :]) for p, j in enumerate(direct) if j in which]

        def fetch(n, p, j):
            return pltpu.make_async_copy(w.shard.at[:, cols_of(n)] if j == 0 else w.got.at[j - 1, :, cols_of(n)], early.at[p], early_sem.at[p])

        def fetch_half(n, j, first):
            p, span = direct.index(j), pl.ds(begins(j, first), half)
            return pltpu.make_async_copy(w.got.at[j - 1, span, cols_of(n)], late.at[lax.rem(n, 2), p, span], late_sem.at[lax.rem(n, 2), 2 * p + int(first)])

        def out_copy(n):
            return pltpu.make_async_copy(outs.at[lax.rem(n, 2)], out_ref.at[:, cols_of(n)], out_sem.at[lax.rem(n, 2)])

        def task(n):
            return Task(w, n, lax.rem(w.first + n, RING))

        def fetch_early(n):
            for p in (0, 1):
                fetch(n, p, p).start()
            task(n).got_all(SWAP_FIRST, 1)
            for j in direct:
                fetch_half(n, j, True).start()

        def add_own(n):
            for p in (0, 1):
                fetch(n, p, p).wait()
            add(n, [whole(0, 0), whole(1, 1)], new=True)

        def add_first(n):
            for j in direct:
                fetch_half(n, j, True).wait()
            add(n, halves(n, True, direct))

        fetch_early(0)
        add_own(0)

        @pl.loop(0, w.count)
        def _(n):
            t = task(n)
            more = n < w.count - 1

            @pl.when(more)
            def _():
                fetch_early(n + 1)

            with jax.named_scope('wait_diagonal'):
                pass_on_diagonal(t)
            fetch(n, 2, 6).start()
            add_first(n)
            t.swap_d().wait_recv()
            fetch(n, 3, 7).start()
            for p, j in ((2, 6), (3, 7)):
                fetch(n, p, j).wait()
                add(n, [whole(p, j)])
            with jax.named_scope('wait_rest'):
                pass_on_rest(t)
            for j in (2, 4):
                fetch_half(n, j, False).start()
            pl.when(more)(lambda: add_own(n + 1))
            for j in (2, 4):
                fetch_half(n, j, False).wait()
            add(n, halves(n, False, (2, 4)))
            t.got_all(SWAP, 1)
            for j in (3, 5):
                fetch_half(n, j, False).start()

            @pl.when(n >= 2)
            def _():
                out_copy(n - 2).wait()

            for j in (3, 5):
                fetch_half(n, j, False).wait()

            @pl.loop(0, rows // row_block)
            def _(m):
                span = span_of(m)
                update = (total[lax.rem(n, 2), span, :] + product(span, halves(n, False, (3, 5)))).astype(BF16)
                outs[lax.rem(n, 2), span, :] = (x_s[span, cols_of(n)].astype(F32) + update.astype(F32)).astype(BF16)

            out_copy(n).start()
            t.sent_all()
            with jax.named_scope('ticks'):
                on_task(out_look + n, out_look, out_look + w.count, arrive, [w])
                on_task(out_look + AHEAD + n, out_look + AHEAD, out_look + AHEAD + w.count, send, [w])

            @pl.when(n == w.count - 1)
            def _():
                out_copy(n - 1).wait()
                out_copy(n).wait()

    dma = pltpu.SemaphoreType.DMA
    with jax.named_scope('ff_out'):
        pl.run_scoped(ff_out_loop, pltpu.VMEM((4, w.rows, w.width), BF16), pltpu.VMEM((2, 4, w.rows, w.width), BF16), pltpu.VMEM((2, rows, w.width), F32),
                      pltpu.VMEM((2, rows, w.width), BF16), dma((4,)), dma((2, 8)), dma((2,)))


def hand_on_kernel(src_ref, dst_ref, held, read_sem, write_sem):
    parts = read_sem.shape[0]
    size = src_ref.shape[0] // parts
    read = lambda k: pltpu.make_async_copy(src_ref.at[pl.ds(k * size, size)], held.at[pl.ds(k * size, size)], read_sem.at[k])
    write = lambda k: pltpu.make_async_copy(held.at[pl.ds(k * size, size)], dst_ref.at[pl.ds(k * size, size)], write_sem.at[k])
    for k in range(parts):
        read(k).start()
    for k in range(parts):
        read(k).wait()
        write(k).start()
    for k in range(parts):
        write(k).wait()


def hand_on(x):
    parts = 24
    any_spec, dma = pl.BlockSpec(memory_space=pl.ANY), pltpu.SemaphoreType.DMA
    return pl.pallas_call(hand_on_kernel, out_shape=jax.ShapeDtypeStruct(x.shape, x.dtype), in_specs=[any_spec], out_specs=any_spec,
                          scratch_shapes=[pltpu.VMEM(x.shape, x.dtype), dma((parts,)), dma((parts,))], name='hand_on')(x)


def local_layer(dec_in, enc_out, dec_mask, enc_mask, rel_bias, norm_self, self_q, self_k, self_v, self_o, norm_cross, cross_q, cross_k, cross_v, cross_o, norm_ff, ff_gate, ff_lin, ff_out):
    batch, tgt, width = dec_in.shape
    src = enc_out.shape[1]
    rows = batch * tgt
    given = dict(self_q=self_q, self_k=self_k, self_v=self_v, self_o=self_o, cross_k=cross_k, cross_v=cross_v, cross_q=cross_q, cross_o=cross_o, ff_gate=ff_gate, ff_lin=ff_lin, ff_out=ff_out)
    names = list(TASKS)
    shards = [given[n] for n in names]
    lanes = -(-2 * tgt // 128) * 128 if tgt % 128 == 0 else -(-(tgt + 1) // 128) * 128
    which = lax.broadcasted_iota(jnp.int32, (4, norm_self.shape[0]), 0)
    norms = jnp.where(which == 0, norm_self[None], jnp.where(which == 1, norm_cross[None], norm_ff[None])).astype(F32)
    any_spec = pl.BlockSpec(memory_space=pl.ANY)
    hbm = lambda *shape: jax.ShapeDtypeStruct(shape, BF16)
    ff = ff_gate.shape[1]
    heads = rel_bias.shape[1]
    outs = [hbm(rows, width)] + [hbm(rows, width)] * 4 + [hbm(batch * src, width)] * 2 + [hbm(rows, ff)] * 2 + [hbm(N_DEV - 1, *s.shape) for s in shards]
    dma = pltpu.SemaphoreType.DMA
    flops = 2 * rows * width * (6 * width + 3 * ff) + 4 * batch * src * width * width
    result = pl.pallas_call(
        lambda *refs: layer_kernel(batch, names, *refs),
        out_shape=outs,
        in_specs=[any_spec] * (6 + len(shards)),
        out_specs=[any_spec] * len(outs),
        scratch_shapes=[
            pltpu.VMEM((rows, width), BF16),
            pltpu.VMEM((rows, ff), BF16),
            pltpu.VMEM((min(GROUP, width) // HEAD_DIM, tgt, tgt), F32),
            pltpu.VMEM((heads, lanes), F32),
            pltpu.VMEM((N_DEV,) + norms.shape, F32),
            pltpu.VMEM((4, width), F32),
            pltpu.VMEM(rel_bias.shape, F32), pltpu.VMEM(dec_mask.shape, jnp.int32), pltpu.VMEM(enc_mask.shape, jnp.int32),
            dma((RING,)), dma((KINDS, RING)), dma((N_DEV,)), dma((N_DEV,)), dma(()), dma((3,)),
        ],
        compiler_params=pltpu.CompilerParams(collective_id=0, has_side_effects=True, vmem_limit_bytes=67_043_328),
        cost_estimate=pl.CostEstimate(flops=flops, bytes_accessed=20 * sum(s.size for s in shards), transcendentals=0),
        name='layer',
    )(rel_bias, dec_mask, enc_mask, norms, dec_in.reshape(rows, width), enc_out.reshape(batch * src, width), *shards)
    return hand_on(result[0]).reshape(dec_in.shape)


def solution(mesh):
    row_spec = P(('dp', 'fsdp'), None, None)
    mask_spec = P(('dp', 'fsdp'), None)
    weight_spec = P('fsdp', None)
    scale_spec = P('fsdp')
    in_specs = (row_spec, row_spec, mask_spec, mask_spec, P(None, None), scale_spec, weight_spec, weight_spec, weight_spec, weight_spec, scale_spec, weight_spec, weight_spec, weight_spec, weight_spec, scale_spec, weight_spec, weight_spec, weight_spec)
    return jax.shard_map(local_layer, mesh=mesh, in_specs=in_specs, out_specs=row_spec, check_vma=False)
```

```python
import math
import jax
import jax.numpy as jnp
from jax import lax
from jax.experimental import pallas as pl
from jax.experimental.pallas import tpu as pltpu
from jax.sharding import PartitionSpec as P

MESH = pl.DeviceIdType.MESH
F32, BF16 = jnp.float32, jnp.bfloat16
HEAD_DIM = 64
NUM_BUCKETS = 32
EXACT_BUCKETS = 16
MAX_DISTANCE = 128
NORM_EPS = 1e-6
MASK_FILL = -1e9
N_DEV = 8

AHEAD, PASS, DONE, RING = 4, 4, 5, 14
PARTNER, FIRST, REST, RELAY, SWAP_FIRST, SWAP, SWAP_D, KINDS = range(8)
TASKS = {'self_q': 8, 'self_k': 8, 'self_v': 8, 'self_o': 8, 'cross_k': 8, 'cross_v': 8, 'cross_q': 8, 'cross_o': 8, 'ff_gate': 20, 'ff_lin': 20, 'ff_out': 16}
ALL_TASKS = sum(TASKS.values())
TICKS = {'head': DONE + 2, 'self_q': 8, 'self_k': 8, 'self_v': 8, 'self_attend': 6, 'self_o': 6, 'cross_k0': 6, 'cross_k1': 5, 'cross_v0': 6, 'cross_v1': 5,
         'cross_q': 6, 'cross_attend': 10, 'cross_o': 6, 'ff_gate': 12, 'ff_lin': 10}
assert sum(TICKS.values()) == ALL_TASKS - TASKS['ff_out'] + DONE
ROW_BLOCK = 512
GROUP = 512


def bucket_ids(length):
    return [offset if offset < EXACT_BUCKETS else min(NUM_BUCKETS - 1, EXACT_BUCKETS + int(math.log(offset / EXACT_BUCKETS) / math.log(MAX_DISTANCE / EXACT_BUCKETS) * (NUM_BUCKETS - EXACT_BUCKETS))) for offset in range(length)]


def bucket_starts(length):
    ids = bucket_ids(length)
    return [next(n for n in range(length) if ids[n] >= b) for b in range(1, ids[-1] + 1)]


class Weight:
    def __init__(self, first, count, shard, got):
        self.first, self.count, self.shard, self.got = first, count, shard, got
        self.rows, self.width = shard.shape[0], shard.shape[1] // count


def layer_kernel(batch, names, rel_in, dec_mask_in, enc_mask_in, norm_ref, dec_ref, enc_ref, *refs):
    n_w = len(names)
    shards, refs = refs[:n_w], refs[n_w:]
    out_ref, q_ref, k_ref, v_ref, c_ref, ck_ref, cv_ref, g_ref, z_ref = refs[:9]
    gots, refs = refs[9:9 + n_w], refs[9 + n_w:]
    x_s, big, bias_s, dist_s, gain_in, gains, rel_ref, dec_mask_ref, enc_mask_ref, send_sem, recv_sem, norm_send, norm_recv, load_sem, small_sem = refs

    me = lax.axis_index('fsdp')
    weights, first = {}, 0
    for name, shard, got in zip(names, shards, gots):
        weights[name] = Weight(first, TASKS[name], shard, got)
        first += TASKS[name]
    rows, width = dec_ref.shape
    tgt = rows // batch
    src = enc_ref.shape[0] // batch
    row_block = min(ROW_BLOCK, rows)

    def remote(src_ref, dst_ref, kind, ring, bit):
        return pltpu.make_async_remote_copy(src_ref=src_ref, dst_ref=dst_ref, send_sem=send_sem.at[ring], recv_sem=recv_sem.at[kind, ring],
                                            device_id={'fsdp': me ^ bit}, device_id_type=MESH)

    class Task:
        def __init__(self, w, m, ring):
            cols = pl.ds(pl.multiple_of(m * w.width, w.width), w.width)
            own = w.shard.at[:, cols]
            slot = lambda j: w.got.at[j - 1, :, cols]
            bottom, top = pl.ds(0, w.rows // 2), pl.ds(w.rows // 2, w.rows // 2)
            low = lambda j: w.got.at[j - 1, bottom, cols]
            high = lambda j: w.got.at[j - 1, top, cols]
            self.to_partner = lambda: remote(own, slot(1), PARTNER, ring, 1)
            self.first_x = lambda: remote(w.shard.at[bottom, cols], low(2), FIRST, ring, 2)
            self.first_y = lambda: remote(w.shard.at[top, cols], high(4), FIRST, ring, 4)
            self.rest_x = lambda: remote(w.shard.at[top, cols], high(2), REST, ring, 2)
            self.rest_y = lambda: remote(w.shard.at[bottom, cols], low(4), REST, ring, 4)
            self.relay_y = lambda: remote(low(2), low(6), RELAY, ring, 4)
            self.relay_x = lambda: remote(high(4), high(6), RELAY, ring, 2)
            self.swap_x = lambda: remote(slot(2), slot(3), SWAP, ring, 1)
            self.swap_y = lambda: remote(slot(4), slot(5), SWAP, ring, 1)
            self.swap_d = lambda: remote(slot(6), slot(7), SWAP_D, ring, 1)
            self.swap_first_x = lambda: remote(low(2), low(3), SWAP_FIRST, ring, 1)
            self.swap_first_y = lambda: remote(high(4), high(5), SWAP_FIRST, ring, 1)
            self.swap_rest_x = lambda: remote(high(2), high(3), SWAP, ring, 1)
            self.swap_rest_y = lambda: remote(low(4), low(5), SWAP, ring, 1)
            self.halves = w is weights['ff_out']
            shape = lambda slots: w.got.at[pl.ds(0, slots), :, cols]
            self.got_all = lambda kind, slots: remote(shape(slots), shape(slots), kind, ring, 1).wait_recv()
            self.sent_all = lambda: remote(shape(7), shape(7), PARTNER, ring, 1).wait_send()

    def send(t):
        for copy in (t.first_x, t.first_y, t.to_partner):
            copy().start()

    def arrive(t):
        t.to_partner().wait_recv()
        t.got_all(FIRST, 1)
        for copy in (t.relay_y, t.relay_x, t.rest_y, t.rest_x, *((t.swap_first_x, t.swap_first_y) if t.halves else ())):
            copy().start()

    def pass_on_diagonal(t):
        t.got_all(RELAY, 1)
        t.swap_d().start()

    def pass_on_rest(t):
        t.got_all(REST, 1)
        for copy in (t.swap_rest_x, t.swap_rest_y) if t.halves else (t.swap_x, t.swap_y):
            copy().start()

    def pass_on(t):
        pass_on_diagonal(t)
        pass_on_rest(t)

    def finish(t):
        t.swap_d().wait_recv()
        t.got_all(SWAP, 2)
        t.sent_all()

    def on_task(t, low, high, act, among=None, stop=ALL_TASKS):
        for w in among or weights.values():
            last = min(w.first + w.count, stop)
            if low < last and w.first < high:
                def run(w=w):
                    act(Task(w, t - w.first, lax.rem(t, RING)))
                if w.first <= low and high <= last:
                    run()
                else:
                    pl.when((t >= w.first) & (t < last))(run)

    streamed = [w for name, w in weights.items() if name != 'ff_out']
    out_look = weights['ff_out'].first + PASS

    def tick(i, low, high):
        on_task(i, low, high, arrive, stop=out_look)
        on_task(i + AHEAD, low + AHEAD, high + AHEAD, send, stop=out_look + AHEAD)
        on_task(i - PASS, low - PASS, high - PASS, pass_on, streamed)
        on_task(i - DONE, low - DONE, high - DONE, finish, streamed)

    done = [0]

    def stage_ticks(name):
        low, count = done[0], TICKS[name]
        done[0] = low + count
        return low, count

    def ticks_before(plan, n, steps, least=min):
        low, count = plan
        spread = steps if count == steps else max(steps - 4, 1)
        return low + least((n * count) // spread, count)

    def run_ticks(plan, n, steps):
        with jax.named_scope('ticks'):
            @pl.loop(ticks_before(plan, n, steps, jnp.minimum), ticks_before(plan, n + 1, steps, jnp.minimum))
            def _(i):
                tick(i, plan[0], plan[0] + plan[1])

    def load(src_ref, dst_ref):
        copy = pltpu.make_async_copy(src_ref, dst_ref, load_sem)
        copy.start()
        copy.wait()

    def norm(which):
        @pl.loop(0, rows // 16)
        def _(r):
            span = pl.ds(pl.multiple_of(r * 16, 16), 16)
            v = x_s[span, :].astype(F32)
            scale = lax.rsqrt(jnp.mean(v * v, axis=-1, keepdims=True) + NORM_EPS)
            big[span, pl.ds(0, width)] = (v * scale * gains[pl.ds(which, 1), :]).astype(BF16)

    def matmul(name, stage, split, store, in_specs=(), ins=(), out_specs=(), outs=()):
        w = weights[name]
        steps, cols = w.count * split, w.width // split
        plan = stage_ticks(stage)
        for n in range(steps):
            assert ticks_before(plan, n, steps) > w.first + min(n + 1, steps - 1) // split + DONE

        def body(own, got, *rest):
            n = pl.program_id(0)

            @pl.loop(0, rows // row_block)
            def _(m):
                span = pl.ds(pl.multiple_of(m * row_block, row_block), row_block)
                total = None
                for j in range(N_DEV):
                    part = big[span, pl.ds(pl.multiple_of((me ^ j) * w.rows, 128), w.rows)]
                    term = jnp.dot(part, own[...] if j == 0 else got[j - 1], preferred_element_type=F32)
                    total = term if total is None else total + term
                store(total, span, n, *rest)

            run_ticks(plan, n, steps)

        with jax.named_scope(stage):
            pltpu.emit_pipeline(
                body, grid=(steps,),
                in_specs=[pl.BlockSpec((w.rows, cols), lambda n: (0, n)), pl.BlockSpec((N_DEV - 1, w.rows, cols), lambda n: (0, 0, n)), *in_specs],
                out_specs=list(out_specs))(w.shard, w.got, *ins, *outs)

    def project(name, stage, dst_ref, half=0):
        cols = weights[name].width

        def store(total, span, n, dst):
            dst[span, :] = total.astype(BF16)

        matmul(name, stage, 1, store, out_specs=[pl.BlockSpec((rows, cols), lambda n: (half, n))], outs=[dst_ref])

    def residual(name, stage):
        cols = weights[name].width

        def store(total, span, n):
            where = (span, pl.ds(pl.multiple_of(n * cols, cols), cols))
            x_s[where] = (x_s[where].astype(F32) + total.astype(BF16).astype(F32)).astype(BF16)

        matmul(name, stage, 1, store)

    left = lax.broadcasted_iota(jnp.int32, (tgt, 2 * HEAD_DIM), 1) < HEAD_DIM

    def softmax(scores):
        e = jnp.exp(scores - jnp.max(scores, axis=-1, keepdims=True))
        return (e * (1.0 / jnp.sum(e, axis=-1, keepdims=True))).astype(BF16)

    def attend(stage, keys, k_src, v_src, prepare, mask_scores):
        group = min(GROUP, width)
        plan = stage_ticks(stage)
        steps = (width // group) * batch

        def body(q, k, v, c):
            g, b = pl.program_id(0), pl.program_id(1)
            prepare(g, b)
            for pair in range(group // (2 * HEAD_DIM)):
                cols = pl.ds(pair * 2 * HEAD_DIM, 2 * HEAD_DIM)
                q_pair = q[:, cols].astype(F32)
                both = jnp.concatenate([jnp.where(left, q_pair, 0.0), jnp.where(left, 0.0, q_pair)], 0).astype(BF16)
                scores = lax.dot_general(both, k[:, cols], (((1,), (1,)), ((), ())), preferred_element_type=F32)
                prob = jnp.concatenate([softmax(mask_scores(scores[h * tgt:(h + 1) * tgt], 2 * pair + h, b)) for h in range(2)], 0)
                ctx = jnp.dot(prob, v[:, cols], preferred_element_type=F32)
                c[:, cols] = jnp.where(left, ctx[:tgt], ctx[tgt:]).astype(BF16)
            run_ticks(plan, g * batch + b, steps)

        spec = lambda length: pl.BlockSpec((length, group), lambda g, b: (b, g))
        with jax.named_scope(stage):
            pltpu.emit_pipeline(body, grid=(width // group, batch), in_specs=[spec(tgt), spec(keys), spec(keys)], out_specs=[spec(tgt)])(q_ref, k_src, v_src, c_ref)

    def self_attention():
        heads = min(GROUP, width) // HEAD_DIM
        causal = lax.broadcasted_iota(jnp.int32, (tgt, tgt), 1) <= lax.broadcasted_iota(jnp.int32, (tgt, tgt), 0)

        def prepare(g, b):
            @pl.when(b == 0)
            def _():
                @pl.loop(0, heads)
                def _(h):
                    row = jnp.broadcast_to(dist_s[pl.ds(g * heads + h, 1), :], (tgt, dist_s.shape[1]))
                    bias_s[h] = pltpu.roll(row, 0, 1, stride=1, stride_axis=0)[:, :tgt]

        def mask_scores(scores, h, b):
            allowed = causal & (dec_mask_ref[pl.ds(b, 1), :] > 0)
            return jnp.where(allowed, scores + bias_s[h], MASK_FILL)

        attend('self_attend', tgt, k_ref, v_ref, prepare, mask_scores)

    def cross_attention():
        def mask_scores(scores, h, b):
            return jnp.where(enc_mask_ref[pl.ds(b, 1), :] > 0, scores, MASK_FILL)

        attend('cross_attend', src, ck_ref, cv_ref, lambda g, b: None, mask_scores)

    hidden = big.at[:, pl.ds(0, width)]

    barrier = pltpu.get_barrier_semaphore()
    for j in range(1, N_DEV):
        pl.semaphore_signal(barrier, inc=1, device_id={'fsdp': me ^ j}, device_id_type=MESH)
    pl.semaphore_wait(barrier, N_DEV - 1)

    @pl.loop(0, AHEAD)
    def _(t):
        on_task(t, 0, AHEAD, send)

    def norm_copy(j):
        return pltpu.make_async_remote_copy(src_ref=norm_ref, dst_ref=gain_in.at[me], send_sem=norm_send.at[j], recv_sem=norm_recv.at[j],
                                            device_id={'fsdp': me ^ j}, device_id_type=MESH)

    for j in range(1, N_DEV):
        norm_copy(j).start()
    load_dec = pltpu.make_async_copy(dec_ref, x_s, load_sem)
    load_dec.start()
    load_norm = pltpu.make_async_copy(norm_ref, gain_in.at[me], norm_send.at[0])
    load_norm.start()
    small = [pltpu.make_async_copy(*pair, small_sem.at[k]) for k, pair in enumerate(((rel_in, rel_ref), (dec_mask_in, dec_mask_ref), (enc_mask_in, enc_mask_ref)))]
    for copy in small:
        copy.start()
    plan = stage_ticks('head')

    def head_ticks(begin, end):
        with jax.named_scope('head'):
            @pl.loop(begin, end)
            def _(i):
                tick(i, plan[0], plan[0] + plan[1])

    head_ticks(0, 2)
    for copy in small:
        copy.wait()
    lanes = dist_s.shape[1]
    row = lax.broadcasted_iota(jnp.int32, (lanes, rel_ref.shape[1]), 0)
    distance = jnp.where(row == 0, 0, lanes - row)
    table = jnp.broadcast_to(rel_ref[0:1, :], row.shape)
    for b, start in enumerate(bucket_starts(tgt)):
        table = jnp.where(distance >= start, rel_ref[b + 1:b + 2, :], table)
    dist_s[...] = table.T
    head_ticks(2, 4)
    for j in range(1, N_DEV):
        norm_copy(j).wait()
    load_norm.wait()
    per = width // N_DEV
    for d in range(N_DEV):
        gains[:, d * per:(d + 1) * per] = gain_in[d]
    load_dec.wait()
    norm(0)
    head_ticks(4, plan[1])

    project('self_q', 'self_q', q_ref)
    project('self_k', 'self_k', k_ref)
    project('self_v', 'self_v', v_ref)
    self_attention()
    load(c_ref, hidden)
    residual('self_o', 'self_o')
    for name, dst in (('cross_k', ck_ref), ('cross_v', cv_ref)):
        for half in range(2):
            load(enc_ref.at[pl.ds(half * rows, rows), :], hidden)
            project(name, f'{name}{half}', dst, half)
    norm(1)
    project('cross_q', 'cross_q', q_ref)
    cross_attention()
    load(c_ref, hidden)
    residual('cross_o', 'cross_o')
    norm(2)

    cols = weights['ff_gate'].width // 2
    block = pl.BlockSpec((rows, cols), lambda n: (0, n))

    def store_gate(total, span, n, g):
        g[span, :] = total.astype(BF16)

    def store_lin(total, span, n, g, z):
        act = jax.nn.gelu(g[span, :].astype(F32), approximate=True)
        z[span, :] = (act * total.astype(BF16).astype(F32)).astype(BF16)

    matmul('ff_gate', 'ff_gate', 2, store_gate, out_specs=[block], outs=[g_ref])
    matmul('ff_lin', 'ff_lin', 2, store_lin, in_specs=[block], ins=[g_ref], out_specs=[block], outs=[z_ref])
    load(z_ref, big)
    w = weights['ff_out']

    def ff_out_loop(early, late, total, outs, early_sem, late_sem, out_sem):
        cols, half = w.width, w.rows // 2
        direct = (2, 4, 3, 5)
        begins = lambda j, first: 0 if (j in (2, 3)) == first else half

        def span_of(m):
            return pl.ds(pl.multiple_of(m * row_block, row_block), row_block)

        def cols_of(n):
            return pl.ds(pl.multiple_of(n * cols, cols), cols)

        def product(span, parts):
            terms = [jnp.dot(big[span, pl.ds(pl.multiple_of((me ^ j) * w.rows + at, 128), size)], read(), preferred_element_type=F32) for j, at, size, read in parts]
            return sum(terms[1:], terms[0])

        def add(n, parts, new=False):
            @pl.loop(0, rows // row_block)
            def _(m):
                at = (lax.rem(n, 2), span_of(m), slice(None))
                part = product(span_of(m), parts)
                total[at] = part if new else total[at] + part

        def whole(p, j):
            return (j, 0, w.rows, lambda: early[p])

        def halves(n, first, which):
            return [(j, begins(j, first), half, lambda p=p, j=j: late[lax.rem(n, 2), p, pl.ds(begins(j, first), half), :]) for p, j in enumerate(direct) if j in which]

        def fetch(n, p, j):
            return pltpu.make_async_copy(w.shard.at[:, cols_of(n)] if j == 0 else w.got.at[j - 1, :, cols_of(n)], early.at[p], early_sem.at[p])

        def fetch_half(n, j, first):
            p, span = direct.index(j), pl.ds(begins(j, first), half)
            return pltpu.make_async_copy(w.got.at[j - 1, span, cols_of(n)], late.at[lax.rem(n, 2), p, span], late_sem.at[lax.rem(n, 2), 2 * p + int(first)])

        def out_copy(n):
            return pltpu.make_async_copy(outs.at[lax.rem(n, 2)], out_ref.at[:, cols_of(n)], out_sem.at[lax.rem(n, 2)])

        def task(n):
            return Task(w, n, lax.rem(w.first + n, RING))

        def fetch_early(n):
            for p in (0, 1):
                fetch(n, p, p).start()
            task(n).got_all(SWAP_FIRST, 1)
            for j in direct:
                fetch_half(n, j, True).start()

        def add_own(n):
            for p in (0, 1):
                fetch(n, p, p).wait()
            add(n, [whole(0, 0), whole(1, 1)], new=True)

        def add_first(n):
            for j in direct:
                fetch_half(n, j, True).wait()
            add(n, halves(n, True, direct))

        fetch_early(0)
        add_own(0)

        @pl.loop(0, w.count)
        def _(n):
            t = task(n)
            more = n < w.count - 1

            @pl.when(more)
            def _():
                fetch_early(n + 1)

            with jax.named_scope('wait_diagonal'):
                pass_on_diagonal(t)
            fetch(n, 2, 6).start()
            add_first(n)
            t.swap_d().wait_recv()
            fetch(n, 3, 7).start()
            for p, j in ((2, 6), (3, 7)):
                fetch(n, p, j).wait()
                add(n, [whole(p, j)])
            with jax.named_scope('wait_rest'):
                pass_on_rest(t)
            for j in (2, 4):
                fetch_half(n, j, False).start()
            pl.when(more)(lambda: add_own(n + 1))
            for j in (2, 4):
                fetch_half(n, j, False).wait()
            add(n, halves(n, False, (2, 4)))
            t.got_all(SWAP, 1)
            for j in (3, 5):
                fetch_half(n, j, False).start()

            @pl.when(n >= 2)
            def _():
                out_copy(n - 2).wait()

            for j in (3, 5):
                fetch_half(n, j, False).wait()

            @pl.loop(0, rows // row_block)
            def _(m):
                span = span_of(m)
                update = (total[lax.rem(n, 2), span, :] + product(span, halves(n, False, (3, 5)))).astype(BF16)
                outs[lax.rem(n, 2), span, :] = (x_s[span, cols_of(n)].astype(F32) + update.astype(F32)).astype(BF16)

            out_copy(n).start()
            t.sent_all()
            with jax.named_scope('ticks'):
                on_task(out_look + n, out_look, out_look + w.count, arrive, [w])
                on_task(out_look + AHEAD + n, out_look + AHEAD, out_look + AHEAD + w.count, send, [w])

            @pl.when(n == w.count - 1)
            def _():
                out_copy(n - 1).wait()
                out_copy(n).wait()

    dma = pltpu.SemaphoreType.DMA
    with jax.named_scope('ff_out'):
        pl.run_scoped(ff_out_loop, pltpu.VMEM((4, w.rows, w.width), BF16), pltpu.VMEM((2, 4, w.rows, w.width), BF16), pltpu.VMEM((2, rows, w.width), F32),
                      pltpu.VMEM((2, rows, w.width), BF16), dma((4,)), dma((2, 8)), dma((2,)))


def hand_on_kernel(src_ref, dst_ref, held, read_sem, write_sem):
    parts = read_sem.shape[0]
    size = src_ref.shape[0] // parts
    read = lambda k: pltpu.make_async_copy(src_ref.at[pl.ds(k * size, size)], held.at[pl.ds(k * size, size)], read_sem.at[k])
    write = lambda k: pltpu.make_async_copy(held.at[pl.ds(k * size, size)], dst_ref.at[pl.ds(k * size, size)], write_sem.at[k])
    for k in range(parts):
        read(k).start()
    for k in range(parts):
        read(k).wait()
        write(k).start()
    for k in range(parts):
        write(k).wait()


def hand_on(x):
    parts = 8
    any_spec, dma = pl.BlockSpec(memory_space=pl.ANY), pltpu.SemaphoreType.DMA
    return pl.pallas_call(hand_on_kernel, out_shape=jax.ShapeDtypeStruct(x.shape, x.dtype), in_specs=[any_spec], out_specs=any_spec,
                          scratch_shapes=[pltpu.VMEM(x.shape, x.dtype), dma((parts,)), dma((parts,))], name='hand_on')(x)


def local_layer(dec_in, enc_out, dec_mask, enc_mask, rel_bias, norm_self, self_q, self_k, self_v, self_o, norm_cross, cross_q, cross_k, cross_v, cross_o, norm_ff, ff_gate, ff_lin, ff_out):
    batch, tgt, width = dec_in.shape
    src = enc_out.shape[1]
    rows = batch * tgt
    given = dict(self_q=self_q, self_k=self_k, self_v=self_v, self_o=self_o, cross_k=cross_k, cross_v=cross_v, cross_q=cross_q, cross_o=cross_o, ff_gate=ff_gate, ff_lin=ff_lin, ff_out=ff_out)
    names = list(TASKS)
    shards = [given[n] for n in names]
    lanes = -(-2 * tgt // 128) * 128 if tgt % 128 == 0 else -(-(tgt + 1) // 128) * 128
    which = lax.broadcasted_iota(jnp.int32, (4, norm_self.shape[0]), 0)
    norms = jnp.where(which == 0, norm_self[None], jnp.where(which == 1, norm_cross[None], norm_ff[None])).astype(F32)
    any_spec = pl.BlockSpec(memory_space=pl.ANY)
    hbm = lambda *shape: jax.ShapeDtypeStruct(shape, BF16)
    ff = ff_gate.shape[1]
    heads = rel_bias.shape[1]
    outs = [hbm(rows, width)] + [hbm(rows, width)] * 4 + [hbm(batch * src, width)] * 2 + [hbm(rows, ff)] * 2 + [hbm(N_DEV - 1, *s.shape) for s in shards]
    dma = pltpu.SemaphoreType.DMA
    flops = 2 * rows * width * (6 * width + 3 * ff) + 4 * batch * src * width * width
    result = pl.pallas_call(
        lambda *refs: layer_kernel(batch, names, *refs),
        out_shape=outs,
        in_specs=[any_spec] * (6 + len(shards)),
        out_specs=[any_spec] * len(outs),
        scratch_shapes=[
            pltpu.VMEM((rows, width), BF16),
            pltpu.VMEM((rows, ff), BF16),
            pltpu.VMEM((min(GROUP, width) // HEAD_DIM, tgt, tgt), F32),
            pltpu.VMEM((heads, lanes), F32),
            pltpu.VMEM((N_DEV,) + norms.shape, F32),
            pltpu.VMEM((4, width), F32),
            pltpu.VMEM(rel_bias.shape, F32), pltpu.VMEM(dec_mask.shape, jnp.int32), pltpu.VMEM(enc_mask.shape, jnp.int32),
            dma((RING,)), dma((KINDS, RING)), dma((N_DEV,)), dma((N_DEV,)), dma(()), dma((3,)),
        ],
        compiler_params=pltpu.CompilerParams(collective_id=0, has_side_effects=True, vmem_limit_bytes=67_043_328),
        cost_estimate=pl.CostEstimate(flops=flops, bytes_accessed=20 * sum(s.size for s in shards), transcendentals=0),
        name='layer',
    )(rel_bias, dec_mask, enc_mask, norms, dec_in.reshape(rows, width), enc_out.reshape(batch * src, width), *shards)
    return hand_on(result[0]).reshape(dec_in.shape)


def solution(mesh):
    row_spec = P(('dp', 'fsdp'), None, None)
    mask_spec = P(('dp', 'fsdp'), None)
    weight_spec = P('fsdp', None)
    scale_spec = P('fsdp')
    in_specs = (row_spec, row_spec, mask_spec, mask_spec, P(None, None), scale_spec, weight_spec, weight_spec, weight_spec, weight_spec, scale_spec, weight_spec, weight_spec, weight_spec, weight_spec, scale_spec, weight_spec, weight_spec, weight_spec)
    return jax.shard_map(local_layer, mesh=mesh, in_specs=in_specs, out_specs=row_spec, check_vma=False)
```
